16 devices in a mesh: dp: 2 (over z), tp: 8 (over y, x, core).
Axes of the slice: x: 2, y: 2, z: 2, core: 2. Of those that a mesh axis runs over, the one named last changes fastest.
Arguments:
- residual: float32 [1024, 1536], P('dp'), parts along dimension 0
- norm_w: bfloat16 [2, 1536], replicated
- w_in: bfloat16 [2, 1536, 2, 3072], P(None, None, None, 'tp')
- conv_w: bfloat16 [2, 4, 3072], P(None, None, 'tp')
- conv_b: bfloat16 [2, 3072], P(None, 'tp')
- w_x: bfloat16 [2, 3072, 128], P(None, 'tp')
- w_dt: bfloat16 [2, 96, 3072], P(None, None, 'tp')
- b_dt: float32 [2, 3072], P(None, 'tp')
- a_log: float32 [2, 16, 3072], P(None, None, 'tp')
- d_skip: float32 [2, 3072], P(None, 'tp')
- w_out: bfloat16 [2, 3072, 1536], P(None, 'tp')
- conv_state: bfloat16 [2, 1024, 3, 3072], P(None, 'dp', None, 'tp'), parts along dimension 1
- ssm_state: float32 [2, 1024, 16, 3072], P(None, 'dp', None, 'tp'), parts along dimension 1
Outputs:
- output 1: float32 [1024, 1536], P('dp'), parts along dimension 0
- output 2: bfloat16 [2, 1024, 3, 3072], P(None, 'dp', None, 'tp'), parts along dimension 1
- output 3: float32 [2, 1024, 16, 3072], P(None, 'dp', None, 'tp'), parts along dimension 1
There are 2 independent parts. The reference program is written for one: setup_inputs(seed, part) draws one part's arguments, and reference() takes and returns one part's arrays. A program takes and returns all parts, laid end to end along the dimension named above; an argument that names none is the same for every part.
All inputs are finite; a program needn't handle non-finite values.
Results may differ from the reference program's by a relative error of at most 0.0189318.
Values are sent between devices in bfloat16 or wider.
A program may use at most 1 GiB of HBM per device.

```python
import math
import jax
import jax.numpy as jnp
from jax import lax

D = 1536
INNER = 3072
STATE = 16
RANK = 96
CONV = 4
LAYERS = 2
BATCH = 512


def setup_inputs(seed: int = 0, part: int = 0) -> dict:
    root_key = jax.random.key(seed)
    shared = jax.random.split(root_key, 10)
    part_keys = jax.random.split(jax.random.fold_in(root_key, part), 3)
    proj_width = RANK + 2 * STATE
    residual = jax.random.normal(part_keys[0], (BATCH, D), jnp.float32)
    norm_w = jax.random.uniform(shared[0], (LAYERS, D), jnp.float32, 0.5, 1.5).astype(jnp.bfloat16)
    w_in = (jax.random.normal(shared[1], (LAYERS, D, 2, INNER), jnp.float32) * D ** -0.5).astype(jnp.bfloat16)
    conv_w = (0.5 * jax.random.normal(shared[2], (LAYERS, CONV, INNER), jnp.float32)).astype(jnp.bfloat16)
    conv_b = (0.3 * jax.random.normal(shared[3], (LAYERS, INNER), jnp.float32)).astype(jnp.bfloat16)
    w_x = (jax.random.normal(shared[4], (LAYERS, INNER, proj_width), jnp.float32) * INNER ** -0.5).astype(jnp.bfloat16)
    w_dt = (jax.random.normal(shared[5], (LAYERS, RANK, INNER), jnp.float32) * (0.25 * RANK ** -0.5)).astype(jnp.bfloat16)
    dt_init = jnp.exp(jax.random.uniform(shared[6], (LAYERS, INNER), jnp.float32, math.log(0.05), math.log(0.25)))
    b_dt = dt_init + jnp.log(-jnp.expm1(-dt_init))
    a_log = jax.random.uniform(shared[7], (LAYERS, STATE, INNER), jnp.float32, -0.7, 0.7)
    d_skip = jax.random.uniform(shared[8], (LAYERS, INNER), jnp.float32, 0.5, 1.5)
    w_out = (jax.random.normal(shared[9], (LAYERS, INNER, D), jnp.float32) * INNER ** -0.5).astype(jnp.bfloat16)
    conv_state = jax.random.normal(part_keys[1], (LAYERS, BATCH, CONV - 1, INNER), jnp.float32).astype(jnp.bfloat16)
    ssm_state = 0.5 * jax.random.normal(part_keys[2], (LAYERS, BATCH, STATE, INNER), jnp.float32)
    return {'residual': residual, 'norm_w': norm_w, 'w_in': w_in, 'conv_w': conv_w, 'conv_b': conv_b, 'w_x': w_x, 'w_dt': w_dt, 'b_dt': b_dt, 'a_log': a_log, 'd_skip': d_skip, 'w_out': w_out, 'conv_state': conv_state, 'ssm_state': ssm_state}


def rms_norm(vector, epsilon):
    return vector * lax.rsqrt(jnp.mean(vector * vector, axis=-1, keepdims=True) + epsilon)


def mamba_layer(residual, params):
    norm_w, w_in, conv_w, conv_b, w_x, w_dt, b_dt, a_log, d_skip, w_out, conv_state, ssm_state = params
    hidden = (rms_norm(residual, 1e-5) * norm_w.astype(jnp.float32)).astype(jnp.bfloat16)
    x_part = jnp.dot(hidden, w_in[:, 0, :], preferred_element_type=jnp.float32).astype(jnp.bfloat16)
    z_part = jnp.dot(hidden, w_in[:, 1, :], preferred_element_type=jnp.float32).astype(jnp.bfloat16)
    window = jnp.concatenate([conv_state, x_part[:, None, :]], axis=1)
    conv_pre = jnp.sum(window.astype(jnp.float32) * conv_w.astype(jnp.float32)[None], axis=1) + conv_b.astype(jnp.float32)
    x_conv = jax.nn.silu(conv_pre).astype(jnp.bfloat16)
    proj_sum = jnp.dot(x_conv, w_x, preferred_element_type=jnp.float32)
    dt_low = rms_norm(proj_sum[:, :RANK], 1e-6).astype(jnp.bfloat16)
    b_vec = rms_norm(proj_sum[:, RANK:RANK + STATE], 1e-6)
    c_vec = rms_norm(proj_sum[:, RANK + STATE:], 1e-6)
    dt_val = jax.nn.softplus(jnp.dot(dt_low, w_dt, preferred_element_type=jnp.float32) + b_dt)
    x_float = x_conv.astype(jnp.float32)
    decay_fac = jnp.exp(dt_val[:, None, :] * -jnp.exp(a_log)[None])
    new_ssm = decay_fac * ssm_state + (dt_val * x_float)[:, None, :] * b_vec[:, :, None]
    y_val = jnp.sum(new_ssm * c_vec[:, :, None], axis=1) + d_skip * x_float
    gated_y = (y_val * jax.nn.silu(z_part.astype(jnp.float32))).astype(jnp.bfloat16)
    out_sum = jnp.dot(gated_y, w_out, preferred_element_type=jnp.float32)
    return residual + out_sum, (window[:, 1:, :], new_ssm)


def reference(residual, norm_w, w_in, conv_w, conv_b, w_x, w_dt, b_dt, a_log, d_skip, w_out, conv_state, ssm_state):
    resid_out, cache_new = lax.scan(mamba_layer, residual, (norm_w, w_in, conv_w, conv_b, w_x, w_dt, b_dt, a_log, d_skip, w_out, conv_state, ssm_state))
    return resid_out, cache_new[0], cache_new[1]
```

```python
import functools

import jax
import jax.numpy as jnp
from jax import lax
from jax.experimental import pallas as pl
from jax.experimental.pallas import tpu as pltpu
from jax.sharding import PartitionSpec as P

MESH = pl.DeviceIdType.MESH
LOG2E = 1.4426950408889634
CHUNKS = 4
COPIES = 8


def rms_scale(vector, epsilon):
    return lax.rsqrt(jnp.mean(vector * vector, axis=-1, keepdims=True) + epsilon)


def mamba_kernel(
    residual, w_in, w_out, conv_state, ssm_state, norm_w, conv_w, conv_b, w_x, w_dt, b_dt, a_log, d_skip,
    r_out, conv_out, ssm0, ssm1,
    res, w_raw, w_xz, wo, conv_old, wdt_pad, hid, xc_buf, z_buf, part, half_in, quart_in, own_in, o_acc,
    p_acc, p_send, p_recv, dt_buf, dx_buf, y_part, yg_buf, send_sem, recv_sem, load_sem, state_sem,
):
    layers = 2
    tokens, width = res.shape
    chunk = tokens // CHUNKS
    own = chunk // 8
    inner = wo.shape[1]
    rank = w_dt.shape[1]
    state = a_log.shape[1]
    lane_tiles = inner // 128
    ssm_bufs = (ssm0, ssm1)

    tp = lax.axis_index("tp")
    core = lax.rem(tp, 2)
    pos_x = lax.rem(lax.div(tp, 2), 2)
    pos_y = lax.div(tp, 4)
    bit_a = pos_x * (1 - core) + pos_y * core
    bit_b = pos_y * (1 - core) + pos_x * core
    peer_c = tp + 1 - 2 * core
    peer_a = tp + (1 - 2 * bit_a) * (2 + 2 * core)
    peer_b = tp + (1 - 2 * bit_b) * (4 - 2 * core)

    def rows_of(q):
        return pl.ds(pl.multiple_of(q * chunk, chunk), chunk)

    half_base = core * (4 * own)
    quart_base = half_base + bit_a * (2 * own)
    own_base = quart_base + bit_b * own

    def part_rows(q, base, count):
        return pl.ds(pl.multiple_of(q * chunk + base, own), count)

    def remote(kind, layer, q, src, dst, peer):
        return pltpu.make_async_remote_copy(
            src_ref=src, dst_ref=dst, send_sem=send_sem.at[kind, layer, q], recv_sem=recv_sem.at[kind, layer, q],
            device_id={"tp": peer}, device_id_type=MESH,
        )

    def p_copy(step, layer, q):
        peer = (peer_c, peer_a, peer_b)[step]
        return remote(step, layer, q, p_send.at[step, rows_of(q)], p_recv.at[step, rows_of(q)], peer)

    def o_copy(step, layer, q):
        if step == 0:
            src = part.at[part_rows(q, (1 - core) * (4 * own), 4 * own)]
            return remote(3, layer, q, src, half_in.at[q], peer_c)
        if step == 1:
            src = part.at[part_rows(q, half_base + (1 - bit_a) * (2 * own), 2 * own)]
            return remote(4, layer, q, src, quart_in.at[q], peer_a)
        src = part.at[part_rows(q, quart_base + (1 - bit_b) * own, own)]
        return remote(5, layer, q, src, own_in.at[q], peer_b)

    def h_copy(step, layer, q):
        base, count, peer = ((own_base, own, peer_b), (quart_base, 2 * own, peer_a), (half_base, 4 * own, peer_c))[step]
        ref = hid.at[part_rows(q, base, count)]
        if step == 0:
            return remote(6, layer, q, ref, ref, peer)
        if step == 1:
            return remote(7, layer, q, ref, ref, peer)
        return remote(2 + 6, layer, q, ref, ref, peer)

    def w_load(layer, tile):
        return pltpu.make_async_copy(w_in.at[layer, :, tile], w_raw.at[tile], load_sem.at[tile])

    def res_load(q):
        return pltpu.make_async_copy(residual.at[rows_of(q)], res.at[rows_of(q)], load_sem.at[4 + q])

    def wo_load(layer):
        return pltpu.make_async_copy(w_out.at[layer], wo.at[layer], load_sem.at[10 + layer])

    def conv_load(layer, row):
        dst = conv_old.at[layer] if row == 0 else conv_out.at[layer, row - 1]
        return pltpu.make_async_copy(conv_state.at[layer, row], dst, load_sem.at[12 + 3 * layer + row])

    def state_load(layer, q):
        return pltpu.make_async_copy(ssm_state.at[layer, rows_of(q)], ssm_bufs[layer].at[rows_of(q)], state_sem.at[layer, q])

    for tile in range(lane_tiles):
        w_load(0, tile).start()
    for q in range(CHUNKS):
        res_load(q).start()
    for row in range(3):
        conv_load(0, row).start()

    barrier = pltpu.get_barrier_semaphore()
    for peer in (peer_c, peer_a, peer_b):
        pl.semaphore_signal(barrier, inc=1, device_id={"tp": peer}, device_id_type=MESH)

    for layer in range(layers):
        wdt_pad[layer, :rank] = w_dt[layer]
        wdt_pad[layer, rank:] = jnp.zeros((128 - rank, inner), jnp.bfloat16)

    def split_weights(layer, block):
        row = lax.broadcasted_iota(jnp.int32, (256, 256), 0)
        col = lax.broadcasted_iota(jnp.int32, (256, 256), 1)
        want = jnp.where(row < 128, 2 * row, 2 * row - 255)
        pick = jnp.where(col == want, 1.0, 0.0).astype(jnp.bfloat16)
        raw = [w_raw.at[tile].reshape(2 * width, 128)[pl.ds(pl.multiple_of(block * 256, 256), 256), :] for tile in range(lane_tiles)]
        both = jnp.dot(pick, jnp.concatenate(raw, axis=1), preferred_element_type=jnp.float32).astype(jnp.bfloat16)
        dst = pl.ds(pl.multiple_of(block * 128, 128), 128)
        w_xz[layer, dst, :inner] = both[:128]
        w_xz[layer, dst, inner:] = both[128:]

    blocks = width // 128
    for tile in range(lane_tiles):
        w_load(0, tile).wait()

    @pl.loop(0, blocks)
    def _(block):
        split_weights(0, block)

    for q in range(CHUNKS):
        state_load(0, q).start()
    wo_load(0).start()
    for tile in range(lane_tiles):
        w_load(1, tile).start()
    for row in range(3):
        conv_load(1, row).start()
    wo_load(1).start()
    for row in range(3):
        conv_load(0, row).wait()
    pl.semaphore_wait(barrier, 3)

    def stage_in(layer, q):
        rows = rows_of(q)
        if layer == 0:
            res_load(q).wait()

            @pl.loop(0, chunk // 16)
            def _(i):
                sub = pl.ds(pl.multiple_of(q * chunk + i * 16, 16), 16)
                r = res[sub, :]
                hid[sub, :] = (r * rms_scale(r, 1e-5) * norm_w[0:1, :].astype(jnp.float32)).astype(jnp.bfloat16)
        else:
            h_copy(2, layer - 1, q).wait()
        xz = jnp.dot(hid[rows, :], w_xz[layer], preferred_element_type=jnp.float32)
        x_val = xz[:, :inner].astype(jnp.bfloat16)
        z_buf[rows, :] = xz[:, inner:].astype(jnp.bfloat16)
        conv_out[layer, 2, rows, :] = x_val
        taps = conv_w[layer].astype(jnp.float32)
        pre = conv_old[layer, rows, :].astype(jnp.float32) * taps[0:1]
        pre = pre + conv_out[layer, 0, rows, :].astype(jnp.float32) * taps[1:2]
        pre = pre + conv_out[layer, 1, rows, :].astype(jnp.float32) * taps[2:3]
        pre = pre + x_val.astype(jnp.float32) * taps[3:4]
        pre = pre + conv_b[layer:layer + 1, :].astype(jnp.float32)
        xc = (pre * jax.nn.sigmoid(pre)).astype(jnp.bfloat16)
        xc_buf[rows, :] = xc
        p = jnp.dot(xc, w_x[layer], preferred_element_type=jnp.float32)
        p_acc[rows, :] = p
        p_send[0, rows, :] = p.astype(jnp.bfloat16)
        p_copy(0, layer, q).start()

    def stage_p(step, layer, q):
        rows = rows_of(q)
        p_copy(step - 1, layer, q).wait()
        p = p_acc[rows, :] + p_recv[step - 1, rows, :].astype(jnp.float32)
        p_acc[rows, :] = p
        p_send[step, rows, :] = p.astype(jnp.bfloat16)
        p_copy(step, layer, q).start()

    def stage_ssm(layer, q):
        rows = rows_of(q)
        state_buf = ssm_bufs[layer]
        p_copy(2, layer, q).wait()
        p = p_acc[rows, :] + p_recv[2, rows, :].astype(jnp.float32)
        lane = lax.broadcasted_iota(jnp.int32, p.shape, 1)
        square = p * p
        is_dt = lane < rank
        is_b = jnp.logical_and(lane >= rank, lane < rank + state)

        def scale_of(mask, count):
            total = jnp.sum(jnp.where(mask, square, 0.0), axis=1, keepdims=True)
            return lax.rsqrt(total * (1.0 / count) + 1e-6)

        scale_dt = scale_of(is_dt, rank)
        scale_b = scale_of(is_b, state)
        scale_c = scale_of(lane >= rank + state, state)
        normed = p * jnp.where(is_dt, scale_dt, jnp.where(is_b, scale_b, scale_c))
        dt_low = jnp.where(is_dt, normed, 0.0).astype(jnp.bfloat16)
        pre = jnp.dot(dt_low, wdt_pad[layer], preferred_element_type=jnp.float32) + b_dt[layer:layer + 1, :]
        dt = jnp.maximum(pre, 0.0) + jnp.log1p(jnp.exp(-jnp.abs(pre)))
        dt_buf[...] = dt
        dx_buf[...] = dt * xc_buf[rows, :].astype(jnp.float32)
        turned = normed.T
        b_cols = turned[rank:rank + state, :]
        c_cols = turned[rank + state:, :]
        decay_rate = jnp.exp(a_log[layer]) * (-LOG2E)
        state_load(layer, q).wait()
        group = 8

        def scan_group(g, carry):
            b_now, c_now = carry
            for j in range(group):
                token = g * group + j
                dt_row = dt_buf[pl.ds(token, 1), :]
                dx_row = dx_buf[pl.ds(token, 1), :]
                old = state_buf[q * chunk + token]
                new = jnp.exp2(dt_row * decay_rate) * old + dx_row * b_now[:, j:j + 1]
                state_buf[q * chunk + token] = new
                weighted = new * c_now[:, j:j + 1]
                partial = weighted[:8] + weighted[8:]
                for tile in range(lane_tiles):
                    y_part[tile, pl.ds(pl.multiple_of(token * 8, 8), 8), :] = partial[:, tile * 128:(tile + 1) * 128]
            return pltpu.roll(b_now, chunk - group, 1), pltpu.roll(c_now, chunk - group, 1)

        lax.fori_loop(0, chunk // group, scan_group, (b_cols, c_cols))

        @pl.loop(0, chunk // 16)
        def _(g):
            ys = []
            for k in range(2):
                first = g * 128 + k * 64
                by_tile = []
                for tile in range(lane_tiles):
                    total = y_part[tile, pl.ds(first, 8, stride=8), :]
                    for sub in range(1, 8):
                        total = total + y_part[tile, pl.ds(first + sub, 8, stride=8), :]
                    by_tile.append(total)
                ys.append(jnp.concatenate(by_tile, axis=1))
            sub_rows = pl.ds(pl.multiple_of(q * chunk + g * 16, 16), 16)
            y = jnp.concatenate(ys, axis=0) + d_skip[layer:layer + 1, :] * xc_buf[sub_rows, :].astype(jnp.float32)
            z = z_buf[sub_rows, :].astype(jnp.float32)
            yg_buf[pl.ds(pl.multiple_of(g * 16, 16), 16), :] = (y * (z * jax.nn.sigmoid(z))).astype(jnp.bfloat16)

        part[rows, :] = jnp.dot(yg_buf[...], wo[layer], preferred_element_type=jnp.float32).astype(jnp.bfloat16)
        o_copy(0, layer, q).start()

    def stage_sum_half(layer, q):
        o_copy(0, layer, q).wait()
        mine = part_rows(q, half_base, 4 * own)
        part[mine, :] = (part[mine, :].astype(jnp.float32) + half_in[q].astype(jnp.float32)).astype(jnp.bfloat16)
        o_copy(1, layer, q).start()

    def stage_sum_quart(layer, q):
        o_copy(1, layer, q).wait()
        mine = part_rows(q, quart_base, 2 * own)
        part[mine, :] = (part[mine, :].astype(jnp.float32) + quart_in[q].astype(jnp.float32)).astype(jnp.bfloat16)
        o_copy(2, layer, q).start()

    def stage_own(layer, q):
        o_copy(2, layer, q).wait()
        mine = part_rows(q, own_base, own)
        o_val = part[mine, :].astype(jnp.float32) + own_in[q].astype(jnp.float32)
        if layer == 0:
            o_acc[q] = o_val
            r = res[mine, :] + o_val
            hid[mine, :] = (r * rms_scale(r, 1e-5) * norm_w[1:2, :].astype(jnp.float32)).astype(jnp.bfloat16)
        else:
            hid[mine, :] = (o_acc[q] + o_val).astype(jnp.bfloat16)
        h_copy(0, layer, q).start()

    def stage_gather(step, layer, q):
        h_copy(step - 1, layer, q).wait()
        h_copy(step, layer, q).start()

    def stage_out(q):
        h_copy(2, layers - 1, q).wait()
        rows = rows_of(q)
        r_out[rows, :] = res[rows, :] + hid[rows, :].astype(jnp.float32)

    stages = []
    for layer in range(layers):
        stages.append(functools.partial(stage_in, layer))
        stages.append(functools.partial(stage_p, 1, layer))
        stages.append(functools.partial(stage_p, 2, layer))
        stages.append(functools.partial(stage_ssm, layer))
        stages.append(functools.partial(stage_sum_half, layer))
        stages.append(functools.partial(stage_sum_quart, layer))
        stages.append(functools.partial(stage_own, layer))
        stages.append(functools.partial(stage_gather, 1, layer))
        stages.append(functools.partial(stage_gather, 2, layer))
    stages.append(stage_out)

    def late_loads(tick):
        @pl.when(tick == 3)
        def _():
            wo_load(0).wait()

        @pl.when(tick == 4)
        def _():
            for tile in range(lane_tiles):
                w_load(1, tile).wait()
            for row in range(3):
                conv_load(1, row).wait()
            wo_load(1).wait()
            for q in range(CHUNKS):
                state_load(1, q).start()

        @pl.when(jnp.logical_and(tick >= 5, tick < 9))
        def _():
            for i in range(blocks // 4):
                split_weights(1, (tick - 5) * (blocks // 4) + i)

    @pl.loop(0, len(stages) + CHUNKS - 1)
    def _(tick):
        late_loads(tick)
        for index in reversed(range(len(stages))):
            q = tick - index

            @pl.when(jnp.logical_and(q >= 0, q < CHUNKS))
            def _():
                stages[index](q)


def dump_kernel(r_val, conv_val, ssm0, ssm1, r_hbm, conv_hbm, ssm_hbm, sems):
    copies = [
        pltpu.make_async_copy(ssm0, ssm_hbm.at[0], sems.at[0]),
        pltpu.make_async_copy(ssm1, ssm_hbm.at[1], sems.at[1]),
        pltpu.make_async_copy(conv_val, conv_hbm, sems.at[2]),
        pltpu.make_async_copy(r_val, r_hbm, sems.at[3]),
    ]
    for copy in copies:
        copy.start()
    for copy in copies:
        copy.wait()


def solution(mesh):
    def device_step(residual, norm_w, w_in, conv_w, conv_b, w_x, w_dt, b_dt, a_log, d_skip, w_out, conv_state, ssm_state):
        tokens, width = residual.shape
        inner = w_out.shape[1]
        state = a_log.shape[1]
        lane_tiles = inner // 128
        chunk = tokens // CHUNKS
        own = chunk // 8
        w_view = w_in.reshape(2, width, 2, lane_tiles, 128).transpose(0, 1, 3, 2, 4)
        conv_view = conv_state.transpose(0, 2, 1, 3)
        vmem = pl.BlockSpec(memory_space=pltpu.VMEM)
        anywhere = pl.BlockSpec(memory_space=pl.ANY)
        hbm = pl.BlockSpec(memory_space=pltpu.HBM)
        f32, bf16 = jnp.float32, jnp.bfloat16
        r_val, conv_val, s0, s1 = pl.pallas_call(
            mamba_kernel,
            name="mamba",
            out_shape=[
                pltpu.VMEM((tokens, width), f32),
                pltpu.VMEM((2, 3, tokens, inner), bf16),
                pltpu.VMEM((tokens, state, inner), f32),
                pltpu.VMEM((tokens, state, inner), f32),
            ],
            in_specs=[hbm] * 5 + [vmem] * 8,
            out_specs=[vmem] * 4,
            scratch_shapes=[
                pltpu.VMEM((tokens, width), f32),
                pltpu.VMEM((lane_tiles, width, 2, 128), bf16),
                pltpu.VMEM((2, width, 2 * inner), bf16),
                pltpu.VMEM((2, inner, width), bf16),
                pltpu.VMEM((2, tokens, inner), bf16),
                pltpu.VMEM((2, 128, inner), bf16),
                pltpu.VMEM((tokens, width), bf16),
                pltpu.VMEM((tokens, inner), bf16),
                pltpu.VMEM((tokens, inner), bf16),
                pltpu.VMEM((tokens, width), bf16),
                pltpu.VMEM((CHUNKS, 4 * own, width), bf16),
                pltpu.VMEM((CHUNKS, 2 * own, width), bf16),
                pltpu.VMEM((CHUNKS, own, width), bf16),
                pltpu.VMEM((CHUNKS, own, width), f32),
                pltpu.VMEM((tokens, 128), f32),
                pltpu.VMEM((3, tokens, 128), bf16),
                pltpu.VMEM((3, tokens, 128), bf16),
                pltpu.VMEM((chunk, inner), f32),
                pltpu.VMEM((chunk, inner), f32),
                pltpu.VMEM((lane_tiles, chunk * 8, 128), f32),
                pltpu.VMEM((chunk, inner), bf16),
                pltpu.SemaphoreType.DMA((COPIES + 1, 2, CHUNKS)),
                pltpu.SemaphoreType.DMA((COPIES + 1, 2, CHUNKS)),
                pltpu.SemaphoreType.DMA((20,)),
                pltpu.SemaphoreType.DMA((2, CHUNKS)),
            ],
            compiler_params=pltpu.CompilerParams(collective_id=0, has_side_effects=True, vmem_limit_bytes=30 * 2**20),
        )(residual, w_view, w_out, conv_view, ssm_state, norm_w, conv_w, conv_b, w_x, w_dt, b_dt, a_log, d_skip)
        r_new, conv_new, ssm_new = pl.pallas_call(
            dump_kernel,
            name="dump",
            out_shape=[
                jax.ShapeDtypeStruct((tokens, width), f32),
                jax.ShapeDtypeStruct((2, 3, tokens, inner), bf16),
                jax.ShapeDtypeStruct(ssm_state.shape, f32),
            ],
            in_specs=[anywhere] * 4,
            out_specs=[hbm] * 3,
            scratch_shapes=[pltpu.SemaphoreType.DMA((4,))],
            compiler_params=pltpu.CompilerParams(vmem_limit_bytes=2**20),
        )(r_val, conv_val, s0, s1)
        return r_new, conv_new.transpose(0, 2, 1, 3), ssm_new

    cache_spec = P(None, 'dp', None, 'tp')
    in_specs = (P('dp', None), P(None, None), P(None, None, None, 'tp'), P(None, None, 'tp'), P(None, 'tp'), P(None, 'tp', None), P(None, None, 'tp'), P(None, 'tp'), P(None, None, 'tp'), P(None, 'tp'), P(None, 'tp', None), cache_spec, cache_spec)
    out_specs = (P('dp', None), cache_spec, cache_spec)
    return jax.shard_map(device_step, mesh=mesh, in_specs=in_specs, out_specs=out_specs, check_vma=False)
```

```python
import functools

import jax
import jax.numpy as jnp
from jax import lax
from jax.experimental import pallas as pl
from jax.experimental.pallas import tpu as pltpu
from jax.sharding import PartitionSpec as P

MESH = pl.DeviceIdType.MESH
LOG2E = 1.4426950408889634
CHUNKS = 4
KINDS = 8
ORDER = (0, 3, 2, 0, 1, 4, 4, 4, 4, 1, 2, 3, 0, 1, 0, 2, 1, 2, 3, 0, 3, 1, 2, 0, 0, 3, 0, 1, 1, 2, 1, 2, 3, 2, 3, 0, 3, 1, 0, 2, 1, 2, 3, 0, 3, 2, 1, 0, 3, 2, 1, 3, 1, 0, 2, 3)

GROUP = 16
ORDER_FIRST = tuple(dict.fromkeys(q for q in ORDER if q < CHUNKS))


def rms_scale(vector, epsilon):
    return lax.rsqrt(jnp.mean(vector * vector, axis=-1, keepdims=True) + epsilon)


def mamba_kernel(
    residual, w_in, w_out, conv_state, ssm_state, norm_w_hbm, conv_w_hbm, conv_b_hbm, w_x_hbm, w_dt_hbm, b_dt_hbm, a_log_hbm, d_skip_hbm,
    r_out, conv_out, ssm0, ssm1,
    res, w_raw, w_xz, wo, conv_old, norm_w, conv_w, conv_b, w_x, w_dt, b_dt, a_log, d_skip, hid, xc_buf, z_buf, part, half_in, half_in2, o_acc,
    p_acc, p_send, p_recv, dt_buf, dx_buf, y_part, yg_buf, send_sem, recv_sem, load_sem, small_sem, state_sem,
):
    layers = 2
    tokens, width = res.shape
    chunk = tokens // CHUNKS
    half = chunk // 2
    inner = wo.shape[1]
    rank = w_dt_hbm.shape[1]
    state = a_log.shape[1]
    lane_tiles = inner // 128
    ssm_bufs = (ssm0, ssm1)

    tp = lax.axis_index("tp")
    core = lax.rem(tp, 2)
    pos_x = lax.rem(lax.div(tp, 2), 2)
    pos_y = lax.div(tp, 4)
    bit_a = pos_x * (1 - core) + pos_y * core
    bit_b = pos_y * (1 - core) + pos_x * core
    peer_c = tp + 1 - 2 * core
    peer_a = tp + (1 - 2 * bit_a) * (2 + 2 * core)
    peer_b = tp + (1 - 2 * bit_b) * (4 - 2 * core)
    peer_d = tp + (1 - 2 * pos_x) * 2 + (1 - 2 * pos_y) * 4
    peers = (peer_c, peer_a, peer_b, peer_d)

    barrier = pltpu.get_barrier_semaphore()
    for peer in peers:
        pl.semaphore_signal(barrier, inc=1, device_id={"tp": peer}, device_id_type=MESH)

    def rows_of(q):
        return pl.ds(q * chunk, chunk)

    def half_rows(q, which):
        return pl.ds(pl.multiple_of(q * chunk + which * half, half), half)

    def remote(kind, layer, q, src, dst, peer):
        return pltpu.make_async_remote_copy(
            src_ref=src, dst_ref=dst, send_sem=send_sem.at[kind, layer, q], recv_sem=recv_sem.at[kind, layer, q],
            device_id={"tp": peer}, device_id_type=MESH,
        )

    def p_copy(step, layer, q):
        src = p_send.at[min(step, 1), rows_of(q)]
        return remote(step, layer, q, src, p_recv.at[step, rows_of(q)], peers[step])

    def o_copy(step, layer, q):
        if step == 0:
            return remote(4, layer, q, part.at[half_rows(q, 1 - core)], half_in.at[0, q], peer_c)
        return remote(4 + step, layer, q, half_in2.at[step - 1, q], half_in.at[step, q], peers[step])

    def h_copy(layer, q):
        ref = hid.at[half_rows(q, core)]
        return remote(7, layer, q, ref, ref, peer_c)

    def w_load(layer, tile):
        return pltpu.make_async_copy(w_in.at[layer, :, tile], w_raw.at[layer, tile], load_sem.at[layer * lane_tiles + tile])

    def res_load(q):
        return pltpu.make_async_copy(residual.at[rows_of(q)], res.at[rows_of(q)], load_sem.at[6 + q])

    def wo_load(layer):
        return pltpu.make_async_copy(w_out.at[layer], wo.at[layer], load_sem.at[10 + layer])

    def conv_load(layer, row):
        dst = conv_old.at[layer] if row == 0 else conv_out.at[layer, row - 1]
        return pltpu.make_async_copy(conv_state.at[layer, row], dst, load_sem.at[12 + 3 * layer + row])

    def state_load(layer, q):
        return pltpu.make_async_copy(ssm_state.at[layer, rows_of(q)], ssm_bufs[layer].at[rows_of(q)], state_sem.at[layer, q])

    small = [
        pltpu.make_async_copy(norm_w_hbm, norm_w, small_sem.at[0]),
        pltpu.make_async_copy(conv_w_hbm, conv_w, small_sem.at[1]),
        pltpu.make_async_copy(conv_b_hbm, conv_b, small_sem.at[2]),
        pltpu.make_async_copy(w_x_hbm, w_x, small_sem.at[3]),
        pltpu.make_async_copy(w_dt_hbm, w_dt.at[:, pl.ds(0, rank)], small_sem.at[4]),
        pltpu.make_async_copy(b_dt_hbm, b_dt, small_sem.at[5]),
        pltpu.make_async_copy(a_log_hbm, a_log, small_sem.at[6]),
        pltpu.make_async_copy(d_skip_hbm, d_skip, small_sem.at[7]),
    ]
    small[0].start()
    res_load(ORDER[0]).start()
    for tile in range(lane_tiles):
        w_load(0, tile).start()
    for q in range(CHUNKS):
        if q != ORDER[0]:
            res_load(q).start()
    for row in range(3):
        conv_load(0, row).start()
    for copy in small[1:]:
        copy.start()
    for layer in range(layers):
        w_dt[layer, rank:] = jnp.zeros((128 - rank, inner), jnp.bfloat16)

    def split_weights(layer, first, count):
        row = lax.broadcasted_iota(jnp.int32, (256, 256), 0)
        col = lax.broadcasted_iota(jnp.int32, (256, 256), 1)
        want = jnp.where(row < 128, 2 * row, 2 * row - 255)
        pick = jnp.where(col == want, 1.0, 0.0).astype(jnp.bfloat16)
        for i in range(count):
            src = pl.ds(pl.multiple_of((first + i) * 256, 256), 256)
            raw = [w_raw.at[layer, tile].reshape(2 * width, 128)[src, :] for tile in range(lane_tiles)]
            both = jnp.dot(pick, jnp.concatenate(raw, axis=1), preferred_element_type=jnp.float32).astype(jnp.bfloat16)
            dst = pl.ds(pl.multiple_of((first + i) * 128, 128), 128)
            w_xz[layer, dst, :inner] = both[:128]
            w_xz[layer, dst, inner:] = both[128:]

    blocks = width // 128
    split_step = 3

    def first_norm(q):
        res_load(q).wait()

        @pl.loop(0, chunk // 32)
        def _(i):
            sub = pl.ds(pl.multiple_of(q * chunk + i * 32, 32), 32)
            r = res[sub, :]
            hid[sub, :] = (r * rms_scale(r, 1e-5) * norm_w[0:1, :].astype(jnp.float32)).astype(jnp.bfloat16)

    small[0].wait()
    first_norm(ORDER[0])
    for tile in range(lane_tiles):
        w_load(0, tile).wait()

    @pl.loop(0, blocks // split_step)
    def _(step):
        split_weights(0, step * split_step, split_step)

    for tile in range(lane_tiles):
        w_load(1, tile).start()
    for q in ORDER_FIRST:
        state_load(0, q).start()
    wo_load(0).start()
    for row in range(3):
        conv_load(0, row).wait()
    for copy in small[1:]:
        copy.wait()
    pl.semaphore_wait(barrier, 4)

    def stage_in(layer, q):
        rows = rows_of(q)
        if layer == 0:
            if q != ORDER[0]:
                first_norm(q)
        else:
            h_copy(layer - 1, q).wait()
        xz = jnp.dot(hid[rows, :], w_xz[layer], preferred_element_type=jnp.float32)
        x_val = xz[:, :inner].astype(jnp.bfloat16)
        z_buf[rows, :] = xz[:, inner:].astype(jnp.bfloat16)
        conv_out[layer, 2, rows, :] = x_val
        taps = conv_w[layer].astype(jnp.float32)
        pre = conv_old[layer, rows, :].astype(jnp.float32) * taps[0:1]
        pre = pre + conv_out[layer, 0, rows, :].astype(jnp.float32) * taps[1:2]
        pre = pre + conv_out[layer, 1, rows, :].astype(jnp.float32) * taps[2:3]
        pre = pre + x_val.astype(jnp.float32) * taps[3:4]
        pre = pre + conv_b[layer:layer + 1, :].astype(jnp.float32)
        xc = (pre * jax.nn.sigmoid(pre)).astype(jnp.bfloat16)
        xc_buf[rows, :] = xc
        p = jnp.dot(xc, w_x[layer], preferred_element_type=jnp.float32)
        p_acc[rows, :] = p
        p_send[0, rows, :] = p.astype(jnp.bfloat16)
        p_copy(0, layer, q).start()

    def stage_p(layer, q):
        rows = rows_of(q)
        p_copy(0, layer, q).wait()
        p = p_acc[rows, :] + p_recv[0, rows, :].astype(jnp.float32)
        p_acc[rows, :] = p
        p_send[1, rows, :] = p.astype(jnp.bfloat16)
        for step in (3, 1, 2):
            p_copy(step, layer, q).start()

    def stage_ssm(layer, q):
        rows = rows_of(q)
        state_buf = ssm_bufs[layer]
        p = p_acc[rows, :]
        for step in (1, 2, 3):
            p_copy(step, layer, q).wait()
            p = p + p_recv[step, rows, :].astype(jnp.float32)
        lane = lax.broadcasted_iota(jnp.int32, p.shape, 1)
        square = p * p
        is_dt = lane < rank
        is_b = jnp.logical_and(lane >= rank, lane < rank + state)

        def scale_of(mask, count):
            total = jnp.sum(jnp.where(mask, square, 0.0), axis=1, keepdims=True)
            return lax.rsqrt(total * (1.0 / count) + 1e-6)

        scale_dt = scale_of(is_dt, rank)
        scale_b = scale_of(is_b, state)
        scale_c = scale_of(lane >= rank + state, state)
        normed = p * jnp.where(is_dt, scale_dt, jnp.where(is_b, scale_b, scale_c))
        dt_low = jnp.where(is_dt, normed, 0.0).astype(jnp.bfloat16)
        pre = jnp.dot(dt_low, w_dt[layer], preferred_element_type=jnp.float32) + b_dt[layer:layer + 1, :]
        dt = jnp.maximum(pre, 0.0) + jnp.log1p(jnp.exp(-jnp.abs(pre)))
        dt_buf[...] = dt
        dx_buf[...] = dt * xc_buf[rows, :].astype(jnp.float32)
        turned = normed.T
        b_cols = turned[rank:rank + state, :]
        c_cols = turned[rank + state:, :]
        decay_rate = jnp.exp(a_log[layer]) * (-LOG2E)
        state_load(layer, q).wait()

        def scan_group(g, carry):
            b_now, c_now = carry
            for j in range(GROUP):
                token = g * GROUP + j
                dt_row = dt_buf[pl.ds(token, 1), :]
                dx_row = dx_buf[pl.ds(token, 1), :]
                old = state_buf[q * chunk + token]
                new = jnp.exp2(dt_row * decay_rate) * old + dx_row * b_now[:, j:j + 1]
                state_buf[q * chunk + token] = new
                weighted = new * c_now[:, j:j + 1]
                partial = weighted[:8] + weighted[8:]
                for tile in range(lane_tiles):
                    y_part[tile, pl.ds(pl.multiple_of(token * 8, 8), 8), :] = partial[:, tile * 128:(tile + 1) * 128]
            return pltpu.roll(b_now, chunk - GROUP, 1), pltpu.roll(c_now, chunk - GROUP, 1)

        lax.fori_loop(0, chunk // GROUP, scan_group, (b_cols, c_cols))

        @pl.loop(0, chunk // 32)
        def _(g):
            for k in range(4):
                first = g * 256 + k * 64
                by_tile = []
                for tile in range(lane_tiles):
                    terms = [y_part[tile, pl.ds(first + sub, 8, stride=8), :] for sub in range(8)]
                    while len(terms) > 1:
                        terms = [terms[i] + terms[i + 1] for i in range(0, len(terms), 2)]
                    by_tile.append(terms[0])
                y_buf_rows = pl.ds(pl.multiple_of(g * 32 + k * 8, 8), 8)
                dt_buf[y_buf_rows, :] = jnp.concatenate(by_tile, axis=1)
            sub = pl.ds(pl.multiple_of(g * 32, 32), 32)
            sub_rows = pl.ds(pl.multiple_of(q * chunk + g * 32, 32), 32)
            y = dt_buf[sub, :] + d_skip[layer:layer + 1, :] * xc_buf[sub_rows, :].astype(jnp.float32)
            z = z_buf[sub_rows, :].astype(jnp.float32)
            yg_buf[sub, :] = (y * (z * jax.nn.sigmoid(z))).astype(jnp.bfloat16)

        if q == ORDER_FIRST[0]:
            wo_load(layer).wait()
        part[rows, :] = jnp.dot(yg_buf[...], wo[layer], preferred_element_type=jnp.float32).astype(jnp.bfloat16)
        o_copy(0, layer, q).start()

    def stage_o(step, layer, q):
        o_copy(step - 1, layer, q).wait()
        mine = part[half_rows(q, core), :] if step == 1 else half_in2[0, q]
        half_in2[step - 1, q] = (mine.astype(jnp.float32) + half_in[step - 1, q].astype(jnp.float32)).astype(jnp.bfloat16)
        o_copy(step, layer, q).start()

    def stage_own(layer, q):
        o_copy(2, layer, q).wait()
        mine = half_rows(q, core)

        @pl.loop(0, half // 16)
        def _(i):
            sub = pl.ds(pl.multiple_of(i * 16, 16), 16)
            dst = pl.ds(pl.multiple_of(q * chunk + core * half + i * 16, 16), 16)
            o_val = half_in2[1, q, sub, :].astype(jnp.float32) + half_in[2, q, sub, :].astype(jnp.float32)
            if layer == 0:
                o_acc[q, sub, :] = o_val
                r = res[dst, :] + o_val
                hid[dst, :] = (r * rms_scale(r, 1e-5) * norm_w[1:2, :].astype(jnp.float32)).astype(jnp.bfloat16)
            else:
                hid[dst, :] = (o_acc[q, sub, :] + o_val).astype(jnp.bfloat16)

        h_copy(layer, q).start()

    def stage_out(q):
        h_copy(layers - 1, q).wait()
        rows = rows_of(q)
        r_out[rows, :] = res[rows, :] + hid[rows, :].astype(jnp.float32)

    stages = []
    for layer in range(layers):
        stages.append(functools.partial(stage_in, layer))
        stages.append(functools.partial(stage_p, layer))
        stages.append(functools.partial(stage_ssm, layer))
        stages.append(functools.partial(stage_o, 1, layer))
        stages.append(functools.partial(stage_o, 2, layer))
        stages.append(functools.partial(stage_own, layer))
    stages.append(stage_out)

    progress = [0] * CHUNKS
    fills = 0
    for q in ORDER:
        if q == CHUNKS:
            if fills == 0:
                for tile in range(lane_tiles):
                    w_load(1, tile).wait()
                for row in range(3):
                    conv_load(1, row).start()
                wo_load(1).start()
                for chunk_index in ORDER_FIRST:
                    state_load(1, chunk_index).start()
            split_weights(1, fills * split_step, split_step)
            fills += 1
        else:
            if q == ORDER_FIRST[0] and progress[q] == 6:
                for row in range(3):
                    conv_load(1, row).wait()
            stages[progress[q]](q)
            progress[q] += 1


def dump_kernel(r_val, conv_val, ssm0, ssm1, r_hbm, conv_hbm, ssm_hbm, sems):
    copies = [
        pltpu.make_async_copy(ssm0, ssm_hbm.at[0], sems.at[0]),
        pltpu.make_async_copy(ssm1, ssm_hbm.at[1], sems.at[1]),
        pltpu.make_async_copy(conv_val, conv_hbm, sems.at[2]),
        pltpu.make_async_copy(r_val, r_hbm, sems.at[3]),
    ]
    for copy in copies:
        copy.start()
    for copy in copies:
        copy.wait()


def solution(mesh):
    def device_step(residual, norm_w, w_in, conv_w, conv_b, w_x, w_dt, b_dt, a_log, d_skip, w_out, conv_state, ssm_state):
        tokens, width = residual.shape
        inner = w_out.shape[1]
        state = a_log.shape[1]
        lane_tiles = inner // 128
        chunk = tokens // CHUNKS
        half = chunk // 2
        w_view = w_in.reshape(2, width, 2, lane_tiles, 128).transpose(0, 1, 3, 2, 4)
        conv_view = conv_state.transpose(0, 2, 1, 3)
        vmem = pl.BlockSpec(memory_space=pltpu.VMEM)
        anywhere = pl.BlockSpec(memory_space=pl.ANY)
        hbm = pl.BlockSpec(memory_space=pltpu.HBM)
        f32, bf16 = jnp.float32, jnp.bfloat16
        r_val, conv_val, s0, s1 = pl.pallas_call(
            mamba_kernel,
            name="mamba",
            out_shape=[
                pltpu.VMEM((tokens, width), f32),
                pltpu.VMEM((2, 3, tokens, inner), bf16),
                pltpu.VMEM((tokens, state, inner), f32),
                pltpu.VMEM((tokens, state, inner), f32),
            ],
            in_specs=[hbm] * 13,
            out_specs=[vmem] * 4,
            scratch_shapes=[
                pltpu.VMEM((tokens, width), f32),
                pltpu.VMEM((2, lane_tiles, width, 2, 128), bf16),
                pltpu.VMEM((2, width, 2 * inner), bf16),
                pltpu.VMEM((2, inner, width), bf16),
                pltpu.VMEM((2, tokens, inner), bf16),
                pltpu.VMEM(norm_w.shape, bf16),
                pltpu.VMEM(conv_w.shape, bf16),
                pltpu.VMEM(conv_b.shape, bf16),
                pltpu.VMEM(w_x.shape, bf16),
                pltpu.VMEM((2, 128, inner), bf16),
                pltpu.VMEM(b_dt.shape, f32),
                pltpu.VMEM(a_log.shape, f32),
                pltpu.VMEM(d_skip.shape, f32),
                pltpu.VMEM((tokens, width), bf16),
                pltpu.VMEM((tokens, inner), bf16),
                pltpu.VMEM((tokens, inner), bf16),
                pltpu.VMEM((tokens, width), bf16),
                pltpu.VMEM((3, CHUNKS, half, width), bf16),
                pltpu.VMEM((2, CHUNKS, half, width), bf16),
                pltpu.VMEM((CHUNKS, half, width), f32),
                pltpu.VMEM((tokens, 128), f32),
                pltpu.VMEM((2, tokens, 128), bf16),
                pltpu.VMEM((4, tokens, 128), bf16),
                pltpu.VMEM((chunk, inner), f32),
                pltpu.VMEM((chunk, inner), f32),
                pltpu.VMEM((lane_tiles, chunk * 8, 128), f32),
                pltpu.VMEM((chunk, inner), bf16),
                pltpu.SemaphoreType.DMA((KINDS, 2, CHUNKS)),
                pltpu.SemaphoreType.DMA((KINDS, 2, CHUNKS)),
                pltpu.SemaphoreType.DMA((18,)),
                pltpu.SemaphoreType.DMA((8,)),
                pltpu.SemaphoreType.DMA((2, CHUNKS)),
            ],
            compiler_params=pltpu.CompilerParams(collective_id=0, has_side_effects=True, vmem_limit_bytes=32 * 2**20),
        )(residual, w_view, w_out, conv_view, ssm_state, norm_w, conv_w, conv_b, w_x, w_dt, b_dt, a_log, d_skip)
        r_new, conv_new, ssm_new = pl.pallas_call(
            dump_kernel,
            name="dump",
            out_shape=[
                jax.ShapeDtypeStruct((tokens, width), f32),
                jax.ShapeDtypeStruct((2, 3, tokens, inner), bf16),
                jax.ShapeDtypeStruct(ssm_state.shape, f32),
            ],
            in_specs=[anywhere] * 4,
            out_specs=[hbm] * 3,
            scratch_shapes=[pltpu.SemaphoreType.DMA((4,))],
            compiler_params=pltpu.CompilerParams(vmem_limit_bytes=2**20),
        )(r_val, conv_val, s0, s1)
        return r_new, conv_new.transpose(0, 2, 1, 3), ssm_new

    cache_spec = P(None, 'dp', None, 'tp')
    in_specs = (P('dp', None), P(None, None), P(None, None, None, 'tp'), P(None, None, 'tp'), P(None, 'tp'), P(None, 'tp', None), P(None, None, 'tp'), P(None, 'tp'), P(None, None, 'tp'), P(None, 'tp'), P(None, 'tp', None), cache_spec, cache_spec)
    out_specs = (P('dp', None), cache_spec, cache_spec)
    return jax.shard_map(device_step, mesh=mesh, in_specs=in_specs, out_specs=out_specs, check_vma=False)
```

```python
import functools

import jax
import jax.numpy as jnp
from jax import lax
from jax.experimental.layout import Layout, with_layout_constraint
from jax.experimental import pallas as pl
from jax.experimental.pallas import tpu as pltpu
from jax.sharding import PartitionSpec as P

MESH = pl.DeviceIdType.MESH
LOG2E = 1.4426950408889634
CHUNKS = 4
KINDS = 10
ORDER = (0, 2, 1, 0, 1, 3, 4, 4, 2, 4, 3, 0, 1, 2, 0, 1, 3, 2, 3, 0, 1, 2, 3, 0, 1, 2, 0, 3, 1, 0, 1, 2, 0, 3, 1, 2, 3, 2, 3, 0, 1, 2, 0, 1, 3, 2, 3, 0, 1, 2, 3, 0, 1, 2, 3, 0, 1, 2, 1, 3, 0, 2, 3)

GROUP = 64
DUMP_PIECES = 4
ORDER_FIRST = tuple(dict.fromkeys(q for q in ORDER if q < CHUNKS))


def rms_scale(vector, epsilon):
    return lax.rsqrt(jnp.mean(vector * vector, axis=-1, keepdims=True) + epsilon)


def mamba_kernel(
    residual, w_in, w_out, conv_state, ssm_state, norm_w_hbm, conv_w_hbm, conv_b_hbm, w_x_hbm, w_dt_hbm, b_dt_hbm, a_log_hbm, d_skip_hbm,
    r_out, conv_out, ssm0, ssm1,
    res, w_raw, w_xz, wo, conv_old, norm_w, conv_w, conv_b, w_x, w_dt, b_dt, a_log, d_skip, hid, xc_buf, z_buf, part, half_in, quart_in, quart_sum, pair_in, o_acc,
    p_acc, p_send, p_recv, rate_buf, dt_buf, dx_buf, y_part, yg_buf, send_sem, recv_sem, load_sem, small_sem, state_sem,
):
    layers = 2
    tokens, width = res.shape
    chunk = tokens // CHUNKS
    half = chunk // 2
    quart = chunk // 4
    inner = wo.shape[1]
    rank = w_dt_hbm.shape[1]
    state = a_log.shape[1]
    lane_tiles = inner // 128
    ssm_bufs = (ssm0, ssm1)

    tp = lax.axis_index("tp")
    core = lax.rem(tp, 2)
    pos_x = lax.rem(lax.div(tp, 2), 2)
    pos_y = lax.div(tp, 4)
    bit_a = pos_x * (1 - core) + pos_y * core
    bit_b = pos_y * (1 - core) + pos_x * core
    peer_c = tp + 1 - 2 * core
    peer_a = tp + (1 - 2 * bit_a) * (2 + 2 * core)
    peer_b = tp + (1 - 2 * bit_b) * (4 - 2 * core)
    peer_d = tp + (1 - 2 * pos_x) * 2 + (1 - 2 * pos_y) * 4
    peers = (peer_c, peer_a, peer_b, peer_d)

    barrier = pltpu.get_barrier_semaphore()
    for peer in peers:
        pl.semaphore_signal(barrier, inc=1, device_id={"tp": peer}, device_id_type=MESH)

    def rows_of(q):
        return pl.ds(q * chunk, chunk)

    def half_rows(q, which):
        return pl.ds(pl.multiple_of(q * chunk + which * half, half), half)

    def quart_rows(q, which_half, which):
        return pl.ds(pl.multiple_of(q * chunk + which_half * half + which * quart, quart), quart)

    def remote(kind, layer, q, src, dst, peer):
        return pltpu.make_async_remote_copy(
            src_ref=src, dst_ref=dst, send_sem=send_sem.at[kind, layer, q], recv_sem=recv_sem.at[kind, layer, q],
            device_id={"tp": peer}, device_id_type=MESH,
        )

    def p_copy(step, layer, q):
        src = p_send.at[min(step, 1), rows_of(q)]
        return remote(step, layer, q, src, p_recv.at[step, rows_of(q)], peers[step])

    def o_copy(step, layer, q):
        if step == 0:
            return remote(4, layer, q, part.at[half_rows(q, 1 - core)], half_in.at[q], peer_c)
        if step == 1:
            return remote(5, layer, q, part.at[quart_rows(q, core, 1 - bit_a)], quart_in.at[q], peer_a)
        return remote(6, layer, q, quart_sum.at[q], pair_in.at[q], peer_b)

    def h_copy(step, layer, q):
        ref = hid.at[quart_rows(q, core, 1 - bit_a if step == 2 else bit_a)]
        return remote(7 + step, layer, q, ref, ref, peer_a if step == 0 else peer_c)

    def w_load(layer):
        return pltpu.make_async_copy(w_in.at[layer], w_raw.at[layer], load_sem.at[layer])

    def res_load(q):
        return pltpu.make_async_copy(residual.at[rows_of(q)], res.at[rows_of(q)], load_sem.at[18 + q])

    def wo_load(layer):
        return pltpu.make_async_copy(w_out.at[layer], wo.at[layer], load_sem.at[10 + layer])

    def conv_load(layer, row):
        dst = conv_old.at[layer] if row == 0 else conv_out.at[layer, row - 1]
        return pltpu.make_async_copy(conv_state.at[layer, row], dst, load_sem.at[12 + 3 * layer + row])

    def state_load(layer, q):
        return pltpu.make_async_copy(ssm_state.at[layer, rows_of(q)], ssm_bufs[layer].at[rows_of(q)], state_sem.at[layer, q])

    small = [
        pltpu.make_async_copy(norm_w_hbm, norm_w, small_sem.at[0]),
        pltpu.make_async_copy(conv_w_hbm, conv_w, small_sem.at[1]),
        pltpu.make_async_copy(conv_b_hbm, conv_b, small_sem.at[2]),
        pltpu.make_async_copy(w_x_hbm, w_x, small_sem.at[3]),
        pltpu.make_async_copy(w_dt_hbm, w_dt.at[:, pl.ds(0, rank)], small_sem.at[4]),
        pltpu.make_async_copy(b_dt_hbm, b_dt, small_sem.at[5]),
        pltpu.make_async_copy(a_log_hbm, a_log, small_sem.at[6]),
        pltpu.make_async_copy(d_skip_hbm, d_skip, small_sem.at[7]),
    ]
    small[0].start()
    res_load(ORDER[0]).start()
    w_load(0).start()
    for q in range(CHUNKS):
        if q != ORDER[0]:
            res_load(q).start()
    for row in range(3):
        conv_load(0, row).start()
    for copy in small[1:]:
        copy.start()
    for layer in range(layers):
        w_dt[layer, rank:] = jnp.zeros((128 - rank, inner), jnp.bfloat16)

    span = 32
    packed = span * lane_tiles * 2
    blocks = width // (2 * span)

    def split_weights(layer, first, count):
        row = lax.broadcasted_iota(jnp.int32, (packed, packed), 0)
        col = lax.broadcasted_iota(jnp.int32, (packed, packed), 1)
        group = lax.div(row, span)
        want = lax.rem(row, span) * (2 * lane_tiles) + lax.rem(group, lane_tiles) * 2 + lax.div(group, lane_tiles)
        pick = jnp.where(col == want, 1.0, 0.0).astype(jnp.bfloat16)

        @pl.loop(0, count // 4)
        def _(step):
            for i in range(4):
                block = first + step * 4 + i
                raw = [w_raw[layer, pl.ds(pl.multiple_of((2 * block + k) * packed, packed), packed), :] for k in range(2)]
                both = jnp.dot(pick, jnp.concatenate(raw, axis=1), preferred_element_type=jnp.float32).astype(jnp.bfloat16)
                for k in range(2):
                    dst = pl.ds(pl.multiple_of((2 * block + k) * span, span), span)
                    for tile in range(2 * lane_tiles):
                        w_xz[layer, dst, tile * 128:(tile + 1) * 128] = both[tile * span:(tile + 1) * span, k * 128:(k + 1) * 128]

    split_step = 8

    def first_norm(q):
        res_load(q).wait()

        @pl.loop(0, chunk // 32)
        def _(i):
            sub = pl.ds(pl.multiple_of(q * chunk + i * 32, 32), 32)
            r = res[sub, :]
            hid[sub, :] = (r * rms_scale(r, 1e-5) * norm_w[0:1, :].astype(jnp.float32)).astype(jnp.bfloat16)

    small[0].wait()
    first_norm(ORDER[0])
    w_load(0).wait()

    split_weights(0, 0, blocks)

    w_load(1).start()
    for q in ORDER_FIRST:
        state_load(0, q).start()
    wo_load(0).start()
    for row in range(3):
        conv_load(0, row).wait()
    for copy in small[1:]:
        copy.wait()
    pl.semaphore_wait(barrier, 4)

    wo_ready = [False] * layers

    def stage_in(layer, q):
        rows = rows_of(q)
        if layer == 0:
            if q != ORDER[0]:
                first_norm(q)
        else:
            h_copy(1, layer - 1, q).wait()
            h_copy(2, layer - 1, q).wait()
        xz = jnp.dot(hid[rows, :], w_xz[layer], preferred_element_type=jnp.float32)
        x_val = xz[:, :inner].astype(jnp.bfloat16)
        z_buf[rows, :] = xz[:, inner:].astype(jnp.bfloat16)
        conv_out[layer, 2, rows, :] = x_val
        taps = conv_w[layer].astype(jnp.float32)
        pre = conv_old[layer, rows, :].astype(jnp.float32) * taps[0:1]
        pre = pre + conv_out[layer, 0, rows, :].astype(jnp.float32) * taps[1:2]
        pre = pre + conv_out[layer, 1, rows, :].astype(jnp.float32) * taps[2:3]
        pre = pre + x_val.astype(jnp.float32) * taps[3:4]
        pre = pre + conv_b[layer:layer + 1, :].astype(jnp.float32)
        xc = (pre * jax.nn.sigmoid(pre)).astype(jnp.bfloat16)
        xc_buf[rows, :] = xc
        p = jnp.dot(xc, w_x[layer], preferred_element_type=jnp.float32)
        p_acc[rows, :] = p
        p_send[0, rows, :] = p.astype(jnp.bfloat16)
        p_copy(0, layer, q).start()

    def stage_p(layer, q):
        rows = rows_of(q)
        p_copy(0, layer, q).wait()
        p = p_acc[rows, :] + p_recv[0, rows, :].astype(jnp.float32)
        p_acc[rows, :] = p
        p_send[1, rows, :] = p.astype(jnp.bfloat16)
        for step in (3, 1, 2):
            p_copy(step, layer, q).start()

    def stage_ssm(layer, q):
        rows = rows_of(q)
        state_buf = ssm_bufs[layer]
        p = p_acc[rows, :]
        for step in (1, 2, 3):
            p_copy(step, layer, q).wait()
            p = p + p_recv[step, rows, :].astype(jnp.float32)
        lane = lax.broadcasted_iota(jnp.int32, p.shape, 1)
        square = p * p
        is_dt = lane < rank
        is_b = jnp.logical_and(lane >= rank, lane < rank + state)

        def scale_of(mask, count):
            total = jnp.sum(jnp.where(mask, square, 0.0), axis=1, keepdims=True)
            return lax.rsqrt(total * (1.0 / count) + 1e-6)

        scale_dt = scale_of(is_dt, rank)
        scale_b = scale_of(is_b, state)
        scale_c = scale_of(lane >= rank + state, state)
        normed = p * jnp.where(is_dt, scale_dt, jnp.where(is_b, scale_b, scale_c))
        dt_low = jnp.where(is_dt, normed, 0.0).astype(jnp.bfloat16)
        pre = jnp.dot(dt_low, w_dt[layer], preferred_element_type=jnp.float32) + b_dt[layer:layer + 1, :]
        dt = jnp.maximum(pre, 0.0) + jnp.log1p(jnp.exp(-jnp.abs(pre)))
        dt_buf[...] = dt
        dx_buf[...] = dt * xc_buf[rows, :].astype(jnp.float32)
        turned = jnp.concatenate([normed] * (128 // chunk), axis=0).T
        b_cols = turned[rank:rank + state, :]
        c_cols = turned[rank + state:, :]
        rate_buf[...] = jnp.exp(a_log[layer]) * (-LOG2E)
        state_load(layer, q).wait()

        def scan_group(g, carry):
            b_now, c_now = carry
            for j in range(GROUP):
                token = g * GROUP + j
                dt_row = dt_buf[pl.ds(token, 1), :]
                dx_row = dx_buf[pl.ds(token, 1), :]
                old = state_buf[q * chunk + token]
                new = jnp.exp2(dt_row * rate_buf[...]) * old + dx_row * b_now[:, j:j + 1]
                state_buf[q * chunk + token] = new
                weighted = new * c_now[:, j:j + 1]
                partial = weighted[:8] + weighted[8:]
                for tile in range(lane_tiles):
                    y_part[tile, pl.ds(pl.multiple_of(token * 8, 8), 8), :] = partial[:, tile * 128:(tile + 1) * 128]
            return pltpu.roll(b_now, 128 - GROUP, 1), pltpu.roll(c_now, 128 - GROUP, 1)

        lax.fori_loop(0, chunk // GROUP, scan_group, (b_cols, c_cols))

        @pl.loop(0, chunk // 32)
        def _(g):
            for k in range(4):
                first = g * 256 + k * 64
                by_tile = []
                for tile in range(lane_tiles):
                    terms = [y_part[tile, pl.ds(first + sub, 8, stride=8), :] for sub in range(8)]
                    while len(terms) > 1:
                        terms = [terms[i] + terms[i + 1] for i in range(0, len(terms), 2)]
                    by_tile.append(terms[0])
                y_buf_rows = pl.ds(pl.multiple_of(g * 32 + k * 8, 8), 8)
                dt_buf[y_buf_rows, :] = jnp.concatenate(by_tile, axis=1)
            sub = pl.ds(pl.multiple_of(g * 32, 32), 32)
            sub_rows = pl.ds(pl.multiple_of(q * chunk + g * 32, 32), 32)
            y = dt_buf[sub, :] + d_skip[layer:layer + 1, :] * xc_buf[sub_rows, :].astype(jnp.float32)
            z = z_buf[sub_rows, :].astype(jnp.float32)
            yg_buf[sub, :] = (y * (z * jax.nn.sigmoid(z))).astype(jnp.bfloat16)

        if not wo_ready[layer]:
            wo_load(layer).wait()
            wo_ready[layer] = True
        part[rows, :] = jnp.dot(yg_buf[...], wo[layer], preferred_element_type=jnp.float32).astype(jnp.bfloat16)
        o_copy(0, layer, q).start()

    def stage_half(layer, q):
        o_copy(0, layer, q).wait()
        mine = half_rows(q, core)
        part[mine, :] = (part[mine, :].astype(jnp.float32) + half_in[q].astype(jnp.float32)).astype(jnp.bfloat16)
        o_copy(1, layer, q).start()

    def stage_quart(layer, q):
        o_copy(1, layer, q).wait()
        mine = part[quart_rows(q, core, bit_a), :]
        quart_sum[q] = (mine.astype(jnp.float32) + quart_in[q].astype(jnp.float32)).astype(jnp.bfloat16)
        o_copy(2, layer, q).start()

    def stage_own(layer, q):
        o_copy(2, layer, q).wait()
        for i in range(quart // 16):
            sub = pl.ds(i * 16, 16)
            dst = pl.ds(pl.multiple_of(q * chunk + core * half + bit_a * quart + i * 16, 16), 16)
            o_val = quart_sum[q, sub, :].astype(jnp.float32) + pair_in[q, sub, :].astype(jnp.float32)
            if layer == 0:
                o_acc[q, sub, :] = o_val
                r = res[dst, :] + o_val
                hid[dst, :] = (r * rms_scale(r, 1e-5) * norm_w[1:2, :].astype(jnp.float32)).astype(jnp.bfloat16)
            else:
                hid[dst, :] = (o_acc[q, sub, :] + o_val).astype(jnp.bfloat16)
        h_copy(0, layer, q).start()
        h_copy(1, layer, q).start()

    def stage_forward(layer, q):
        h_copy(0, layer, q).wait()
        h_copy(2, layer, q).start()

    def stage_out(q):
        h_copy(1, layers - 1, q).wait()
        h_copy(2, layers - 1, q).wait()
        rows = rows_of(q)
        r_out[rows, :] = res[rows, :] + hid[rows, :].astype(jnp.float32)

    stages = []
    for layer in range(layers):
        stages.append(functools.partial(stage_in, layer))
        stages.append(functools.partial(stage_p, layer))
        stages.append(functools.partial(stage_ssm, layer))
        stages.append(functools.partial(stage_half, layer))
        stages.append(functools.partial(stage_quart, layer))
        stages.append(functools.partial(stage_own, layer))
        stages.append(functools.partial(stage_forward, layer))
    stages.append(stage_out)

    per_layer = len(stages) // layers
    progress = [0] * CHUNKS
    second_ready = False
    fills = 0
    for q in ORDER:
        if q == CHUNKS:
            if fills == 0:
                w_load(1).wait()
                for row in range(3):
                    conv_load(1, row).start()
                wo_load(1).start()
                for chunk_index in ORDER_FIRST:
                    state_load(1, chunk_index).start()
            split_weights(1, fills * split_step, split_step)
            fills += 1
        else:
            if progress[q] == per_layer and not second_ready:
                for row in range(3):
                    conv_load(1, row).wait()
                second_ready = True
            stages[progress[q]](q)
            progress[q] += 1


def dump_kernel(r_val, conv_val, ssm0, ssm1, r_hbm, conv_hbm, ssm_hbm, sems):
    copies = [pltpu.make_async_copy(r_val, r_hbm, sems.at[0]), pltpu.make_async_copy(conv_val, conv_hbm, sems.at[1])]
    piece = ssm0.shape[0] // DUMP_PIECES
    for i in range(DUMP_PIECES):
        for layer, ssm in enumerate((ssm0, ssm1)):
            rows = pl.ds(i * piece, piece)
            copies.append(pltpu.make_async_copy(ssm.at[rows], ssm_hbm.at[layer, rows], sems.at[2 + 2 * i + layer]))
    for copy in copies:
        copy.start()
    for copy in copies:
        copy.wait()


def solution(mesh):
    def device_step(residual, norm_w, w_in, conv_w, conv_b, w_x, w_dt, b_dt, a_log, d_skip, w_out, conv_state, ssm_state):
        tokens, width = residual.shape
        inner = w_out.shape[1]
        state = a_log.shape[1]
        lane_tiles = inner // 128
        chunk = tokens // CHUNKS
        half = chunk // 2
        quart = chunk // 4
        w_view = w_in.reshape(2, width, 2, lane_tiles, 128).transpose(0, 1, 3, 2, 4)
        w_view = with_layout_constraint(w_view, Layout(major_to_minor=(0, 1, 2, 3, 4))).reshape(2, width * 2 * lane_tiles, 128)
        conv_view = conv_state.transpose(0, 2, 1, 3)
        vmem = pl.BlockSpec(memory_space=pltpu.VMEM)
        anywhere = pl.BlockSpec(memory_space=pl.ANY)
        hbm = pl.BlockSpec(memory_space=pltpu.HBM)
        f32, bf16 = jnp.float32, jnp.bfloat16
        r_val, conv_val, s0, s1 = pl.pallas_call(
            mamba_kernel,
            name="mamba",
            out_shape=[
                pltpu.VMEM((tokens, width), f32),
                pltpu.VMEM((2, 3, tokens, inner), bf16),
                pltpu.VMEM((tokens, state, inner), f32),
                pltpu.VMEM((tokens, state, inner), f32),
            ],
            in_specs=[hbm] * 13,
            out_specs=[vmem] * 4,
            scratch_shapes=[
                pltpu.VMEM((tokens, width), f32),
                pltpu.VMEM((2, width * 2 * lane_tiles, 128), bf16),
                pltpu.VMEM((2, width, 2 * inner), bf16),
                pltpu.VMEM((2, inner, width), bf16),
                pltpu.VMEM((2, tokens, inner), bf16),
                pltpu.VMEM(norm_w.shape, bf16),
                pltpu.VMEM(conv_w.shape, bf16),
                pltpu.VMEM(conv_b.shape, bf16),
                pltpu.VMEM(w_x.shape, bf16),
                pltpu.VMEM((2, 128, inner), bf16),
                pltpu.VMEM(b_dt.shape, f32),
                pltpu.VMEM(a_log.shape, f32),
                pltpu.VMEM(d_skip.shape, f32),
                pltpu.VMEM((tokens, width), bf16),
                pltpu.VMEM((tokens, inner), bf16),
                pltpu.VMEM((tokens, inner), bf16),
                pltpu.VMEM((tokens, width), bf16),
                pltpu.VMEM((CHUNKS, half, width), bf16),
                pltpu.VMEM((CHUNKS, half // 2, width), bf16),
                pltpu.VMEM((CHUNKS, half // 2, width), bf16),
                pltpu.VMEM((CHUNKS, half // 2, width), bf16),
                pltpu.VMEM((CHUNKS, half // 2, width), f32),
                pltpu.VMEM((tokens, 128), f32),
                pltpu.VMEM((2, tokens, 128), bf16),
                pltpu.VMEM((4, tokens, 128), bf16),
                pltpu.VMEM((state, inner), f32),
                pltpu.VMEM((chunk, inner), f32),
                pltpu.VMEM((chunk, inner), f32),
                pltpu.VMEM((lane_tiles, chunk * 8, 128), f32),
                pltpu.VMEM((chunk, inner), bf16),
                pltpu.SemaphoreType.DMA((KINDS, 2, CHUNKS)),
                pltpu.SemaphoreType.DMA((KINDS, 2, CHUNKS)),
                pltpu.SemaphoreType.DMA((18 + CHUNKS,)),
                pltpu.SemaphoreType.DMA((8,)),
                pltpu.SemaphoreType.DMA((2, CHUNKS)),
            ],
            compiler_params=pltpu.CompilerParams(collective_id=0, has_side_effects=True, vmem_limit_bytes=32 * 2**20),
        )(residual, w_view, w_out, conv_view, ssm_state, norm_w, conv_w, conv_b, w_x, w_dt, b_dt, a_log, d_skip)
        r_new, conv_new, ssm_new = pl.pallas_call(
            dump_kernel,
            name="dump",
            out_shape=[
                jax.ShapeDtypeStruct((tokens, width), f32),
                jax.ShapeDtypeStruct((2, 3, tokens, inner), bf16),
                jax.ShapeDtypeStruct(ssm_state.shape, f32),
            ],
            in_specs=[anywhere] * 4,
            out_specs=[hbm] * 3,
            scratch_shapes=[pltpu.SemaphoreType.DMA((2 + 2 * DUMP_PIECES,))],
            compiler_params=pltpu.CompilerParams(vmem_limit_bytes=2**20),
        )(r_val, conv_val, s0, s1)
        return r_new, conv_new.transpose(0, 2, 1, 3), ssm_new

    cache_spec = P(None, 'dp', None, 'tp')
    in_specs = (P('dp', None), P(None, None), P(None, None, None, 'tp'), P(None, None, 'tp'), P(None, 'tp'), P(None, 'tp', None), P(None, None, 'tp'), P(None, 'tp'), P(None, None, 'tp'), P(None, 'tp'), P(None, 'tp', None), cache_spec, cache_spec)
    out_specs = (P('dp', None), cache_spec, cache_spec)
    return jax.shard_map(device_step, mesh=mesh, in_specs=in_specs, out_specs=out_specs, check_vma=False)
```

```python
import functools

import jax
import jax.numpy as jnp
from jax import lax
from jax.experimental.layout import Layout, with_layout_constraint
from jax.experimental import pallas as pl
from jax.experimental.pallas import tpu as pltpu
from jax.sharding import PartitionSpec as P

MESH = pl.DeviceIdType.MESH
LOG2E = 1.4426950408889634
CHUNKS = 8
KINDS = 10
OFFSETS = ((0, 0, 2, 7, 9, 13, 17, 21), (23, 23, 25, 30, 32, 37, 45, 52))
LAST_OFFSET = 55
SPLIT_OFFSET = 17
GROUP = 64
DUMP_PIECES = 4
SPLIT_STEP = 4


def rms_scale(vector, epsilon):
    return lax.rsqrt(jnp.mean(vector * vector, axis=-1, keepdims=True) + epsilon)


def mamba_kernel(
    residual, w_in, w_out, conv_state, ssm_state, norm_w_hbm, conv_w_hbm, conv_b_hbm, w_x_hbm, w_dt_hbm, b_dt_hbm, a_log_hbm, d_skip_hbm,
    r_out, conv_out, ssm0, ssm1,
    res, w_raw, w_xz, wo, conv_old, norm_w, conv_w, conv_b, w_x, w_dt, b_dt, a_log, d_skip, hid, xc_buf, z_buf, part, half_in, quart_in, quart_sum, pair_in, o_acc,
    p_acc, p_send, p_recv, rate_buf, dt_buf, dx_buf, y_part, yg_buf, send_sem, recv_sem, load_sem, small_sem, state_sem,
):
    layers = 2
    tokens, width = res.shape
    chunk = tokens // CHUNKS
    half = chunk // 2
    quart = chunk // 4
    inner = wo.shape[1]
    rank = w_dt_hbm.shape[1]
    state = a_log.shape[1]
    lane_tiles = inner // 128
    ssm_bufs = (ssm0, ssm1)

    tp = lax.axis_index("tp")
    core = lax.rem(tp, 2)
    pos_x = lax.rem(lax.div(tp, 2), 2)
    pos_y = lax.div(tp, 4)
    bit_a = pos_x * (1 - core) + pos_y * core
    bit_b = pos_y * (1 - core) + pos_x * core
    peer_c = tp + 1 - 2 * core
    peer_a = tp + (1 - 2 * bit_a) * (2 + 2 * core)
    peer_b = tp + (1 - 2 * bit_b) * (4 - 2 * core)
    peer_d = tp + (1 - 2 * pos_x) * 2 + (1 - 2 * pos_y) * 4
    peers = (peer_c, peer_a, peer_b, peer_d)

    barrier = pltpu.get_barrier_semaphore()
    for peer in peers:
        pl.semaphore_signal(barrier, inc=1, device_id={"tp": peer}, device_id_type=MESH)

    def rows_of(q):
        return pl.ds(pl.multiple_of(q * chunk, chunk), chunk)

    def half_rows(q, which):
        return pl.ds(pl.multiple_of(q * chunk + which * half, half), half)

    def quart_rows(q, which_half, which):
        return pl.ds(pl.multiple_of(q * chunk + which_half * half + which * quart, quart), quart)

    def remote(kind, layer, q, src, dst, peer):
        return pltpu.make_async_remote_copy(
            src_ref=src, dst_ref=dst, send_sem=send_sem.at[kind, layer, q], recv_sem=recv_sem.at[kind, layer, q],
            device_id={"tp": peer}, device_id_type=MESH,
        )

    def p_copy(step, layer, q):
        src = p_send.at[min(step, 1), rows_of(q)]
        return remote(step, layer, q, src, p_recv.at[step, rows_of(q)], peers[step])

    def o_copy(step, layer, q):
        if step == 0:
            return remote(4, layer, q, part.at[half_rows(q, 1 - core)], half_in.at[q], peer_c)
        if step == 1:
            return remote(5, layer, q, part.at[quart_rows(q, core, 1 - bit_a)], quart_in.at[q], peer_a)
        return remote(6, layer, q, quart_sum.at[q], pair_in.at[q], peer_b)

    def h_copy(step, layer, q):
        ref = hid.at[quart_rows(q, core, 1 - bit_a if step == 2 else bit_a)]
        return remote(7 + step, layer, q, ref, ref, peer_a if step == 0 else peer_c)

    def w_load(layer):
        return pltpu.make_async_copy(w_in.at[layer], w_raw.at[layer], load_sem.at[layer])

    def res_load(q):
        return pltpu.make_async_copy(residual.at[rows_of(q)], res.at[rows_of(q)], load_sem.at[18 + q])

    def wo_load(layer):
        return pltpu.make_async_copy(w_out.at[layer], wo.at[layer], load_sem.at[10 + layer])

    def conv_load(layer, row):
        dst = conv_old.at[layer] if row == 0 else conv_out.at[layer, row - 1]
        return pltpu.make_async_copy(conv_state.at[layer, row], dst, load_sem.at[12 + 3 * layer + row])

    def state_load(layer, q):
        return pltpu.make_async_copy(ssm_state.at[layer, rows_of(q)], ssm_bufs[layer].at[rows_of(q)], state_sem.at[layer, q])

    small = [
        pltpu.make_async_copy(norm_w_hbm, norm_w, small_sem.at[0]),
        pltpu.make_async_copy(conv_w_hbm, conv_w, small_sem.at[1]),
        pltpu.make_async_copy(conv_b_hbm, conv_b, small_sem.at[2]),
        pltpu.make_async_copy(w_x_hbm, w_x, small_sem.at[3]),
        pltpu.make_async_copy(w_dt_hbm, w_dt.at[:, pl.ds(0, rank)], small_sem.at[4]),
        pltpu.make_async_copy(b_dt_hbm, b_dt, small_sem.at[5]),
        pltpu.make_async_copy(a_log_hbm, a_log, small_sem.at[6]),
        pltpu.make_async_copy(d_skip_hbm, d_skip, small_sem.at[7]),
    ]
    small[0].start()
    res_load(0).start()
    w_load(0).start()
    for q in range(1, CHUNKS):
        res_load(q).start()
    for row in range(3):
        conv_load(0, row).start()
    for copy in small[1:]:
        copy.start()
    for layer in range(layers):
        w_dt[layer, rank:] = jnp.zeros((128 - rank, inner), jnp.bfloat16)

    span = 32
    packed = span * lane_tiles * 2
    blocks = width // (2 * span)

    def split_weights(layer, first, count):
        row = lax.broadcasted_iota(jnp.int32, (packed, packed), 0)
        col = lax.broadcasted_iota(jnp.int32, (packed, packed), 1)
        group = lax.div(row, span)
        want = lax.rem(row, span) * (2 * lane_tiles) + lax.rem(group, lane_tiles) * 2 + lax.div(group, lane_tiles)
        pick = jnp.where(col == want, 1.0, 0.0).astype(jnp.bfloat16)

        @pl.loop(0, count // SPLIT_STEP)
        def _(step):
            for i in range(SPLIT_STEP):
                block = first + step * SPLIT_STEP + i
                raw = [w_raw[layer, pl.ds(pl.multiple_of((2 * block + k) * packed, packed), packed), :] for k in range(2)]
                both = jnp.dot(pick, jnp.concatenate(raw, axis=1), preferred_element_type=jnp.float32).astype(jnp.bfloat16)
                for k in range(2):
                    dst = pl.ds(pl.multiple_of((2 * block + k) * span, span), span)
                    for tile in range(2 * lane_tiles):
                        w_xz[layer, dst, tile * 128:(tile + 1) * 128] = both[tile * span:(tile + 1) * span, k * 128:(k + 1) * 128]

    def first_norm(q):
        res_load(q).wait()

        @pl.loop(0, chunk // 32)
        def _(i):
            sub = pl.ds(pl.multiple_of(q * chunk + i * 32, 32), 32)
            r = res[sub, :]
            hid[sub, :] = (r * rms_scale(r, 1e-5) * norm_w[0:1, :].astype(jnp.float32)).astype(jnp.bfloat16)

    small[0].wait()
    first_norm(0)
    w_load(0).wait()

    split_weights(0, 0, blocks)

    w_load(1).start()
    for q in range(CHUNKS):
        state_load(0, q).start()
    wo_load(0).start()
    for row in range(3):
        conv_load(0, row).wait()
    for copy in small[1:]:
        copy.wait()
    pl.semaphore_wait(barrier, 4)

    def stage_in(layer, q):
        rows = rows_of(q)
        if layer == 0:
            @pl.when(q > 0)
            def _():
                first_norm(q)
        else:
            h_copy(1, layer - 1, q).wait()
            h_copy(2, layer - 1, q).wait()

            @pl.when(q == 0)
            def _():
                for row in range(3):
                    conv_load(1, row).wait()

        x_val = jnp.dot(hid[rows, :], w_xz[layer, :, :inner], preferred_element_type=jnp.float32).astype(jnp.bfloat16)
        conv_out[layer, 2, rows, :] = x_val
        taps = conv_w[layer].astype(jnp.float32)
        pre = conv_old[layer, rows, :].astype(jnp.float32) * taps[0:1]
        pre = pre + conv_out[layer, 0, rows, :].astype(jnp.float32) * taps[1:2]
        pre = pre + conv_out[layer, 1, rows, :].astype(jnp.float32) * taps[2:3]
        pre = pre + x_val.astype(jnp.float32) * taps[3:4]
        pre = pre + conv_b[layer:layer + 1, :].astype(jnp.float32)
        xc = (pre * jax.nn.sigmoid(pre)).astype(jnp.bfloat16)
        xc_buf[rows, :] = xc
        p = jnp.dot(xc, w_x[layer], preferred_element_type=jnp.float32)
        p_acc[rows, :] = p
        p_send[0, rows, :] = p.astype(jnp.bfloat16)
        p_copy(0, layer, q).start()

    def stage_z(layer, q):
        rows = rows_of(q)
        z = jnp.dot(hid[rows, :], w_xz[layer, :, inner:], preferred_element_type=jnp.float32).astype(jnp.bfloat16).astype(jnp.float32)
        z_buf[rows, :] = z * jax.nn.sigmoid(z)

    def stage_p(layer, q):
        rows = rows_of(q)
        p_copy(0, layer, q).wait()
        p = p_acc[rows, :] + p_recv[0, rows, :].astype(jnp.float32)
        p_acc[rows, :] = p
        p_send[1, rows, :] = p.astype(jnp.bfloat16)
        for step in (3, 1, 2):
            p_copy(step, layer, q).start()

    def stage_ssm(layer, q):
        rows = rows_of(q)
        state_buf = ssm_bufs[layer]
        p = p_acc[rows, :]
        for step in (1, 2, 3):
            p_copy(step, layer, q).wait()
            p = p + p_recv[step, rows, :].astype(jnp.float32)
        lane = lax.broadcasted_iota(jnp.int32, p.shape, 1)
        square = p * p
        is_dt = lane < rank
        is_b = jnp.logical_and(lane >= rank, lane < rank + state)

        def scale_of(mask, count):
            total = jnp.sum(jnp.where(mask, square, 0.0), axis=1, keepdims=True)
            return lax.rsqrt(total * (1.0 / count) + 1e-6)

        scale_dt = scale_of(is_dt, rank)
        scale_b = scale_of(is_b, state)
        scale_c = scale_of(lane >= rank + state, state)
        normed = p * jnp.where(is_dt, scale_dt, jnp.where(is_b, scale_b, scale_c))
        dt_low = jnp.where(is_dt, normed, 0.0).astype(jnp.bfloat16)
        pre = jnp.dot(dt_low, w_dt[layer], preferred_element_type=jnp.float32) + b_dt[layer:layer + 1, :]
        dt = jnp.maximum(pre, 0.0) + jnp.log1p(jnp.exp(-jnp.abs(pre)))
        dt_buf[...] = dt
        dx_buf[...] = dt * xc_buf[rows, :].astype(jnp.float32)
        turned = jnp.concatenate([normed] * (128 // chunk), axis=0).T
        b_cols = turned[rank:rank + state, :]
        c_cols = turned[rank + state:, :]
        rate_buf[...] = jnp.exp(a_log[layer]) * (-LOG2E)
        state_load(layer, q).wait()

        def scan_group(g, carry):
            b_now, c_now = carry
            for j in range(GROUP):
                token = g * GROUP + j
                y_rows = pl.ds(token * 8, 8) if chunk == GROUP else pl.ds(pl.multiple_of(token * 8, 8), 8)
                dt_row = dt_buf[pl.ds(token, 1), :]
                dx_row = dx_buf[pl.ds(token, 1), :]
                old = state_buf[q * chunk + token]
                new = jnp.exp2(dt_row * rate_buf[...]) * old + dx_row * b_now[:, j:j + 1]
                state_buf[q * chunk + token] = new
                weighted = new * c_now[:, j:j + 1]
                partial = weighted[:8] + weighted[8:]
                for tile in range(lane_tiles):
                    y_part[tile, y_rows, :] = partial[:, tile * 128:(tile + 1) * 128]
            return pltpu.roll(b_now, 128 - GROUP, 1), pltpu.roll(c_now, 128 - GROUP, 1)

        if chunk == GROUP:
            scan_group(0, (b_cols, c_cols))
        else:
            lax.fori_loop(0, chunk // GROUP, scan_group, (b_cols, c_cols))

        @pl.loop(0, chunk // 16)
        def _(g):
            halves = []
            for k in range(2):
                first = g * 128 + k * 64
                by_tile = []
                for tile in range(lane_tiles):
                    terms = [y_part[tile, pl.ds(first + sub, 8, stride=8), :] for sub in range(8)]
                    while len(terms) > 1:
                        terms = [terms[i] + terms[i + 1] for i in range(0, len(terms), 2)]
                    by_tile.append(terms[0])
                halves.append(jnp.concatenate(by_tile, axis=1))
            sub = pl.ds(pl.multiple_of(g * 16, 16), 16)
            sub_rows = pl.ds(pl.multiple_of(q * chunk + g * 16, 16), 16)
            y = jnp.concatenate(halves, axis=0) + d_skip[layer:layer + 1, :] * xc_buf[sub_rows, :].astype(jnp.float32)
            yg_buf[sub, :] = (y * z_buf[sub_rows, :]).astype(jnp.bfloat16)

        @pl.when(q == 0)
        def _():
            wo_load(layer).wait()

        part[rows, :] = jnp.dot(yg_buf[...], wo[layer], preferred_element_type=jnp.float32).astype(jnp.bfloat16)
        o_copy(0, layer, q).start()

    def stage_half(layer, q):
        o_copy(0, layer, q).wait()
        mine = half_rows(q, core)
        part[mine, :] = (part[mine, :].astype(jnp.float32) + half_in[q].astype(jnp.float32)).astype(jnp.bfloat16)
        o_copy(1, layer, q).start()

    def stage_quart(layer, q):
        o_copy(1, layer, q).wait()
        mine = part[quart_rows(q, core, bit_a), :]
        quart_sum[q] = (mine.astype(jnp.float32) + quart_in[q].astype(jnp.float32)).astype(jnp.bfloat16)
        o_copy(2, layer, q).start()

    def stage_own(layer, q):
        o_copy(2, layer, q).wait()
        for i in range(quart // 16):
            sub = pl.ds(i * 16, 16)
            dst = pl.ds(pl.multiple_of(q * chunk + core * half + bit_a * quart + i * 16, 16), 16)
            o_val = quart_sum[q, sub, :].astype(jnp.float32) + pair_in[q, sub, :].astype(jnp.float32)
            if layer == 0:
                o_acc[q, sub, :] = o_val
                r = res[dst, :] + o_val
                hid[dst, :] = (r * rms_scale(r, 1e-5) * norm_w[1:2, :].astype(jnp.float32)).astype(jnp.bfloat16)
            else:
                hid[dst, :] = (o_acc[q, sub, :] + o_val).astype(jnp.bfloat16)
        h_copy(0, layer, q).start()
        h_copy(1, layer, q).start()

    def stage_forward(layer, q):
        h_copy(0, layer, q).wait()
        h_copy(2, layer, q).start()

    def stage_out(q):
        h_copy(1, layers - 1, q).wait()
        h_copy(2, layers - 1, q).wait()
        rows = rows_of(q)
        r_out[rows, :] = res[rows, :] + hid[rows, :].astype(jnp.float32)

    def stage_split(step):
        @pl.when(step == 0)
        def _():
            w_load(1).wait()
            for row in range(3):
                conv_load(1, row).start()
            wo_load(1).start()
            for q in range(CHUNKS):
                state_load(1, q).start()

        split_weights(1, step * SPLIT_STEP, SPLIT_STEP)

    stages = (stage_in, stage_z, stage_p, stage_ssm, stage_half, stage_quart, stage_own, stage_forward)
    splits = blocks // SPLIT_STEP

    def when_in(tick, offset, count, work):
        @pl.when(jnp.logical_and(tick >= offset, tick < offset + count))
        def _():
            work(tick - offset)

    @pl.loop(0, LAST_OFFSET + CHUNKS)
    def _(tick):
        for layer in range(layers):
            def layer_stages(_, layer=layer):
                for stage, offset in zip(stages, OFFSETS[layer]):
                    when_in(tick, offset, CHUNKS, functools.partial(stage, layer))
                if layer == 0:
                    when_in(tick, SPLIT_OFFSET, splits, stage_split)
                else:
                    when_in(tick, LAST_OFFSET, CHUNKS, stage_out)

            first, last = OFFSETS[layer][0], max(OFFSETS[layer][-1], LAST_OFFSET if layer else SPLIT_OFFSET)
            when_in(tick, first, last + CHUNKS - first, layer_stages)


def dump_kernel(r_val, conv_val, ssm0, ssm1, r_hbm, conv_hbm, ssm_hbm, sems):
    copies = [pltpu.make_async_copy(r_val, r_hbm, sems.at[0]), pltpu.make_async_copy(conv_val, conv_hbm, sems.at[1])]
    piece = ssm0.shape[0] // DUMP_PIECES
    for i in range(DUMP_PIECES):
        for layer, ssm in enumerate((ssm0, ssm1)):
            rows = pl.ds(i * piece, piece)
            copies.append(pltpu.make_async_copy(ssm.at[rows], ssm_hbm.at[layer, rows], sems.at[2 + 2 * i + layer]))
    for copy in copies:
        copy.start()
    for copy in copies:
        copy.wait()


def solution(mesh):
    def device_step(residual, norm_w, w_in, conv_w, conv_b, w_x, w_dt, b_dt, a_log, d_skip, w_out, conv_state, ssm_state):
        tokens, width = residual.shape
        inner = w_out.shape[1]
        state = a_log.shape[1]
        lane_tiles = inner // 128
        chunk = tokens // CHUNKS
        half = chunk // 2
        quart = chunk // 4
        w_view = w_in.reshape(2, width, 2, lane_tiles, 128).transpose(0, 1, 3, 2, 4)
        w_view = with_layout_constraint(w_view, Layout(major_to_minor=(0, 1, 2, 3, 4))).reshape(2, width * 2 * lane_tiles, 128)
        conv_view = conv_state.transpose(0, 2, 1, 3)
        vmem = pl.BlockSpec(memory_space=pltpu.VMEM)
        anywhere = pl.BlockSpec(memory_space=pl.ANY)
        hbm = pl.BlockSpec(memory_space=pltpu.HBM)
        f32, bf16 = jnp.float32, jnp.bfloat16
        r_val, conv_val, s0, s1 = pl.pallas_call(
            mamba_kernel,
            name="mamba",
            out_shape=[
                pltpu.VMEM((tokens, width), f32),
                pltpu.VMEM((2, 3, tokens, inner), bf16),
                pltpu.VMEM((tokens, state, inner), f32),
                pltpu.VMEM((tokens, state, inner), f32),
            ],
            in_specs=[hbm] * 13,
            out_specs=[vmem] * 4,
            scratch_shapes=[
                pltpu.VMEM((tokens, width), f32),
                pltpu.VMEM((2, width * 2 * lane_tiles, 128), bf16),
                pltpu.VMEM((2, width, 2 * inner), bf16),
                pltpu.VMEM((2, inner, width), bf16),
                pltpu.VMEM((2, tokens, inner), bf16),
                pltpu.VMEM(norm_w.shape, bf16),
                pltpu.VMEM(conv_w.shape, bf16),
                pltpu.VMEM(conv_b.shape, bf16),
                pltpu.VMEM(w_x.shape, bf16),
                pltpu.VMEM((2, 128, inner), bf16),
                pltpu.VMEM(b_dt.shape, f32),
                pltpu.VMEM(a_log.shape, f32),
                pltpu.VMEM(d_skip.shape, f32),
                pltpu.VMEM((tokens, width), bf16),
                pltpu.VMEM((tokens, inner), bf16),
                pltpu.VMEM((tokens, inner), f32),
                pltpu.VMEM((tokens, width), bf16),
                pltpu.VMEM((CHUNKS, half, width), bf16),
                pltpu.VMEM((CHUNKS, half // 2, width), bf16),
                pltpu.VMEM((CHUNKS, half // 2, width), bf16),
                pltpu.VMEM((CHUNKS, half // 2, width), bf16),
                pltpu.VMEM((CHUNKS, half // 2, width), f32),
                pltpu.VMEM((tokens, 128), f32),
                pltpu.VMEM((2, tokens, 128), bf16),
                pltpu.VMEM((4, tokens, 128), bf16),
                pltpu.VMEM((state, inner), f32),
                pltpu.VMEM((chunk, inner), f32),
                pltpu.VMEM((chunk, inner), f32),
                pltpu.VMEM((lane_tiles, chunk * 8, 128), f32),
                pltpu.VMEM((chunk, inner), bf16),
                pltpu.SemaphoreType.DMA((KINDS, 2, CHUNKS)),
                pltpu.SemaphoreType.DMA((KINDS, 2, CHUNKS)),
                pltpu.SemaphoreType.DMA((18 + CHUNKS,)),
                pltpu.SemaphoreType.DMA((8,)),
                pltpu.SemaphoreType.DMA((2, CHUNKS)),
            ],
            compiler_params=pltpu.CompilerParams(collective_id=0, has_side_effects=True, vmem_limit_bytes=32 * 2**20),
        )(residual, w_view, w_out, conv_view, ssm_state, norm_w, conv_w, conv_b, w_x, w_dt, b_dt, a_log, d_skip)
        r_new, conv_new, ssm_new = pl.pallas_call(
            dump_kernel,
            name="dump",
            out_shape=[
                jax.ShapeDtypeStruct((tokens, width), f32),
                jax.ShapeDtypeStruct((2, 3, tokens, inner), bf16),
                jax.ShapeDtypeStruct(ssm_state.shape, f32),
            ],
            in_specs=[anywhere] * 4,
            out_specs=[hbm] * 3,
            scratch_shapes=[pltpu.SemaphoreType.DMA((2 + 2 * DUMP_PIECES,))],
            compiler_params=pltpu.CompilerParams(vmem_limit_bytes=2**20),
        )(r_val, conv_val, s0, s1)
        return r_new, conv_new.transpose(0, 2, 1, 3), ssm_new

    cache_spec = P(None, 'dp', None, 'tp')
    in_specs = (P('dp', None), P(None, None), P(None, None, None, 'tp'), P(None, None, 'tp'), P(None, 'tp'), P(None, 'tp', None), P(None, None, 'tp'), P(None, 'tp'), P(None, None, 'tp'), P(None, 'tp'), P(None, 'tp', None), cache_spec, cache_spec)
    out_specs = (P('dp', None), cache_spec, cache_spec)
    return jax.shard_map(device_step, mesh=mesh, in_specs=in_specs, out_specs=out_specs, check_vma=False)
```

```python
import functools

import jax
import jax.numpy as jnp
from jax import lax
from jax.experimental.layout import Layout, with_layout_constraint
from jax.experimental import pallas as pl
from jax.experimental.pallas import tpu as pltpu
from jax.sharding import PartitionSpec as P

MESH = pl.DeviceIdType.MESH
LOG2E = 1.4426950408889634
CHUNKS = 4
KINDS = 10
OFFSETS = ((0, 0, 1, 8, 10, 13, 16, 18), (19, 20, 20, 23, 25, 28, 31, 34))
LAST_OFFSET = 35
SPLIT_OFFSET = 2
GROUP = 64
DUMP_PIECES = 4
SPLIT_STEP = 4


def rms_scale(vector, epsilon):
    return lax.rsqrt(jnp.mean(vector * vector, axis=-1, keepdims=True) + epsilon)


def mamba_kernel(
    residual, w_in, w_out, conv_state, ssm_state, norm_w_hbm, conv_w_hbm, conv_b_hbm, w_x_hbm, w_dt_hbm, b_dt_hbm, a_log_hbm, d_skip_hbm,
    r_out, conv_out, ssm0, ssm1,
    res, w_raw, w_xz, wo, conv_old, norm_w, conv_w, conv_b, w_x, w_dt, b_dt, a_log, d_skip, hid, xc_buf, z_buf, part, half_in, quart_in, quart_sum, pair_in, o_acc,
    p_acc, p_send, p_recv, rate_buf, dt_buf, dx_buf, y_part, yg_buf, send_sem, recv_sem, load_sem, small_sem, state_sem,
):
    layers = 2
    tokens, width = res.shape
    chunk = tokens // CHUNKS
    half = chunk // 2
    quart = chunk // 4
    inner = wo.shape[1]
    rank = w_dt_hbm.shape[1]
    state = a_log.shape[1]
    lane_tiles = inner // 128
    ssm_bufs = (ssm0, ssm1)

    tp = lax.axis_index("tp")
    core = lax.rem(tp, 2)
    pos_x = lax.rem(lax.div(tp, 2), 2)
    pos_y = lax.div(tp, 4)
    bit_a = pos_x * (1 - core) + pos_y * core
    bit_b = pos_y * (1 - core) + pos_x * core
    peer_c = tp + 1 - 2 * core
    peer_a = tp + (1 - 2 * bit_a) * (2 + 2 * core)
    peer_b = tp + (1 - 2 * bit_b) * (4 - 2 * core)
    peer_d = tp + (1 - 2 * pos_x) * 2 + (1 - 2 * pos_y) * 4
    peers = (peer_c, peer_a, peer_b, peer_d)

    barrier = pltpu.get_barrier_semaphore()
    for peer in peers:
        pl.semaphore_signal(barrier, inc=1, device_id={"tp": peer}, device_id_type=MESH)

    def rows_of(q):
        return pl.ds(pl.multiple_of(q * chunk, chunk), chunk)

    def half_rows(q, which):
        return pl.ds(pl.multiple_of(q * chunk + which * half, half), half)

    def quart_rows(q, which_half, which):
        return pl.ds(pl.multiple_of(q * chunk + which_half * half + which * quart, quart), quart)

    def remote(kind, layer, q, src, dst, peer):
        return pltpu.make_async_remote_copy(
            src_ref=src, dst_ref=dst, send_sem=send_sem.at[kind, layer, q], recv_sem=recv_sem.at[kind, layer, q],
            device_id={"tp": peer}, device_id_type=MESH,
        )

    def p_copy(step, layer, q):
        src = p_send.at[min(step, 1), rows_of(q)]
        return remote(step, layer, q, src, p_recv.at[step, rows_of(q)], peers[step])

    def o_copy(step, layer, q):
        if step == 0:
            return remote(4, layer, q, part.at[half_rows(q, 1 - core)], half_in.at[q], peer_c)
        if step == 1:
            return remote(5, layer, q, part.at[quart_rows(q, core, 1 - bit_a)], quart_in.at[q], peer_a)
        return remote(6, layer, q, quart_sum.at[q], pair_in.at[q], peer_b)

    def h_copy(step, layer, q):
        ref = hid.at[quart_rows(q, core, 1 - bit_a if step == 2 else bit_a)]
        return remote(7 + step, layer, q, ref, ref, peer_a if step == 0 else peer_c)

    def w_load(layer):
        return pltpu.make_async_copy(w_in.at[layer], w_raw.at[layer], load_sem.at[layer])

    def res_load(q):
        return pltpu.make_async_copy(residual.at[rows_of(q)], res.at[rows_of(q)], load_sem.at[18 + q])

    def wo_load(layer):
        return pltpu.make_async_copy(w_out.at[layer], wo.at[layer], load_sem.at[10 + layer])

    def conv_load(layer, row):
        dst = conv_old.at[layer] if row == 0 else conv_out.at[layer, row - 1]
        return pltpu.make_async_copy(conv_state.at[layer, row], dst, load_sem.at[12 + 3 * layer + row])

    def state_load(layer, q):
        return pltpu.make_async_copy(ssm_state.at[layer, rows_of(q)], ssm_bufs[layer].at[rows_of(q)], state_sem.at[layer, q])

    small = [
        pltpu.make_async_copy(norm_w_hbm, norm_w, small_sem.at[0]),
        pltpu.make_async_copy(conv_w_hbm, conv_w, small_sem.at[1]),
        pltpu.make_async_copy(conv_b_hbm, conv_b, small_sem.at[2]),
        pltpu.make_async_copy(w_x_hbm, w_x, small_sem.at[3]),
        pltpu.make_async_copy(w_dt_hbm, w_dt.at[:, pl.ds(0, rank)], small_sem.at[4]),
        pltpu.make_async_copy(b_dt_hbm, b_dt, small_sem.at[5]),
        pltpu.make_async_copy(a_log_hbm, a_log, small_sem.at[6]),
        pltpu.make_async_copy(d_skip_hbm, d_skip, small_sem.at[7]),
    ]
    small[0].start()
    res_load(0).start()
    w_load(0).start()
    for q in range(1, CHUNKS):
        res_load(q).start()
    for row in range(3):
        conv_load(0, row).start()
    for copy in small[1:]:
        copy.start()
    for layer in range(layers):
        w_dt[layer, rank:] = jnp.zeros((128 - rank, inner), jnp.bfloat16)

    span = 32
    packed = span * lane_tiles * 2
    blocks = width // (2 * span)

    def split_weights(layer, first, count):
        row = lax.broadcasted_iota(jnp.int32, (packed, packed), 0)
        col = lax.broadcasted_iota(jnp.int32, (packed, packed), 1)
        group = lax.div(row, span)
        want = lax.rem(row, span) * (2 * lane_tiles) + lax.rem(group, lane_tiles) * 2 + lax.div(group, lane_tiles)
        pick = jnp.where(col == want, 1.0, 0.0).astype(jnp.bfloat16)

        @pl.loop(0, count // SPLIT_STEP)
        def _(step):
            for i in range(SPLIT_STEP):
                block = first + step * SPLIT_STEP + i
                raw = [w_raw[layer, pl.ds(pl.multiple_of((2 * block + k) * packed, packed), packed), :] for k in range(2)]
                both = jnp.dot(pick, jnp.concatenate(raw, axis=1), preferred_element_type=jnp.float32).astype(jnp.bfloat16)
                for k in range(2):
                    dst = pl.ds(pl.multiple_of((2 * block + k) * span, span), span)
                    for tile in range(2 * lane_tiles):
                        w_xz[layer, dst, tile * 128:(tile + 1) * 128] = both[tile * span:(tile + 1) * span, k * 128:(k + 1) * 128]

    def first_norm(q):
        res_load(q).wait()

        @pl.loop(0, chunk // 32)
        def _(i):
            sub = pl.ds(pl.multiple_of(q * chunk + i * 32, 32), 32)
            r = res[sub, :]
            hid[sub, :] = (r * rms_scale(r, 1e-5) * norm_w[0:1, :].astype(jnp.float32)).astype(jnp.bfloat16)

    small[0].wait()
    first_norm(0)
    w_load(0).wait()

    split_weights(0, 0, blocks)

    w_load(1).start()
    for q in range(CHUNKS):
        state_load(0, q).start()
    wo_load(0).start()
    for row in range(3):
        conv_load(0, row).wait()
    for copy in small[1:]:
        copy.wait()
    pl.semaphore_wait(barrier, 4)

    def stage_in(layer, q):
        rows = rows_of(q)
        if layer == 0:
            @pl.when(q > 0)
            def _():
                first_norm(q)
        else:
            h_copy(1, layer - 1, q).wait()
            h_copy(2, layer - 1, q).wait()

            @pl.when(q == 0)
            def _():
                for row in range(3):
                    conv_load(1, row).wait()

        x_val = jnp.dot(hid[rows, :], w_xz[layer, :, :inner], preferred_element_type=jnp.float32).astype(jnp.bfloat16)
        conv_out[layer, 2, rows, :] = x_val
        taps = conv_w[layer].astype(jnp.float32)
        pre = conv_old[layer, rows, :].astype(jnp.float32) * taps[0:1]
        pre = pre + conv_out[layer, 0, rows, :].astype(jnp.float32) * taps[1:2]
        pre = pre + conv_out[layer, 1, rows, :].astype(jnp.float32) * taps[2:3]
        pre = pre + x_val.astype(jnp.float32) * taps[3:4]
        pre = pre + conv_b[layer:layer + 1, :].astype(jnp.float32)
        xc = (pre * jax.nn.sigmoid(pre)).astype(jnp.bfloat16)
        xc_buf[rows, :] = xc
        p = jnp.dot(xc, w_x[layer], preferred_element_type=jnp.float32)
        p_acc[rows, :] = p
        p_send[0, rows, :] = p.astype(jnp.bfloat16)
        p_copy(0, layer, q).start()

    def stage_z(layer, q):
        rows = rows_of(q)
        z = jnp.dot(hid[rows, :], w_xz[layer, :, inner:], preferred_element_type=jnp.float32).astype(jnp.bfloat16).astype(jnp.float32)
        z_buf[rows, :] = z * jax.nn.sigmoid(z)

    def stage_p(layer, q):
        rows = rows_of(q)
        p_copy(0, layer, q).wait()
        p = p_acc[rows, :] + p_recv[0, rows, :].astype(jnp.float32)
        p_acc[rows, :] = p
        p_send[1, rows, :] = p.astype(jnp.bfloat16)
        for step in (3, 1, 2):
            p_copy(step, layer, q).start()

    def stage_ssm(layer, q):
        rows = rows_of(q)
        state_buf = ssm_bufs[layer]
        p = p_acc[rows, :]
        for step in (1, 2, 3):
            p_copy(step, layer, q).wait()
            p = p + p_recv[step, rows, :].astype(jnp.float32)
        lane = lax.broadcasted_iota(jnp.int32, p.shape, 1)
        square = p * p
        is_dt = lane < rank
        is_b = jnp.logical_and(lane >= rank, lane < rank + state)

        def scale_of(mask, count):
            total = jnp.sum(jnp.where(mask, square, 0.0), axis=1, keepdims=True)
            return lax.rsqrt(total * (1.0 / count) + 1e-6)

        scale_dt = scale_of(is_dt, rank)
        scale_b = scale_of(is_b, state)
        scale_c = scale_of(lane >= rank + state, state)
        normed = p * jnp.where(is_dt, scale_dt, jnp.where(is_b, scale_b, scale_c))
        dt_low = jnp.where(is_dt, normed, 0.0).astype(jnp.bfloat16)
        pre = jnp.dot(dt_low, w_dt[layer], preferred_element_type=jnp.float32) + b_dt[layer:layer + 1, :]
        dt = jnp.maximum(pre, 0.0) + jnp.log1p(jnp.exp(-jnp.abs(pre)))
        dt_buf[...] = dt
        dx_buf[...] = dt * xc_buf[rows, :].astype(jnp.float32)
        turned = jnp.concatenate([normed] * (128 // chunk), axis=0).T
        b_cols = turned[rank:rank + state, :]
        c_cols = turned[rank + state:, :]
        rate_buf[...] = jnp.exp(a_log[layer]) * (-LOG2E)
        state_load(layer, q).wait()

        def scan_group(g, carry):
            b_now, c_now = carry
            for j in range(GROUP):
                token = g * GROUP + j
                y_rows = pl.ds(token * 8, 8) if chunk == GROUP else pl.ds(pl.multiple_of(token * 8, 8), 8)
                dt_row = dt_buf[pl.ds(token, 1), :]
                dx_row = dx_buf[pl.ds(token, 1), :]
                old = state_buf[q * chunk + token]
                new = jnp.exp2(dt_row * rate_buf[...]) * old + dx_row * b_now[:, j:j + 1]
                state_buf[q * chunk + token] = new
                weighted = new * c_now[:, j:j + 1]
                partial = weighted[:8] + weighted[8:]
                for tile in range(lane_tiles):
                    y_part[tile, y_rows, :] = partial[:, tile * 128:(tile + 1) * 128]
            return pltpu.roll(b_now, 128 - GROUP, 1), pltpu.roll(c_now, 128 - GROUP, 1)

        if chunk == GROUP:
            scan_group(0, (b_cols, c_cols))
        else:
            lax.fori_loop(0, chunk // GROUP, scan_group, (b_cols, c_cols))

        @pl.loop(0, chunk // 16)
        def _(g):
            halves = []
            for k in range(2):
                first = g * 128 + k * 64
                by_tile = []
                for tile in range(lane_tiles):
                    terms = [y_part[tile, pl.ds(first + sub, 8, stride=8), :] for sub in range(8)]
                    while len(terms) > 1:
                        terms = [terms[i] + terms[i + 1] for i in range(0, len(terms), 2)]
                    by_tile.append(terms[0])
                halves.append(jnp.concatenate(by_tile, axis=1))
            sub = pl.ds(pl.multiple_of(g * 16, 16), 16)
            sub_rows = pl.ds(pl.multiple_of(q * chunk + g * 16, 16), 16)
            y = jnp.concatenate(halves, axis=0) + d_skip[layer:layer + 1, :] * xc_buf[sub_rows, :].astype(jnp.float32)
            yg_buf[sub, :] = (y * z_buf[sub_rows, :]).astype(jnp.bfloat16)

        @pl.when(q == 0)
        def _():
            wo_load(layer).wait()

        part[rows, :] = jnp.dot(yg_buf[...], wo[layer], preferred_element_type=jnp.float32).astype(jnp.bfloat16)
        o_copy(0, layer, q).start()

    def stage_half(layer, q):
        o_copy(0, layer, q).wait()
        mine = half_rows(q, core)
        part[mine, :] = (part[mine, :].astype(jnp.float32) + half_in[q].astype(jnp.float32)).astype(jnp.bfloat16)
        o_copy(1, layer, q).start()

    def stage_quart(layer, q):
        o_copy(1, layer, q).wait()
        mine = part[quart_rows(q, core, bit_a), :]
        quart_sum[q] = (mine.astype(jnp.float32) + quart_in[q].astype(jnp.float32)).astype(jnp.bfloat16)
        o_copy(2, layer, q).start()

    def stage_own(layer, q):
        o_copy(2, layer, q).wait()
        for i in range(quart // 16):
            sub = pl.ds(i * 16, 16)
            dst = pl.ds(pl.multiple_of(q * chunk + core * half + bit_a * quart + i * 16, 16), 16)
            o_val = quart_sum[q, sub, :].astype(jnp.float32) + pair_in[q, sub, :].astype(jnp.float32)
            if layer == 0:
                o_acc[q, sub, :] = o_val
                r = res[dst, :] + o_val
                hid[dst, :] = (r * rms_scale(r, 1e-5) * norm_w[1:2, :].astype(jnp.float32)).astype(jnp.bfloat16)
            else:
                hid[dst, :] = (o_acc[q, sub, :] + o_val).astype(jnp.bfloat16)
        h_copy(0, layer, q).start()
        h_copy(1, layer, q).start()

    def stage_forward(layer, q):
        h_copy(0, layer, q).wait()
        h_copy(2, layer, q).start()

    def stage_out(q):
        h_copy(1, layers - 1, q).wait()
        h_copy(2, layers - 1, q).wait()
        rows = rows_of(q)
        r_out[rows, :] = res[rows, :] + hid[rows, :].astype(jnp.float32)

    def stage_split(step):
        @pl.when(step == 0)
        def _():
            w_load(1).wait()
            for row in range(3):
                conv_load(1, row).start()
            wo_load(1).start()
            for q in range(CHUNKS):
                state_load(1, q).start()

        split_weights(1, step * SPLIT_STEP, SPLIT_STEP)

    stages = (stage_in, stage_z, stage_p, stage_ssm, stage_half, stage_quart, stage_own, stage_forward)
    splits = blocks // SPLIT_STEP

    def when_in(tick, offset, count, work):
        @pl.when(jnp.logical_and(tick >= offset, tick < offset + count))
        def _():
            work(tick - offset)

    @pl.loop(0, LAST_OFFSET + CHUNKS)
    def _(tick):
        for layer in range(layers):
            def layer_stages(_, layer=layer):
                for stage, offset in zip(stages, OFFSETS[layer]):
                    when_in(tick, offset, CHUNKS, functools.partial(stage, layer))
                if layer == 0:
                    when_in(tick, SPLIT_OFFSET, splits, stage_split)
                else:
                    when_in(tick, LAST_OFFSET, CHUNKS, stage_out)

            first, last = OFFSETS[layer][0], max(OFFSETS[layer][-1], LAST_OFFSET if layer else SPLIT_OFFSET)
            when_in(tick, first, last + CHUNKS - first, layer_stages)


def dump_kernel(r_val, conv_val, ssm0, ssm1, r_hbm, conv_hbm, ssm_hbm, sems):
    copies = [pltpu.make_async_copy(r_val, r_hbm, sems.at[0]), pltpu.make_async_copy(conv_val, conv_hbm, sems.at[1])]
    piece = ssm0.shape[0] // DUMP_PIECES
    for i in range(DUMP_PIECES):
        for layer, ssm in enumerate((ssm0, ssm1)):
            rows = pl.ds(i * piece, piece)
            copies.append(pltpu.make_async_copy(ssm.at[rows], ssm_hbm.at[layer, rows], sems.at[2 + 2 * i + layer]))
    for copy in copies:
        copy.start()
    for copy in copies:
        copy.wait()


def solution(mesh):
    def device_step(residual, norm_w, w_in, conv_w, conv_b, w_x, w_dt, b_dt, a_log, d_skip, w_out, conv_state, ssm_state):
        tokens, width = residual.shape
        inner = w_out.shape[1]
        state = a_log.shape[1]
        lane_tiles = inner // 128
        chunk = tokens // CHUNKS
        half = chunk // 2
        quart = chunk // 4
        w_view = w_in.reshape(2, width, 2, lane_tiles, 128).transpose(0, 1, 3, 2, 4)
        w_view = with_layout_constraint(w_view, Layout(major_to_minor=(0, 1, 2, 3, 4))).reshape(2, width * 2 * lane_tiles, 128)
        conv_view = conv_state.transpose(0, 2, 1, 3)
        vmem = pl.BlockSpec(memory_space=pltpu.VMEM)
        anywhere = pl.BlockSpec(memory_space=pl.ANY)
        hbm = pl.BlockSpec(memory_space=pltpu.HBM)
        f32, bf16 = jnp.float32, jnp.bfloat16
        r_val, conv_val, s0, s1 = pl.pallas_call(
            mamba_kernel,
            name="mamba",
            out_shape=[
                pltpu.VMEM((tokens, width), f32),
                pltpu.VMEM((2, 3, tokens, inner), bf16),
                pltpu.VMEM((tokens, state, inner), f32),
                pltpu.VMEM((tokens, state, inner), f32),
            ],
            in_specs=[hbm] * 13,
            out_specs=[vmem] * 4,
            scratch_shapes=[
                pltpu.VMEM((tokens, width), f32),
                pltpu.VMEM((2, width * 2 * lane_tiles, 128), bf16),
                pltpu.VMEM((2, width, 2 * inner), bf16),
                pltpu.VMEM((2, inner, width), bf16),
                pltpu.VMEM((2, tokens, inner), bf16),
                pltpu.VMEM(norm_w.shape, bf16),
                pltpu.VMEM(conv_w.shape, bf16),
                pltpu.VMEM(conv_b.shape, bf16),
                pltpu.VMEM(w_x.shape, bf16),
                pltpu.VMEM((2, 128, inner), bf16),
                pltpu.VMEM(b_dt.shape, f32),
                pltpu.VMEM(a_log.shape, f32),
                pltpu.VMEM(d_skip.shape, f32),
                pltpu.VMEM((tokens, width), bf16),
                pltpu.VMEM((tokens, inner), bf16),
                pltpu.VMEM((tokens, inner), f32),
                pltpu.VMEM((tokens, width), bf16),
                pltpu.VMEM((CHUNKS, half, width), bf16),
                pltpu.VMEM((CHUNKS, half // 2, width), bf16),
                pltpu.VMEM((CHUNKS, half // 2, width), bf16),
                pltpu.VMEM((CHUNKS, half // 2, width), bf16),
                pltpu.VMEM((CHUNKS, half // 2, width), f32),
                pltpu.VMEM((tokens, 128), f32),
                pltpu.VMEM((2, tokens, 128), bf16),
                pltpu.VMEM((4, tokens, 128), bf16),
                pltpu.VMEM((state, inner), f32),
                pltpu.VMEM((chunk, inner), f32),
                pltpu.VMEM((chunk, inner), f32),
                pltpu.VMEM((lane_tiles, chunk * 8, 128), f32),
                pltpu.VMEM((chunk, inner), bf16),
                pltpu.SemaphoreType.DMA((KINDS, 2, CHUNKS)),
                pltpu.SemaphoreType.DMA((KINDS, 2, CHUNKS)),
                pltpu.SemaphoreType.DMA((18 + CHUNKS,)),
                pltpu.SemaphoreType.DMA((8,)),
                pltpu.SemaphoreType.DMA((2, CHUNKS)),
            ],
            compiler_params=pltpu.CompilerParams(collective_id=0, has_side_effects=True, vmem_limit_bytes=32 * 2**20),
        )(residual, w_view, w_out, conv_view, ssm_state, norm_w, conv_w, conv_b, w_x, w_dt, b_dt, a_log, d_skip)
        r_new, conv_new, ssm_new = pl.pallas_call(
            dump_kernel,
            name="dump",
            out_shape=[
                jax.ShapeDtypeStruct((tokens, width), f32),
                jax.ShapeDtypeStruct((2, 3, tokens, inner), bf16),
                jax.ShapeDtypeStruct(ssm_state.shape, f32),
            ],
            in_specs=[anywhere] * 4,
            out_specs=[hbm] * 3,
            scratch_shapes=[pltpu.SemaphoreType.DMA((2 + 2 * DUMP_PIECES,))],
            compiler_params=pltpu.CompilerParams(vmem_limit_bytes=2**20),
        )(r_val, conv_val, s0, s1)
        return r_new, conv_new.transpose(0, 2, 1, 3), ssm_new

    cache_spec = P(None, 'dp', None, 'tp')
    in_specs = (P('dp', None), P(None, None), P(None, None, None, 'tp'), P(None, None, 'tp'), P(None, 'tp'), P(None, 'tp', None), P(None, None, 'tp'), P(None, 'tp'), P(None, None, 'tp'), P(None, 'tp'), P(None, 'tp', None), cache_spec, cache_spec)
    out_specs = (P('dp', None), cache_spec, cache_spec)
    return jax.shard_map(device_step, mesh=mesh, in_specs=in_specs, out_specs=out_specs, check_vma=False)
```

```python
import functools

import jax
import jax.numpy as jnp
from jax import lax
from jax.experimental.layout import Layout, with_layout_constraint
from jax.experimental import pallas as pl
from jax.experimental.pallas import tpu as pltpu
from jax.sharding import PartitionSpec as P

MESH = pl.DeviceIdType.MESH
LOG2E = 1.4426950408889634
CHUNKS = 8
KINDS = 10
ORDER = (0, 1, 0, 3, 7, 0, 1, 7, 2, 1, 3, 5, 3, 7, 4, 2, 6, 6, 4, 5, 8, 2, 5, 4, 8, 8, 6, 0, 1, 3, 0, 2, 1, 4, 3, 6, 2, 0, 4, 5, 1, 6, 7, 3, 5, 2, 0, 7, 1, 8, 8, 6, 4, 8, 5, 2, 0, 3, 7, 1, 0, 6, 4, 1, 5, 2, 1, 0, 0, 3, 7, 1, 2, 2, 6, 4, 3, 2, 5, 3, 6, 6, 4, 4, 3, 7, 0, 6, 5, 4, 1, 5, 7, 0, 5, 7, 2, 1, 7, 3, 6, 4, 3, 2, 1, 5, 6, 0, 7, 4, 5, 3, 7, 2, 6, 1, 4, 5, 7, 3, 2, 6, 0, 4, 1, 5, 7, 0, 4, 5, 2, 3, 6, 7, 4, 0, 1, 2, 5, 6, 3, 7)

GROUP = 16
DUMP_PIECES = 4
ORDER_FIRST = tuple(dict.fromkeys(q for q in ORDER if q < CHUNKS))


def rms_scale(vector, epsilon):
    return lax.rsqrt(jnp.mean(vector * vector, axis=-1, keepdims=True) + epsilon)


def mamba_kernel(
    residual, w_in, w_out, conv_state, ssm_state, norm_w_hbm, conv_w_hbm, conv_b_hbm, w_x_hbm, w_dt_hbm, b_dt_hbm, a_log_hbm, d_skip_hbm,
    r_out, conv_out, ssm0, ssm1,
    res, w_raw, w_xz, wo, conv_old, norm_w, conv_w, conv_b, w_x, w_dt, b_dt, a_log, d_skip, hid, xc_buf, z_buf, part, half_in, quart_in, quart_sum, pair_in, o_acc,
    p_acc, p_send, p_recv, rate_buf, dt_buf, dx_buf, y_part, yg_buf, send_sem, recv_sem, load_sem, small_sem, state_sem,
):
    layers = 2
    tokens, width = res.shape
    chunk = tokens // CHUNKS
    half = chunk // 2
    quart = chunk // 4
    inner = wo.shape[1]
    rank = w_dt_hbm.shape[1]
    state = a_log.shape[1]
    lane_tiles = inner // 128
    ssm_bufs = (ssm0, ssm1)

    tp = lax.axis_index("tp")
    core = lax.rem(tp, 2)
    pos_x = lax.rem(lax.div(tp, 2), 2)
    pos_y = lax.div(tp, 4)
    bit_a = pos_x * (1 - core) + pos_y * core
    bit_b = pos_y * (1 - core) + pos_x * core
    peer_c = tp + 1 - 2 * core
    peer_a = tp + (1 - 2 * bit_a) * (2 + 2 * core)
    peer_b = tp + (1 - 2 * bit_b) * (4 - 2 * core)
    peer_d = tp + (1 - 2 * pos_x) * 2 + (1 - 2 * pos_y) * 4
    peers = (peer_c, peer_a, peer_b, peer_d)

    barrier = pltpu.get_barrier_semaphore()
    for peer in peers:
        pl.semaphore_signal(barrier, inc=1, device_id={"tp": peer}, device_id_type=MESH)

    def rows_of(q):
        return pl.ds(q * chunk, chunk)

    def half_rows(q, which):
        return pl.ds(pl.multiple_of(q * chunk + which * half, half), half)

    def quart_rows(q, which_half, which):
        return pl.ds(pl.multiple_of(q * chunk + which_half * half + which * quart, quart), quart)

    def remote(kind, layer, q, src, dst, peer):
        return pltpu.make_async_remote_copy(
            src_ref=src, dst_ref=dst, send_sem=send_sem.at[kind, layer, q], recv_sem=recv_sem.at[kind, layer, q],
            device_id={"tp": peer}, device_id_type=MESH,
        )

    def p_copy(step, layer, q):
        src = p_send.at[min(step, 1), rows_of(q)]
        return remote(step, layer, q, src, p_recv.at[step, rows_of(q)], peers[step])

    def o_copy(step, layer, q):
        if step == 0:
            return remote(4, layer, q, part.at[half_rows(q, 1 - core)], half_in.at[q], peer_c)
        if step == 1:
            return remote(5, layer, q, part.at[quart_rows(q, core, 1 - bit_a)], quart_in.at[q], peer_a)
        return remote(6, layer, q, quart_sum.at[q], pair_in.at[q], peer_b)

    def h_copy(step, layer, q):
        ref = hid.at[quart_rows(q, core, 1 - bit_a if step == 2 else bit_a)]
        return remote(7 + step, layer, q, ref, ref, peer_a if step == 0 else peer_c)

    def w_load(layer):
        return pltpu.make_async_copy(w_in.at[layer], w_raw.at[layer], load_sem.at[layer])

    def res_load(q):
        return pltpu.make_async_copy(residual.at[rows_of(q)], res.at[rows_of(q)], load_sem.at[18 + q])

    def wo_load(layer):
        return pltpu.make_async_copy(w_out.at[layer], wo.at[layer], load_sem.at[10 + layer])

    def conv_load(layer, row):
        dst = conv_old.at[layer] if row == 0 else conv_out.at[layer, row - 1]
        return pltpu.make_async_copy(conv_state.at[layer, row], dst, load_sem.at[12 + 3 * layer + row])

    def state_load(layer, q):
        return pltpu.make_async_copy(ssm_state.at[layer, rows_of(q)], ssm_bufs[layer].at[rows_of(q)], state_sem.at[layer, q])

    small = [
        pltpu.make_async_copy(norm_w_hbm, norm_w, small_sem.at[0]),
        pltpu.make_async_copy(conv_w_hbm, conv_w, small_sem.at[1]),
        pltpu.make_async_copy(conv_b_hbm, conv_b, small_sem.at[2]),
        pltpu.make_async_copy(w_x_hbm, w_x, small_sem.at[3]),
        pltpu.make_async_copy(w_dt_hbm, w_dt.at[:, pl.ds(0, rank)], small_sem.at[4]),
        pltpu.make_async_copy(b_dt_hbm, b_dt, small_sem.at[5]),
        pltpu.make_async_copy(a_log_hbm, a_log, small_sem.at[6]),
        pltpu.make_async_copy(d_skip_hbm, d_skip, small_sem.at[7]),
    ]
    small[0].start()
    res_load(ORDER[0]).start()
    w_load(0).start()
    for q in range(CHUNKS):
        if q != ORDER[0]:
            res_load(q).start()
    for row in range(3):
        conv_load(0, row).start()
    for copy in small[1:]:
        copy.start()
    for layer in range(layers):
        w_dt[layer, rank:] = jnp.zeros((128 - rank, inner), jnp.bfloat16)

    span = 32
    packed = span * lane_tiles * 2
    blocks = width // (2 * span)

    def split_weights(layer, first, count):
        row = lax.broadcasted_iota(jnp.int32, (packed, packed), 0)
        col = lax.broadcasted_iota(jnp.int32, (packed, packed), 1)
        group = lax.div(row, span)
        want = lax.rem(row, span) * (2 * lane_tiles) + lax.rem(group, lane_tiles) * 2 + lax.div(group, lane_tiles)
        pick = jnp.where(col == want, 1.0, 0.0).astype(jnp.bfloat16)

        @pl.loop(0, count // 4)
        def _(step):
            for i in range(4):
                block = first + step * 4 + i
                raw = [w_raw[layer, pl.ds(pl.multiple_of((2 * block + k) * packed, packed), packed), :] for k in range(2)]
                both = jnp.dot(pick, jnp.concatenate(raw, axis=1), preferred_element_type=jnp.float32).astype(jnp.bfloat16)
                for k in range(2):
                    dst = pl.ds(pl.multiple_of((2 * block + k) * span, span), span)
                    for tile in range(2 * lane_tiles):
                        w_xz[layer, dst, tile * 128:(tile + 1) * 128] = both[tile * span:(tile + 1) * span, k * 128:(k + 1) * 128]

    split_step = 4

    def first_norm(q):
        res_load(q).wait()

        @pl.loop(0, chunk // 32)
        def _(i):
            sub = pl.ds(pl.multiple_of(q * chunk + i * 32, 32), 32)
            r = res[sub, :]
            hid[sub, :] = (r * rms_scale(r, 1e-5) * norm_w[0:1, :].astype(jnp.float32)).astype(jnp.bfloat16)

    small[0].wait()
    first_norm(ORDER[0])
    w_load(0).wait()

    split_weights(0, 0, blocks)

    w_load(1).start()
    for q in ORDER_FIRST:
        state_load(0, q).start()
    wo_load(0).start()
    for row in range(3):
        conv_load(0, row).wait()
    for copy in small[1:]:
        copy.wait()
    pl.semaphore_wait(barrier, 4)

    wo_ready = [False] * layers

    def stage_in(layer, q):
        rows = rows_of(q)
        if layer == 0:
            if q != ORDER[0]:
                first_norm(q)
        else:
            h_copy(1, layer - 1, q).wait()
            h_copy(2, layer - 1, q).wait()
        x_val = jnp.dot(hid[rows, :], w_xz[layer, :, :inner], preferred_element_type=jnp.float32).astype(jnp.bfloat16)
        conv_out[layer, 2, rows, :] = x_val
        taps = conv_w[layer].astype(jnp.float32)
        pre = conv_old[layer, rows, :].astype(jnp.float32) * taps[0:1]
        pre = pre + conv_out[layer, 0, rows, :].astype(jnp.float32) * taps[1:2]
        pre = pre + conv_out[layer, 1, rows, :].astype(jnp.float32) * taps[2:3]
        pre = pre + x_val.astype(jnp.float32) * taps[3:4]
        pre = pre + conv_b[layer:layer + 1, :].astype(jnp.float32)
        xc = (pre * jax.nn.sigmoid(pre)).astype(jnp.bfloat16)
        xc_buf[rows, :] = xc
        p = jnp.dot(xc, w_x[layer], preferred_element_type=jnp.float32)
        p_acc[rows, :] = p
        p_send[0, rows, :] = p.astype(jnp.bfloat16)
        p_copy(0, layer, q).start()

    def stage_z(layer, q):
        rows = rows_of(q)
        z = jnp.dot(hid[rows, :], w_xz[layer, :, inner:], preferred_element_type=jnp.float32).astype(jnp.bfloat16).astype(jnp.float32)
        z_buf[rows, :] = z * jax.nn.sigmoid(z)

    def stage_p(layer, q):
        rows = rows_of(q)
        p_copy(0, layer, q).wait()
        p = p_acc[rows, :] + p_recv[0, rows, :].astype(jnp.float32)
        p_acc[rows, :] = p
        p_send[1, rows, :] = p.astype(jnp.bfloat16)
        for step in (3, 1, 2):
            p_copy(step, layer, q).start()

    def stage_ssm(layer, q):
        rows = rows_of(q)
        state_buf = ssm_bufs[layer]
        p = p_acc[rows, :]
        for step in (1, 2, 3):
            p_copy(step, layer, q).wait()
            p = p + p_recv[step, rows, :].astype(jnp.float32)
        lane = lax.broadcasted_iota(jnp.int32, p.shape, 1)
        square = p * p
        is_dt = lane < rank
        is_b = jnp.logical_and(lane >= rank, lane < rank + state)

        def scale_of(mask, count):
            total = jnp.sum(jnp.where(mask, square, 0.0), axis=1, keepdims=True)
            return lax.rsqrt(total * (1.0 / count) + 1e-6)

        scale_dt = scale_of(is_dt, rank)
        scale_b = scale_of(is_b, state)
        scale_c = scale_of(lane >= rank + state, state)
        normed = p * jnp.where(is_dt, scale_dt, jnp.where(is_b, scale_b, scale_c))
        dt_low = jnp.where(is_dt, normed, 0.0).astype(jnp.bfloat16)
        pre = jnp.dot(dt_low, w_dt[layer], preferred_element_type=jnp.float32) + b_dt[layer:layer + 1, :]
        dt = jnp.maximum(pre, 0.0) + jnp.log1p(jnp.exp(-jnp.abs(pre)))
        dt_buf[...] = dt
        dx_buf[...] = dt * xc_buf[rows, :].astype(jnp.float32)
        turned = jnp.concatenate([normed] * (128 // chunk), axis=0).T
        b_cols = turned[rank:rank + state, :]
        c_cols = turned[rank + state:, :]
        rate_buf[...] = jnp.exp(a_log[layer]) * (-LOG2E)
        state_load(layer, q).wait()

        def scan_group(g, carry):
            b_now, c_now = carry
            first = pl.multiple_of(g * GROUP, GROUP)
            states = state_buf.at[pl.ds(q * chunk + first, GROUP)]
            dts = dt_buf.at[pl.ds(first, GROUP)]
            dxs = dx_buf.at[pl.ds(first, GROUP)]
            ys = [y_part.at[tile, pl.ds(pl.multiple_of(first * 8, 8 * GROUP), 8 * GROUP)] for tile in range(lane_tiles)]
            for j in range(GROUP):
                new = jnp.exp2(dts[j:j + 1] * rate_buf[...]) * states[j] + dxs[j:j + 1] * b_now[:, j:j + 1]
                states[j] = new
                weighted = new * c_now[:, j:j + 1]
                partial = weighted[:8] + weighted[8:]
                for tile in range(lane_tiles):
                    ys[tile][j * 8:(j + 1) * 8] = partial[:, tile * 128:(tile + 1) * 128]
            return pltpu.roll(b_now, 128 - GROUP, 1), pltpu.roll(c_now, 128 - GROUP, 1)

        lax.fori_loop(0, chunk // GROUP, scan_group, (b_cols, c_cols))

        @pl.loop(0, chunk // 16)
        def _(g):
            halves = []
            for k in range(2):
                first = g * 128 + k * 64
                by_tile = []
                for tile in range(lane_tiles):
                    total = y_part[tile, pl.ds(first, 8, stride=8), :]
                    for step in range(1, 8):
                        total = total + y_part[tile, pl.ds(first + step, 8, stride=8), :]
                    by_tile.append(total)
                halves.append(jnp.concatenate(by_tile, axis=1))
            sub = pl.ds(pl.multiple_of(g * 16, 16), 16)
            sub_rows = pl.ds(pl.multiple_of(q * chunk + g * 16, 16), 16)
            y = jnp.concatenate(halves, axis=0) + d_skip[layer:layer + 1, :] * xc_buf[sub_rows, :].astype(jnp.float32)
            yg_buf[sub, :] = (y * z_buf[sub_rows, :]).astype(jnp.bfloat16)

        if not wo_ready[layer]:
            wo_load(layer).wait()
            wo_ready[layer] = True
        part[rows, :] = jnp.dot(yg_buf[...], wo[layer], preferred_element_type=jnp.float32).astype(jnp.bfloat16)
        o_copy(0, layer, q).start()

    def stage_half(layer, q):
        o_copy(0, layer, q).wait()
        mine = half_rows(q, core)
        part[mine, :] = (part[mine, :].astype(jnp.float32) + half_in[q].astype(jnp.float32)).astype(jnp.bfloat16)
        o_copy(1, layer, q).start()

    def stage_quart(layer, q):
        o_copy(1, layer, q).wait()
        mine = part[quart_rows(q, core, bit_a), :]
        quart_sum[q] = (mine.astype(jnp.float32) + quart_in[q].astype(jnp.float32)).astype(jnp.bfloat16)
        o_copy(2, layer, q).start()

    def stage_own(layer, q):
        o_copy(2, layer, q).wait()
        for i in range(quart // 16):
            sub = pl.ds(i * 16, 16)
            dst = pl.ds(pl.multiple_of(q * chunk + core * half + bit_a * quart + i * 16, 16), 16)
            o_val = quart_sum[q, sub, :].astype(jnp.float32) + pair_in[q, sub, :].astype(jnp.float32)
            if layer == 0:
                o_acc[q, sub, :] = o_val
                r = res[dst, :] + o_val
                hid[dst, :] = (r * rms_scale(r, 1e-5) * norm_w[1:2, :].astype(jnp.float32)).astype(jnp.bfloat16)
            else:
                hid[dst, :] = (o_acc[q, sub, :] + o_val).astype(jnp.bfloat16)
        h_copy(0, layer, q).start()
        h_copy(1, layer, q).start()

    def stage_forward(layer, q):
        h_copy(0, layer, q).wait()
        h_copy(2, layer, q).start()

    def stage_out(q):
        h_copy(1, layers - 1, q).wait()
        h_copy(2, layers - 1, q).wait()
        rows = rows_of(q)
        r_out[rows, :] = res[rows, :] + hid[rows, :].astype(jnp.float32)

    stages = []
    for layer in range(layers):
        stages.append(functools.partial(stage_in, layer))
        stages.append(functools.partial(stage_z, layer))
        stages.append(functools.partial(stage_p, layer))
        stages.append(functools.partial(stage_ssm, layer))
        stages.append(functools.partial(stage_half, layer))
        stages.append(functools.partial(stage_quart, layer))
        stages.append(functools.partial(stage_own, layer))
        stages.append(functools.partial(stage_forward, layer))
    stages.append(stage_out)

    per_layer = len(stages) // layers
    progress = [0] * CHUNKS
    second_ready = False
    fills = 0
    for q in ORDER:
        if q == CHUNKS:
            if fills == 0:
                w_load(1).wait()
                for row in range(3):
                    conv_load(1, row).start()
                wo_load(1).start()
                for chunk_index in ORDER_FIRST:
                    state_load(1, chunk_index).start()
            split_weights(1, fills * split_step, split_step)
            fills += 1
        else:
            if progress[q] == per_layer and not second_ready:
                for row in range(3):
                    conv_load(1, row).wait()
                second_ready = True
            stages[progress[q]](q)
            progress[q] += 1


def dump_kernel(r_val, conv_val, ssm0, ssm1, r_hbm, conv_hbm, ssm_hbm, sems):
    copies = [pltpu.make_async_copy(r_val, r_hbm, sems.at[0]), pltpu.make_async_copy(conv_val, conv_hbm, sems.at[1])]
    piece = ssm0.shape[0] // DUMP_PIECES
    for i in range(DUMP_PIECES):
        for layer, ssm in enumerate((ssm0, ssm1)):
            rows = pl.ds(i * piece, piece)
            copies.append(pltpu.make_async_copy(ssm.at[rows], ssm_hbm.at[layer, rows], sems.at[2 + 2 * i + layer]))
    for copy in copies:
        copy.start()
    for copy in copies:
        copy.wait()


def solution(mesh):
    def device_step(residual, norm_w, w_in, conv_w, conv_b, w_x, w_dt, b_dt, a_log, d_skip, w_out, conv_state, ssm_state):
        tokens, width = residual.shape
        inner = w_out.shape[1]
        state = a_log.shape[1]
        lane_tiles = inner // 128
        chunk = tokens // CHUNKS
        half = chunk // 2
        quart = chunk // 4
        w_view = w_in.reshape(2, width, 2, lane_tiles, 128).transpose(0, 1, 3, 2, 4)
        w_view = with_layout_constraint(w_view, Layout(major_to_minor=(0, 1, 2, 3, 4))).reshape(2, width * 2 * lane_tiles, 128)
        conv_view = conv_state.transpose(0, 2, 1, 3)
        vmem = pl.BlockSpec(memory_space=pltpu.VMEM)
        anywhere = pl.BlockSpec(memory_space=pl.ANY)
        hbm = pl.BlockSpec(memory_space=pltpu.HBM)
        f32, bf16 = jnp.float32, jnp.bfloat16
        r_val, conv_val, s0, s1 = pl.pallas_call(
            mamba_kernel,
            name="mamba",
            out_shape=[
                pltpu.VMEM((tokens, width), f32),
                pltpu.VMEM((2, 3, tokens, inner), bf16),
                pltpu.VMEM((tokens, state, inner), f32),
                pltpu.VMEM((tokens, state, inner), f32),
            ],
            in_specs=[hbm] * 13,
            out_specs=[vmem] * 4,
            scratch_shapes=[
                pltpu.VMEM((tokens, width), f32),
                pltpu.VMEM((2, width * 2 * lane_tiles, 128), bf16),
                pltpu.VMEM((2, width, 2 * inner), bf16),
                pltpu.VMEM((2, inner, width), bf16),
                pltpu.VMEM((2, tokens, inner), bf16),
                pltpu.VMEM(norm_w.shape, bf16),
                pltpu.VMEM(conv_w.shape, bf16),
                pltpu.VMEM(conv_b.shape, bf16),
                pltpu.VMEM(w_x.shape, bf16),
                pltpu.VMEM((2, 128, inner), bf16),
                pltpu.VMEM(b_dt.shape, f32),
                pltpu.VMEM(a_log.shape, f32),
                pltpu.VMEM(d_skip.shape, f32),
                pltpu.VMEM((tokens, width), bf16),
                pltpu.VMEM((tokens, inner), bf16),
                pltpu.VMEM((tokens, inner), f32),
                pltpu.VMEM((tokens, width), bf16),
                pltpu.VMEM((CHUNKS, half, width), bf16),
                pltpu.VMEM((CHUNKS, half // 2, width), bf16),
                pltpu.VMEM((CHUNKS, half // 2, width), bf16),
                pltpu.VMEM((CHUNKS, half // 2, width), bf16),
                pltpu.VMEM((CHUNKS, half // 2, width), f32),
                pltpu.VMEM((tokens, 128), f32),
                pltpu.VMEM((2, tokens, 128), bf16),
                pltpu.VMEM((4, tokens, 128), bf16),
                pltpu.VMEM((state, inner), f32),
                pltpu.VMEM((chunk, inner), f32),
                pltpu.VMEM((chunk, inner), f32),
                pltpu.VMEM((lane_tiles, chunk * 8, 128), f32),
                pltpu.VMEM((chunk, inner), bf16),
                pltpu.SemaphoreType.DMA((KINDS, 2, CHUNKS)),
                pltpu.SemaphoreType.DMA((KINDS, 2, CHUNKS)),
                pltpu.SemaphoreType.DMA((18 + CHUNKS,)),
                pltpu.SemaphoreType.DMA((8,)),
                pltpu.SemaphoreType.DMA((2, CHUNKS)),
            ],
            compiler_params=pltpu.CompilerParams(collective_id=0, has_side_effects=True, vmem_limit_bytes=32 * 2**20),
        )(residual, w_view, w_out, conv_view, ssm_state, norm_w, conv_w, conv_b, w_x, w_dt, b_dt, a_log, d_skip)
        r_new, conv_new, ssm_new = pl.pallas_call(
            dump_kernel,
            name="dump",
            out_shape=[
                jax.ShapeDtypeStruct((tokens, width), f32),
                jax.ShapeDtypeStruct((2, 3, tokens, inner), bf16),
                jax.ShapeDtypeStruct(ssm_state.shape, f32),
            ],
            in_specs=[anywhere] * 4,
            out_specs=[hbm] * 3,
            scratch_shapes=[pltpu.SemaphoreType.DMA((2 + 2 * DUMP_PIECES,))],
            compiler_params=pltpu.CompilerParams(vmem_limit_bytes=2**20),
        )(r_val, conv_val, s0, s1)
        return r_new, conv_new.transpose(0, 2, 1, 3), ssm_new

    cache_spec = P(None, 'dp', None, 'tp')
    in_specs = (P('dp', None), P(None, None), P(None, None, None, 'tp'), P(None, None, 'tp'), P(None, 'tp'), P(None, 'tp', None), P(None, None, 'tp'), P(None, 'tp'), P(None, None, 'tp'), P(None, 'tp'), P(None, 'tp', None), cache_spec, cache_spec)
    out_specs = (P('dp', None), cache_spec, cache_spec)
    return jax.shard_map(device_step, mesh=mesh, in_specs=in_specs, out_specs=out_specs, check_vma=False)
```

```python
import functools

import jax
import jax.numpy as jnp
from jax import lax
from jax.experimental.layout import Layout, with_layout_constraint
from jax.experimental import pallas as pl
from jax.experimental.pallas import tpu as pltpu
from jax.sharding import PartitionSpec as P

MESH = pl.DeviceIdType.MESH
LOG2E = 1.4426950408889634
SIZES = (64, 128, 128, 128, 64)
CHUNKS = len(SIZES)
STARTS = tuple(sum(SIZES[:q]) for q in range(CHUNKS))
LARGEST = max(SIZES)
KINDS = 10
ORDER = (0, 1, 0, 1, 5, 0, 2, 1, 3, 5, 5, 2, 4, 5, 5, 2, 4, 3, 3, 0, 1, 4, 0, 2, 1, 3, 0, 2, 5, 4, 3, 1, 0, 4, 2, 3, 1, 4, 0, 2, 0, 3, 1, 4, 1, 0, 2, 1, 0, 3, 1, 4, 2, 2, 3, 3, 2, 4, 0, 3, 4, 1, 4, 0, 2, 1, 3, 2, 0, 4, 3, 4, 1, 2, 3, 0, 4, 1, 2, 3, 4, 0, 1, 0, 2, 3, 4, 1, 2, 3, 4)

W_PIECES = 3
GROUP = 32
DUMP_PIECES = 4
ORDER_FIRST = tuple(dict.fromkeys(q for q in ORDER if q < CHUNKS))


def rms_scale(vector, epsilon):
    return lax.rsqrt(jnp.mean(vector * vector, axis=-1, keepdims=True) + epsilon)


def mamba_kernel(
    residual, w_in, w_out, conv_state, ssm_state, norm_w_hbm, conv_w_hbm, conv_b_hbm, w_x_hbm, w_dt_hbm, b_dt_hbm, a_log_hbm, d_skip_hbm,
    r_out, conv_out, ssm0, ssm1,
    res, w_raw, w_xz, wo, conv_old, norm_w, conv_w, conv_b, w_x, w_dt, b_dt, a_log, d_skip, hid, xc_buf, z_buf, part, half_in, quart_in, quart_sum, pair_in, o_acc,
    p_acc, p_send, p_recv, rate_buf, dt_buf, dx_buf, y_part, yg_buf, send_sem, recv_sem, load_sem, small_sem, state_sem,
):
    layers = 2
    tokens, width = res.shape
    inner = wo.shape[1]
    rank = w_dt_hbm.shape[1]
    state = a_log.shape[1]
    lane_tiles = inner // 128
    ssm_bufs = (ssm0, ssm1)

    tp = lax.axis_index("tp")
    core = lax.rem(tp, 2)
    pos_x = lax.rem(lax.div(tp, 2), 2)
    pos_y = lax.div(tp, 4)
    bit_a = pos_x * (1 - core) + pos_y * core
    bit_b = pos_y * (1 - core) + pos_x * core
    peer_c = tp + 1 - 2 * core
    peer_a = tp + (1 - 2 * bit_a) * (2 + 2 * core)
    peer_b = tp + (1 - 2 * bit_b) * (4 - 2 * core)
    peer_d = tp + (1 - 2 * pos_x) * 2 + (1 - 2 * pos_y) * 4
    peers = (peer_c, peer_a, peer_b, peer_d)

    barrier = pltpu.get_barrier_semaphore()
    for peer in peers:
        pl.semaphore_signal(barrier, inc=1, device_id={"tp": peer}, device_id_type=MESH)

    def rows_of(q):
        return pl.ds(STARTS[q], SIZES[q])

    def half_rows(q, which):
        half = SIZES[q] // 2
        return pl.ds(pl.multiple_of(STARTS[q] + which * half, half), half)

    def quart_rows(q, which_half, which):
        quart = SIZES[q] // 4
        return pl.ds(pl.multiple_of(STARTS[q] + which_half * (2 * quart) + which * quart, quart), quart)

    def landing(ref, q, parts):
        return ref.at[pl.ds(STARTS[q] // parts, SIZES[q] // parts)]

    def remote(kind, layer, q, src, dst, peer):
        return pltpu.make_async_remote_copy(
            src_ref=src, dst_ref=dst, send_sem=send_sem.at[kind, layer, q], recv_sem=recv_sem.at[kind, layer, q],
            device_id={"tp": peer}, device_id_type=MESH,
        )

    def p_copy(step, layer, q):
        src = p_send.at[min(step, 1), rows_of(q)]
        return remote(step, layer, q, src, p_recv.at[step, rows_of(q)], peers[step])

    def o_copy(step, layer, q):
        if step == 0:
            return remote(4, layer, q, part.at[half_rows(q, 1 - core)], landing(half_in, q, 2), peer_c)
        if step == 1:
            return remote(5, layer, q, part.at[quart_rows(q, core, 1 - bit_a)], landing(quart_in, q, 4), peer_a)
        return remote(6, layer, q, landing(quart_sum, q, 4), landing(pair_in, q, 4), peer_b)

    def h_copy(step, layer, q):
        ref = hid.at[quart_rows(q, core, 1 - bit_a if step == 2 else bit_a)]
        return remote(7 + step, layer, q, ref, ref, peer_a if step == 0 else peer_c)

    def w_load(layer, piece):
        rows = pl.ds(piece * (w_raw.shape[1] // W_PIECES), w_raw.shape[1] // W_PIECES)
        return pltpu.make_async_copy(w_in.at[layer, rows], w_raw.at[layer, rows], load_sem.at[layer * W_PIECES + piece])

    def res_load(q):
        return pltpu.make_async_copy(residual.at[rows_of(q)], res.at[rows_of(q)], load_sem.at[18 + q])

    def wo_load(layer):
        return pltpu.make_async_copy(w_out.at[layer], wo.at[layer], load_sem.at[10 + layer])

    def conv_load(layer, row):
        dst = conv_old.at[layer] if row == 0 else conv_out.at[layer, row - 1]
        return pltpu.make_async_copy(conv_state.at[layer, row], dst, load_sem.at[12 + 3 * layer + row])

    def state_load(layer, q):
        return pltpu.make_async_copy(ssm_state.at[layer, rows_of(q)], ssm_bufs[layer].at[rows_of(q)], state_sem.at[layer, q])

    small = [
        pltpu.make_async_copy(norm_w_hbm, norm_w, small_sem.at[0]),
        pltpu.make_async_copy(conv_w_hbm, conv_w, small_sem.at[1]),
        pltpu.make_async_copy(conv_b_hbm, conv_b, small_sem.at[2]),
        pltpu.make_async_copy(w_x_hbm, w_x, small_sem.at[3]),
        pltpu.make_async_copy(w_dt_hbm, w_dt.at[:, pl.ds(0, rank)], small_sem.at[4]),
        pltpu.make_async_copy(b_dt_hbm, b_dt, small_sem.at[5]),
        pltpu.make_async_copy(a_log_hbm, a_log, small_sem.at[6]),
        pltpu.make_async_copy(d_skip_hbm, d_skip, small_sem.at[7]),
    ]
    small[0].start()
    res_load(ORDER[0]).start()
    for piece in range(W_PIECES):
        w_load(0, piece).start()
    for q in range(CHUNKS):
        if q != ORDER[0]:
            res_load(q).start()
    for row in range(3):
        conv_load(0, row).start()
    for copy in small[1:]:
        copy.start()
    for layer in range(layers):
        w_dt[layer, rank:] = jnp.zeros((128 - rank, inner), jnp.bfloat16)

    span = 32
    packed = span * lane_tiles * 2
    blocks = width // (2 * span)

    def split_weights(layer, first, count):
        row = lax.broadcasted_iota(jnp.int32, (packed, packed), 0)
        col = lax.broadcasted_iota(jnp.int32, (packed, packed), 1)
        group = lax.div(row, span)
        want = lax.rem(row, span) * (2 * lane_tiles) + lax.rem(group, lane_tiles) * 2 + lax.div(group, lane_tiles)
        pick = jnp.where(col == want, 1.0, 0.0).astype(jnp.bfloat16)

        @pl.loop(0, count // 4)
        def _(step):
            for i in range(4):
                block = first + step * 4 + i
                raw = [w_raw[layer, pl.ds(pl.multiple_of((2 * block + k) * packed, packed), packed), :] for k in range(2)]
                both = jnp.dot(pick, jnp.concatenate(raw, axis=1), preferred_element_type=jnp.float32).astype(jnp.bfloat16)
                for k in range(2):
                    dst = pl.ds(pl.multiple_of((2 * block + k) * span, span), span)
                    for tile in range(2 * lane_tiles):
                        w_xz[layer, dst, tile * 128:(tile + 1) * 128] = both[tile * span:(tile + 1) * span, k * 128:(k + 1) * 128]

    split_step = 4

    def first_norm(q):
        res_load(q).wait()

        @pl.loop(0, SIZES[q] // 32)
        def _(i):
            sub = pl.ds(pl.multiple_of(STARTS[q] + i * 32, 32), 32)
            r = res[sub, :]
            hid[sub, :] = (r * rms_scale(r, 1e-5) * norm_w[0:1, :].astype(jnp.float32)).astype(jnp.bfloat16)

    small[0].wait()
    first_norm(ORDER[0])

    for piece in range(W_PIECES):
        w_load(0, piece).wait()
        split_weights(0, piece * (blocks // W_PIECES), blocks // W_PIECES)

    for piece in range(W_PIECES):
        w_load(1, piece).start()
    for q in ORDER_FIRST:
        state_load(0, q).start()
    wo_load(0).start()
    for row in range(3):
        conv_load(0, row).wait()
    for copy in small[1:]:
        copy.wait()
    pl.semaphore_wait(barrier, 4)

    wo_ready = [False] * layers

    def stage_in(layer, q):
        rows = rows_of(q)
        if layer == 0:
            if q != ORDER[0]:
                first_norm(q)
        else:
            h_copy(1, layer - 1, q).wait()
            h_copy(2, layer - 1, q).wait()
        x_val = jnp.dot(hid[rows, :], w_xz[layer, :, :inner], preferred_element_type=jnp.float32).astype(jnp.bfloat16)
        conv_out[layer, 2, rows, :] = x_val
        taps = conv_w[layer].astype(jnp.float32)
        pre = conv_old[layer, rows, :].astype(jnp.float32) * taps[0:1]
        pre = pre + conv_out[layer, 0, rows, :].astype(jnp.float32) * taps[1:2]
        pre = pre + conv_out[layer, 1, rows, :].astype(jnp.float32) * taps[2:3]
        pre = pre + x_val.astype(jnp.float32) * taps[3:4]
        pre = pre + conv_b[layer:layer + 1, :].astype(jnp.float32)
        xc = (pre * jax.nn.sigmoid(pre)).astype(jnp.bfloat16)
        xc_buf[rows, :] = xc
        p = jnp.dot(xc, w_x[layer], preferred_element_type=jnp.float32)
        p_acc[rows, :] = p
        p_send[0, rows, :] = p.astype(jnp.bfloat16)
        p_copy(0, layer, q).start()

    def stage_z(layer, q):
        rows = rows_of(q)
        z = jnp.dot(hid[rows, :], w_xz[layer, :, inner:], preferred_element_type=jnp.float32).astype(jnp.bfloat16).astype(jnp.float32)
        z_buf[rows, :] = z * jax.nn.sigmoid(z)

    def stage_p(layer, q):
        rows = rows_of(q)
        p_copy(0, layer, q).wait()
        p = p_acc[rows, :] + p_recv[0, rows, :].astype(jnp.float32)
        p_acc[rows, :] = p
        p_send[1, rows, :] = p.astype(jnp.bfloat16)
        for step in (3, 1, 2):
            p_copy(step, layer, q).start()

    def stage_ssm(layer, q):
        rows, start, chunk = rows_of(q), STARTS[q], SIZES[q]
        state_buf = ssm_bufs[layer]
        p = p_acc[rows, :]
        for step in (1, 2, 3):
            p_copy(step, layer, q).wait()
            p = p + p_recv[step, rows, :].astype(jnp.float32)
        lane = lax.broadcasted_iota(jnp.int32, p.shape, 1)
        square = p * p
        is_dt = lane < rank
        is_b = jnp.logical_and(lane >= rank, lane < rank + state)

        def scale_of(mask, count):
            total = jnp.sum(jnp.where(mask, square, 0.0), axis=1, keepdims=True)
            return lax.rsqrt(total * (1.0 / count) + 1e-6)

        scale_dt = scale_of(is_dt, rank)
        scale_b = scale_of(is_b, state)
        scale_c = scale_of(lane >= rank + state, state)
        normed = p * jnp.where(is_dt, scale_dt, jnp.where(is_b, scale_b, scale_c))
        dt_low = jnp.where(is_dt, normed, 0.0).astype(jnp.bfloat16)
        pre = jnp.dot(dt_low, w_dt[layer], preferred_element_type=jnp.float32) + b_dt[layer:layer + 1, :]
        dt = jnp.maximum(pre, 0.0) + jnp.log1p(jnp.exp(-jnp.abs(pre)))
        dt_buf[:chunk] = dt
        dx_buf[:chunk] = dt * xc_buf[rows, :].astype(jnp.float32)
        turned = jnp.concatenate([normed] * (128 // chunk), axis=0).T
        b_cols = turned[rank:rank + state, :]
        c_cols = turned[rank + state:, :]
        rate_buf[...] = jnp.exp(a_log[layer]) * (-LOG2E)
        state_load(layer, q).wait()

        def scan_group(g, carry):
            b_now, c_now = carry
            first = pl.multiple_of(g * GROUP, GROUP)
            states = state_buf.at[pl.ds(start + first, GROUP)]
            dts = dt_buf.at[pl.ds(first, GROUP)]
            dxs = dx_buf.at[pl.ds(first, GROUP)]
            ys = [y_part.at[tile, pl.ds(pl.multiple_of(first * 8, 8 * GROUP), 8 * GROUP)] for tile in range(lane_tiles)]
            for j in range(GROUP):
                new = jnp.exp2(dts[j:j + 1] * rate_buf[...]) * states[j] + dxs[j:j + 1] * b_now[:, j:j + 1]
                states[j] = new
                weighted = new * c_now[:, j:j + 1]
                partial = weighted[:8] + weighted[8:]
                for tile in range(lane_tiles):
                    ys[tile][j * 8:(j + 1) * 8] = partial[:, tile * 128:(tile + 1) * 128]
            return pltpu.roll(b_now, 128 - GROUP, 1), pltpu.roll(c_now, 128 - GROUP, 1)

        lax.fori_loop(0, chunk // GROUP, scan_group, (b_cols, c_cols))

        @pl.loop(0, chunk // 16)
        def _(g):
            halves = []
            for k in range(2):
                first = g * 128 + k * 64
                by_tile = []
                for tile in range(lane_tiles):
                    total = y_part[tile, pl.ds(first, 8, stride=8), :]
                    for step in range(1, 8):
                        total = total + y_part[tile, pl.ds(first + step, 8, stride=8), :]
                    by_tile.append(total)
                halves.append(jnp.concatenate(by_tile, axis=1))
            sub = pl.ds(pl.multiple_of(g * 16, 16), 16)
            sub_rows = pl.ds(pl.multiple_of(start + g * 16, 16), 16)
            y = jnp.concatenate(halves, axis=0) + d_skip[layer:layer + 1, :] * xc_buf[sub_rows, :].astype(jnp.float32)
            yg_buf[sub, :] = (y * z_buf[sub_rows, :]).astype(jnp.bfloat16)

        if not wo_ready[layer]:
            wo_load(layer).wait()
            wo_ready[layer] = True
        part[rows, :] = jnp.dot(yg_buf[:chunk], wo[layer], preferred_element_type=jnp.float32).astype(jnp.bfloat16)
        o_copy(0, layer, q).start()

    def stage_half(layer, q):
        o_copy(0, layer, q).wait()
        mine = half_rows(q, core)
        part[mine, :] = (part[mine, :].astype(jnp.float32) + half_in[pl.ds(STARTS[q] // 2, SIZES[q] // 2), :].astype(jnp.float32)).astype(jnp.bfloat16)
        o_copy(1, layer, q).start()

    def stage_quart(layer, q):
        o_copy(1, layer, q).wait()
        mine = part[quart_rows(q, core, bit_a), :]
        quarter = pl.ds(STARTS[q] // 4, SIZES[q] // 4)
        quart_sum[quarter, :] = (mine.astype(jnp.float32) + quart_in[quarter, :].astype(jnp.float32)).astype(jnp.bfloat16)
        o_copy(2, layer, q).start()

    def stage_own(layer, q):
        o_copy(2, layer, q).wait()
        quart = SIZES[q] // 4
        for i in range(quart // 16):
            sub = pl.ds(STARTS[q] // 4 + i * 16, 16)
            dst = pl.ds(pl.multiple_of(STARTS[q] + core * (2 * quart) + bit_a * quart + i * 16, 16), 16)
            o_val = quart_sum[sub, :].astype(jnp.float32) + pair_in[sub, :].astype(jnp.float32)
            if layer == 0:
                o_acc[sub, :] = o_val
                r = res[dst, :] + o_val
                hid[dst, :] = (r * rms_scale(r, 1e-5) * norm_w[1:2, :].astype(jnp.float32)).astype(jnp.bfloat16)
            else:
                hid[dst, :] = (o_acc[sub, :] + o_val).astype(jnp.bfloat16)
        h_copy(0, layer, q).start()
        h_copy(1, layer, q).start()

    def stage_forward(layer, q):
        h_copy(0, layer, q).wait()
        h_copy(2, layer, q).start()

    def stage_out(q):
        h_copy(1, layers - 1, q).wait()
        h_copy(2, layers - 1, q).wait()
        rows = rows_of(q)
        r_out[rows, :] = res[rows, :] + hid[rows, :].astype(jnp.float32)

    stages = []
    for layer in range(layers):
        stages.append(functools.partial(stage_in, layer))
        stages.append(functools.partial(stage_z, layer))
        stages.append(functools.partial(stage_p, layer))
        stages.append(functools.partial(stage_ssm, layer))
        stages.append(functools.partial(stage_half, layer))
        stages.append(functools.partial(stage_quart, layer))
        stages.append(functools.partial(stage_own, layer))
        stages.append(functools.partial(stage_forward, layer))
    stages.append(stage_out)

    per_layer = len(stages) // layers
    progress = [0] * CHUNKS
    second_ready = False
    fills = 0
    for q in ORDER:
        if q == CHUNKS:
            if fills == 0:
                for piece in range(W_PIECES):
                    w_load(1, piece).wait()
                for row in range(3):
                    conv_load(1, row).start()
                wo_load(1).start()
                for chunk_index in ORDER_FIRST:
                    state_load(1, chunk_index).start()
            split_weights(1, fills * split_step, split_step)
            fills += 1
        else:
            if progress[q] == per_layer and not second_ready:
                for row in range(3):
                    conv_load(1, row).wait()
                second_ready = True
            stages[progress[q]](q)
            progress[q] += 1


def dump_kernel(r_val, conv_val, ssm0, ssm1, r_hbm, conv_hbm, ssm_hbm, sems):
    copies = [pltpu.make_async_copy(r_val, r_hbm, sems.at[0]), pltpu.make_async_copy(conv_val, conv_hbm, sems.at[1])]
    piece = ssm0.shape[0] // DUMP_PIECES
    for i in range(DUMP_PIECES):
        for layer, ssm in enumerate((ssm0, ssm1)):
            rows = pl.ds(i * piece, piece)
            copies.append(pltpu.make_async_copy(ssm.at[rows], ssm_hbm.at[layer, rows], sems.at[2 + 2 * i + layer]))
    for copy in copies:
        copy.start()
    for copy in copies:
        copy.wait()


def solution(mesh):
    def device_step(residual, norm_w, w_in, conv_w, conv_b, w_x, w_dt, b_dt, a_log, d_skip, w_out, conv_state, ssm_state):
        tokens, width = residual.shape
        inner = w_out.shape[1]
        state = a_log.shape[1]
        lane_tiles = inner // 128
        w_view = w_in.reshape(2, width, 2, lane_tiles, 128).transpose(0, 1, 3, 2, 4)
        w_view = with_layout_constraint(w_view, Layout(major_to_minor=(0, 1, 2, 3, 4))).reshape(2, width * 2 * lane_tiles, 128)
        conv_view = conv_state.transpose(0, 2, 1, 3)
        vmem = pl.BlockSpec(memory_space=pltpu.VMEM)
        anywhere = pl.BlockSpec(memory_space=pl.ANY)
        hbm = pl.BlockSpec(memory_space=pltpu.HBM)
        f32, bf16 = jnp.float32, jnp.bfloat16
        r_val, conv_val, s0, s1 = pl.pallas_call(
            mamba_kernel,
            name="mamba",
            out_shape=[
                pltpu.VMEM((tokens, width), f32),
                pltpu.VMEM((2, 3, tokens, inner), bf16),
                pltpu.VMEM((tokens, state, inner), f32),
                pltpu.VMEM((tokens, state, inner), f32),
            ],
            in_specs=[hbm] * 13,
            out_specs=[vmem] * 4,
            scratch_shapes=[
                pltpu.VMEM((tokens, width), f32),
                pltpu.VMEM((2, width * 2 * lane_tiles, 128), bf16),
                pltpu.VMEM((2, width, 2 * inner), bf16),
                pltpu.VMEM((2, inner, width), bf16),
                pltpu.VMEM((2, tokens, inner), bf16),
                pltpu.VMEM(norm_w.shape, bf16),
                pltpu.VMEM(conv_w.shape, bf16),
                pltpu.VMEM(conv_b.shape, bf16),
                pltpu.VMEM(w_x.shape, bf16),
                pltpu.VMEM((2, 128, inner), bf16),
                pltpu.VMEM(b_dt.shape, f32),
                pltpu.VMEM(a_log.shape, f32),
                pltpu.VMEM(d_skip.shape, f32),
                pltpu.VMEM((tokens, width), bf16),
                pltpu.VMEM((tokens, inner), bf16),
                pltpu.VMEM((tokens, inner), f32),
                pltpu.VMEM((tokens, width), bf16),
                pltpu.VMEM((tokens // 2, width), bf16),
                pltpu.VMEM((tokens // 4, width), bf16),
                pltpu.VMEM((tokens // 4, width), bf16),
                pltpu.VMEM((tokens // 4, width), bf16),
                pltpu.VMEM((tokens // 4, width), f32),
                pltpu.VMEM((tokens, 128), f32),
                pltpu.VMEM((2, tokens, 128), bf16),
                pltpu.VMEM((4, tokens, 128), bf16),
                pltpu.VMEM((state, inner), f32),
                pltpu.VMEM((LARGEST, inner), f32),
                pltpu.VMEM((LARGEST, inner), f32),
                pltpu.VMEM((lane_tiles, LARGEST * 8, 128), f32),
                pltpu.VMEM((LARGEST, inner), bf16),
                pltpu.SemaphoreType.DMA((KINDS, 2, CHUNKS)),
                pltpu.SemaphoreType.DMA((KINDS, 2, CHUNKS)),
                pltpu.SemaphoreType.DMA((18 + CHUNKS,)),
                pltpu.SemaphoreType.DMA((8,)),
                pltpu.SemaphoreType.DMA((2, CHUNKS)),
            ],
            compiler_params=pltpu.CompilerParams(collective_id=0, has_side_effects=True, vmem_limit_bytes=32 * 2**20),
        )(residual, w_view, w_out, conv_view, ssm_state, norm_w, conv_w, conv_b, w_x, w_dt, b_dt, a_log, d_skip)
        r_new, conv_new, ssm_new = pl.pallas_call(
            dump_kernel,
            name="dump",
            out_shape=[
                jax.ShapeDtypeStruct((tokens, width), f32),
                jax.ShapeDtypeStruct((2, 3, tokens, inner), bf16),
                jax.ShapeDtypeStruct(ssm_state.shape, f32),
            ],
            in_specs=[anywhere] * 4,
            out_specs=[hbm] * 3,
            scratch_shapes=[pltpu.SemaphoreType.DMA((2 + 2 * DUMP_PIECES,))],
            compiler_params=pltpu.CompilerParams(vmem_limit_bytes=2**20),
        )(r_val, conv_val, s0, s1)
        return r_new, conv_new.transpose(0, 2, 1, 3), ssm_new

    cache_spec = P(None, 'dp', None, 'tp')
    in_specs = (P('dp', None), P(None, None), P(None, None, None, 'tp'), P(None, None, 'tp'), P(None, 'tp'), P(None, 'tp', None), P(None, None, 'tp'), P(None, 'tp'), P(None, None, 'tp'), P(None, 'tp'), P(None, 'tp', None), cache_spec, cache_spec)
    out_specs = (P('dp', None), cache_spec, cache_spec)
    return jax.shard_map(device_step, mesh=mesh, in_specs=in_specs, out_specs=out_specs, check_vma=False)
```

```python
import functools

import jax
import jax.numpy as jnp
from jax import lax
from jax.experimental.layout import Layout, with_layout_constraint
from jax.experimental import pallas as pl
from jax.experimental.pallas import tpu as pltpu
from jax.sharding import PartitionSpec as P

MESH = pl.DeviceIdType.MESH
LOG2E = 1.4426950408889634
SIZES = (64, 128, 128, 128, 64)
CHUNKS = len(SIZES)
STARTS = tuple(sum(SIZES[:q]) for q in range(CHUNKS))
LARGEST = max(SIZES)
KINDS = 10
ORDER = (0, 1, 3, 0, 2, 1, 4, 2, 3, 0, 1, 4, 0, 2, 1, 3, 5, 0, 5, 2, 4, 3, 1, 5, 4, 5, 0, 5, 2, 3, 5, 1, 4, 0, 2, 3, 1, 0, 4, 1, 2, 0, 3, 1, 2, 3, 4, 2, 0, 4, 3, 1, 4, 0, 2, 1, 3, 2, 0, 4, 3, 4, 1, 2, 3, 0, 4, 1, 2, 3, 4, 1, 2, 3, 0, 4, 3, 0, 1, 2, 4)

W_PIECES = 3
GROUPS = {64: 16, 128: 64}
DUMP_PIECES = 4
ORDER_FIRST = tuple(dict.fromkeys(q for q in ORDER if q < CHUNKS))


def rms_scale(vector, epsilon):
    return lax.rsqrt(jnp.mean(vector * vector, axis=-1, keepdims=True) + epsilon)


def mamba_kernel(
    residual, w_in, w_out, conv_state, ssm_state, norm_w_hbm, conv_w_hbm, conv_b_hbm, w_x_hbm, w_dt_hbm, b_dt_hbm, a_log_hbm, d_skip_hbm,
    r_out, conv_out, ssm0, ssm1,
    res, w_raw, w_xz, wo, conv_old, norm_w, conv_w, conv_b, w_x, w_dt, b_dt, a_log, d_skip, hid, xc_buf, z_buf, part, half_in, quart_in, quart_sum, pair_in, o_acc,
    p_acc, p_send, p_recv, dt_buf, dx_buf, y_part, yg_buf, send_sem, recv_sem, load_sem, small_sem, state_sem,
):
    layers = 2
    tokens, width = res.shape
    inner = wo.shape[1]
    rank = w_dt_hbm.shape[1]
    state = a_log.shape[1]
    lane_tiles = inner // 128
    ssm_bufs = (ssm0, ssm1)

    tp = lax.axis_index("tp")
    core = lax.rem(tp, 2)
    pos_x = lax.rem(lax.div(tp, 2), 2)
    pos_y = lax.div(tp, 4)
    bit_a = pos_x * (1 - core) + pos_y * core
    bit_b = pos_y * (1 - core) + pos_x * core
    peer_c = tp + 1 - 2 * core
    peer_a = tp + (1 - 2 * bit_a) * (2 + 2 * core)
    peer_b = tp + (1 - 2 * bit_b) * (4 - 2 * core)
    peer_d = tp + (1 - 2 * pos_x) * 2 + (1 - 2 * pos_y) * 4
    peers = (peer_c, peer_a, peer_b, peer_d)

    barrier = pltpu.get_barrier_semaphore()
    for peer in peers:
        pl.semaphore_signal(barrier, inc=1, device_id={"tp": peer}, device_id_type=MESH)

    def rows_of(q):
        return pl.ds(STARTS[q], SIZES[q])

    def half_rows(q, which):
        half = SIZES[q] // 2
        return pl.ds(pl.multiple_of(STARTS[q] + which * half, half), half)

    def quart_rows(q, which_half, which):
        quart = SIZES[q] // 4
        return pl.ds(pl.multiple_of(STARTS[q] + which_half * (2 * quart) + which * quart, quart), quart)

    def landing(ref, q, parts):
        return ref.at[pl.ds(STARTS[q] // parts, SIZES[q] // parts)]

    def remote(kind, layer, q, src, dst, peer):
        return pltpu.make_async_remote_copy(
            src_ref=src, dst_ref=dst, send_sem=send_sem.at[kind, layer, q], recv_sem=recv_sem.at[kind, layer, q],
            device_id={"tp": peer}, device_id_type=MESH,
        )

    def p_copy(step, layer, q):
        src = p_send.at[min(step, 1), rows_of(q)]
        return remote(step, layer, q, src, p_recv.at[step, rows_of(q)], peers[step])

    def o_copy(step, layer, q):
        if step == 0:
            return remote(4, layer, q, part.at[half_rows(q, 1 - core)], landing(half_in, q, 2), peer_c)
        if step == 1:
            return remote(5, layer, q, part.at[quart_rows(q, core, 1 - bit_a)], landing(quart_in, q, 4), peer_a)
        return remote(6, layer, q, landing(quart_sum, q, 4), landing(pair_in, q, 4), peer_b)

    def h_copy(step, layer, q):
        ref = hid.at[quart_rows(q, core, 1 - bit_a if step == 2 else bit_a)]
        return remote(7 + step, layer, q, ref, ref, peer_a if step == 0 else peer_c)

    def w_load(layer, piece):
        rows = pl.ds(piece * (w_raw.shape[1] // W_PIECES), w_raw.shape[1] // W_PIECES)
        return pltpu.make_async_copy(w_in.at[layer, rows], w_raw.at[layer, rows], load_sem.at[layer * W_PIECES + piece])

    def res_load(q):
        return pltpu.make_async_copy(residual.at[rows_of(q)], res.at[rows_of(q)], load_sem.at[18 + q])

    def wo_load(layer):
        return pltpu.make_async_copy(w_out.at[layer], wo.at[layer], load_sem.at[10 + layer])

    def conv_load(layer, row):
        dst = conv_old.at[layer] if row == 0 else conv_out.at[layer, row - 1]
        return pltpu.make_async_copy(conv_state.at[layer, row], dst, load_sem.at[12 + 3 * layer + row])

    def state_load(layer, q):
        return pltpu.make_async_copy(ssm_state.at[layer, rows_of(q)], ssm_bufs[layer].at[rows_of(q)], state_sem.at[layer, q])

    small = [
        pltpu.make_async_copy(norm_w_hbm, norm_w, small_sem.at[0]),
        pltpu.make_async_copy(conv_w_hbm, conv_w, small_sem.at[1]),
        pltpu.make_async_copy(conv_b_hbm, conv_b, small_sem.at[2]),
        pltpu.make_async_copy(w_x_hbm, w_x, small_sem.at[3]),
        pltpu.make_async_copy(w_dt_hbm, w_dt.at[:, pl.ds(0, rank)], small_sem.at[4]),
        pltpu.make_async_copy(b_dt_hbm, b_dt, small_sem.at[5]),
        pltpu.make_async_copy(a_log_hbm, a_log, small_sem.at[6]),
        pltpu.make_async_copy(d_skip_hbm, d_skip, small_sem.at[7]),
    ]
    small[0].start()
    res_load(ORDER[0]).start()
    for piece in range(W_PIECES):
        w_load(0, piece).start()
    for q in range(CHUNKS):
        if q != ORDER[0]:
            res_load(q).start()
    for row in range(3):
        conv_load(0, row).start()
    for copy in small[1:]:
        copy.start()
    for layer in range(layers):
        w_dt[layer, rank:] = jnp.zeros((128 - rank, inner), jnp.bfloat16)

    span = 32
    packed = span * lane_tiles * 2
    blocks = width // (2 * span)

    def split_weights(layer, first, count):
        row = lax.broadcasted_iota(jnp.int32, (packed, packed), 0)
        col = lax.broadcasted_iota(jnp.int32, (packed, packed), 1)
        group = lax.div(row, span)
        want = lax.rem(row, span) * (2 * lane_tiles) + lax.rem(group, lane_tiles) * 2 + lax.div(group, lane_tiles)
        pick = jnp.where(col == want, 1.0, 0.0).astype(jnp.bfloat16)

        @pl.loop(0, count // 4)
        def _(step):
            for i in range(4):
                block = first + step * 4 + i
                raw = [w_raw[layer, pl.ds(pl.multiple_of((2 * block + k) * packed, packed), packed), :] for k in range(2)]
                both = jnp.dot(pick, jnp.concatenate(raw, axis=1), preferred_element_type=jnp.float32).astype(jnp.bfloat16)
                for k in range(2):
                    dst = pl.ds(pl.multiple_of((2 * block + k) * span, span), span)
                    for tile in range(2 * lane_tiles):
                        w_xz[layer, dst, tile * 128:(tile + 1) * 128] = both[tile * span:(tile + 1) * span, k * 128:(k + 1) * 128]

    split_step = 4

    def first_norm(q):
        res_load(q).wait()

        @pl.loop(0, SIZES[q] // 32)
        def _(i):
            sub = pl.ds(pl.multiple_of(STARTS[q] + i * 32, 32), 32)
            r = res[sub, :]
            hid[sub, :] = (r * rms_scale(r, 1e-5) * norm_w[0:1, :].astype(jnp.float32)).astype(jnp.bfloat16)

    small[0].wait()
    first_norm(ORDER[0])

    for piece in range(W_PIECES):
        w_load(0, piece).wait()
        split_weights(0, piece * (blocks // W_PIECES), blocks // W_PIECES)

    for piece in range(W_PIECES):
        w_load(1, piece).start()
    for q in ORDER_FIRST:
        state_load(0, q).start()
    wo_load(0).start()
    for row in range(3):
        conv_load(0, row).wait()
    for copy in small[1:]:
        copy.wait()
    pl.semaphore_wait(barrier, 4)

    wo_ready = [False] * layers

    def stage_in(layer, q):
        rows = rows_of(q)
        if layer == 0:
            if q != ORDER[0]:
                first_norm(q)
        else:
            h_copy(1, layer - 1, q).wait()
            h_copy(2, layer - 1, q).wait()
        xz = jnp.dot(hid[rows, :], w_xz[layer], preferred_element_type=jnp.float32).astype(jnp.bfloat16)
        x_val = xz[:, :inner]
        z = xz[:, inner:].astype(jnp.float32)
        z_buf[rows, :] = z * jax.nn.sigmoid(z)
        conv_out[layer, 2, rows, :] = x_val
        taps = conv_w[layer].astype(jnp.float32)
        pre = conv_old[layer, rows, :].astype(jnp.float32) * taps[0:1]
        pre = pre + conv_out[layer, 0, rows, :].astype(jnp.float32) * taps[1:2]
        pre = pre + conv_out[layer, 1, rows, :].astype(jnp.float32) * taps[2:3]
        pre = pre + x_val.astype(jnp.float32) * taps[3:4]
        pre = pre + conv_b[layer:layer + 1, :].astype(jnp.float32)
        xc = (pre * jax.nn.sigmoid(pre)).astype(jnp.bfloat16)
        xc_buf[rows, :] = xc
        p = jnp.dot(xc, w_x[layer], preferred_element_type=jnp.float32)
        p_acc[rows, :] = p
        p_send[0, rows, :] = p.astype(jnp.bfloat16)
        p_copy(0, layer, q).start()

    def stage_p(layer, q):
        rows = rows_of(q)
        p_copy(0, layer, q).wait()
        p = p_acc[rows, :] + p_recv[0, rows, :].astype(jnp.float32)
        p_acc[rows, :] = p
        p_send[1, rows, :] = p.astype(jnp.bfloat16)
        for step in (3, 1, 2):
            p_copy(step, layer, q).start()

    def stage_ssm(layer, q):
        rows, start, chunk = rows_of(q), STARTS[q], SIZES[q]
        state_buf = ssm_bufs[layer]
        p = p_acc[rows, :]
        for step in (1, 2, 3):
            p_copy(step, layer, q).wait()
            p = p + p_recv[step, rows, :].astype(jnp.float32)
        lane = lax.broadcasted_iota(jnp.int32, p.shape, 1)
        square = p * p
        is_dt = lane < rank
        is_b = jnp.logical_and(lane >= rank, lane < rank + state)

        def scale_of(mask, count):
            total = jnp.sum(jnp.where(mask, square, 0.0), axis=1, keepdims=True)
            return lax.rsqrt(total * (1.0 / count) + 1e-6)

        scale_dt = scale_of(is_dt, rank)
        scale_b = scale_of(is_b, state)
        scale_c = scale_of(lane >= rank + state, state)
        normed = p * jnp.where(is_dt, scale_dt, jnp.where(is_b, scale_b, scale_c))
        dt_low = jnp.where(is_dt, normed, 0.0).astype(jnp.bfloat16)
        pre = jnp.dot(dt_low, w_dt[layer], preferred_element_type=jnp.float32) + b_dt[layer:layer + 1, :]
        dt = jnp.maximum(pre, 0.0) + jnp.log1p(jnp.exp(-jnp.abs(pre)))
        dt_buf[:chunk] = dt
        dx_buf[:chunk] = dt * xc_buf[rows, :].astype(jnp.float32)
        turned = jnp.concatenate([normed] * (128 // chunk), axis=0).T
        b_cols = turned[rank:rank + state, :]
        c_cols = turned[rank + state:, :]
        state_load(layer, q).wait()

        group = GROUPS[chunk]
        rate = jnp.exp(a_log[layer]) * (-LOG2E)

        def scan_group(g, carry):
            b_now, c_now = carry
            first = pl.multiple_of(g * group, group)
            states = state_buf.at[pl.ds(start + first, group)]
            dts = dt_buf.at[pl.ds(first, group)]
            dxs = dx_buf.at[pl.ds(first, group)]
            ys = [y_part.at[tile, pl.ds(pl.multiple_of(first * 8, 8 * group), 8 * group)] for tile in range(lane_tiles)]
            for j in range(group):
                new = jnp.exp2(dts[j:j + 1] * rate) * states[j] + dxs[j:j + 1] * b_now[:, j:j + 1]
                states[j] = new
                weighted = new * c_now[:, j:j + 1]
                partial = weighted[:8] + weighted[8:]
                for tile in range(lane_tiles):
                    ys[tile][j * 8:(j + 1) * 8] = partial[:, tile * 128:(tile + 1) * 128]
            return pltpu.roll(b_now, 128 - group, 1), pltpu.roll(c_now, 128 - group, 1)

        lax.fori_loop(0, chunk // group, scan_group, (b_cols, c_cols))

        @pl.loop(0, chunk // 16)
        def _(g):
            halves = []
            for k in range(2):
                first = g * 128 + k * 64
                by_tile = []
                for tile in range(lane_tiles):
                    total = y_part[tile, pl.ds(first, 8, stride=8), :]
                    for step in range(1, 8):
                        total = total + y_part[tile, pl.ds(first + step, 8, stride=8), :]
                    by_tile.append(total)
                halves.append(jnp.concatenate(by_tile, axis=1))
            sub = pl.ds(pl.multiple_of(g * 16, 16), 16)
            sub_rows = pl.ds(pl.multiple_of(start + g * 16, 16), 16)
            y = jnp.concatenate(halves, axis=0) + d_skip[layer:layer + 1, :] * xc_buf[sub_rows, :].astype(jnp.float32)
            yg_buf[sub, :] = (y * z_buf[sub_rows, :]).astype(jnp.bfloat16)

        if not wo_ready[layer]:
            wo_load(layer).wait()
            wo_ready[layer] = True
        part[rows, :] = jnp.dot(yg_buf[:chunk], wo[layer], preferred_element_type=jnp.float32).astype(jnp.bfloat16)
        o_copy(0, layer, q).start()

    def stage_half(layer, q):
        o_copy(0, layer, q).wait()
        mine = half_rows(q, core)
        part[mine, :] = (part[mine, :].astype(jnp.float32) + half_in[pl.ds(STARTS[q] // 2, SIZES[q] // 2), :].astype(jnp.float32)).astype(jnp.bfloat16)
        o_copy(1, layer, q).start()

    def stage_quart(layer, q):
        o_copy(1, layer, q).wait()
        mine = part[quart_rows(q, core, bit_a), :]
        quarter = pl.ds(STARTS[q] // 4, SIZES[q] // 4)
        quart_sum[quarter, :] = (mine.astype(jnp.float32) + quart_in[quarter, :].astype(jnp.float32)).astype(jnp.bfloat16)
        o_copy(2, layer, q).start()

    def stage_own(layer, q):
        o_copy(2, layer, q).wait()
        quart = SIZES[q] // 4
        for i in range(quart // 16):
            sub = pl.ds(STARTS[q] // 4 + i * 16, 16)
            dst = pl.ds(pl.multiple_of(STARTS[q] + core * (2 * quart) + bit_a * quart + i * 16, 16), 16)
            o_val = quart_sum[sub, :].astype(jnp.float32) + pair_in[sub, :].astype(jnp.float32)
            if layer == 0:
                o_acc[sub, :] = o_val
                r = res[dst, :] + o_val
                hid[dst, :] = (r * rms_scale(r, 1e-5) * norm_w[1:2, :].astype(jnp.float32)).astype(jnp.bfloat16)
            else:
                hid[dst, :] = (o_acc[sub, :] + o_val).astype(jnp.bfloat16)
        h_copy(0, layer, q).start()
        h_copy(1, layer, q).start()

    def stage_forward(layer, q):
        h_copy(0, layer, q).wait()
        h_copy(2, layer, q).start()

    def stage_out(q):
        h_copy(1, layers - 1, q).wait()
        h_copy(2, layers - 1, q).wait()
        rows = rows_of(q)
        r_out[rows, :] = res[rows, :] + hid[rows, :].astype(jnp.float32)

    stages = []
    for layer in range(layers):
        stages.append(functools.partial(stage_in, layer))
        stages.append(functools.partial(stage_p, layer))
        stages.append(functools.partial(stage_ssm, layer))
        stages.append(functools.partial(stage_half, layer))
        stages.append(functools.partial(stage_quart, layer))
        stages.append(functools.partial(stage_own, layer))
        stages.append(functools.partial(stage_forward, layer))
    stages.append(stage_out)

    per_layer = len(stages) // layers
    progress = [0] * CHUNKS
    second_ready = False
    fills = 0
    for q in ORDER:
        if q == CHUNKS:
            if fills == 0:
                for piece in range(W_PIECES):
                    w_load(1, piece).wait()
                for row in range(3):
                    conv_load(1, row).start()
                wo_load(1).start()
                for chunk_index in ORDER_FIRST:
                    state_load(1, chunk_index).start()
            split_weights(1, fills * split_step, split_step)
            fills += 1
        else:
            if progress[q] == per_layer and not second_ready:
                for row in range(3):
                    conv_load(1, row).wait()
                second_ready = True
            stages[progress[q]](q)
            progress[q] += 1


def dump_kernel(r_val, conv_val, ssm0, ssm1, r_hbm, conv_hbm, ssm_hbm, sems):
    copies = [pltpu.make_async_copy(r_val, r_hbm, sems.at[0]), pltpu.make_async_copy(conv_val, conv_hbm, sems.at[1])]
    piece = ssm0.shape[0] // DUMP_PIECES
    for i in range(DUMP_PIECES):
        for layer, ssm in enumerate((ssm0, ssm1)):
            rows = pl.ds(i * piece, piece)
            copies.append(pltpu.make_async_copy(ssm.at[rows], ssm_hbm.at[layer, rows], sems.at[2 + 2 * i + layer]))
    for copy in copies:
        copy.start()
    for copy in copies:
        copy.wait()


def solution(mesh):
    def device_step(residual, norm_w, w_in, conv_w, conv_b, w_x, w_dt, b_dt, a_log, d_skip, w_out, conv_state, ssm_state):
        tokens, width = residual.shape
        inner = w_out.shape[1]
        state = a_log.shape[1]
        lane_tiles = inner // 128
        w_view = w_in.reshape(2, width, 2, lane_tiles, 128).transpose(0, 1, 3, 2, 4)
        w_view = with_layout_constraint(w_view, Layout(major_to_minor=(0, 1, 2, 3, 4))).reshape(2, width * 2 * lane_tiles, 128)
        conv_view = conv_state.transpose(0, 2, 1, 3)
        vmem = pl.BlockSpec(memory_space=pltpu.VMEM)
        anywhere = pl.BlockSpec(memory_space=pl.ANY)
        hbm = pl.BlockSpec(memory_space=pltpu.HBM)
        f32, bf16 = jnp.float32, jnp.bfloat16
        r_val, conv_val, s0, s1 = pl.pallas_call(
            mamba_kernel,
            name="mamba",
            out_shape=[
                pltpu.VMEM((tokens, width), f32),
                pltpu.VMEM((2, 3, tokens, inner), bf16),
                pltpu.VMEM((tokens, state, inner), f32),
                pltpu.VMEM((tokens, state, inner), f32),
            ],
            in_specs=[hbm] * 13,
            out_specs=[vmem] * 4,
            scratch_shapes=[
                pltpu.VMEM((tokens, width), f32),
                pltpu.VMEM((2, width * 2 * lane_tiles, 128), bf16),
                pltpu.VMEM((2, width, 2 * inner), bf16),
                pltpu.VMEM((2, inner, width), bf16),
                pltpu.VMEM((2, tokens, inner), bf16),
                pltpu.VMEM(norm_w.shape, bf16),
                pltpu.VMEM(conv_w.shape, bf16),
                pltpu.VMEM(conv_b.shape, bf16),
                pltpu.VMEM(w_x.shape, bf16),
                pltpu.VMEM((2, 128, inner), bf16),
                pltpu.VMEM(b_dt.shape, f32),
                pltpu.VMEM(a_log.shape, f32),
                pltpu.VMEM(d_skip.shape, f32),
                pltpu.VMEM((tokens, width), bf16),
                pltpu.VMEM((tokens, inner), bf16),
                pltpu.VMEM((tokens, inner), f32),
                pltpu.VMEM((tokens, width), bf16),
                pltpu.VMEM((tokens // 2, width), bf16),
                pltpu.VMEM((tokens // 4, width), bf16),
                pltpu.VMEM((tokens // 4, width), bf16),
                pltpu.VMEM((tokens // 4, width), bf16),
                pltpu.VMEM((tokens // 4, width), f32),
                pltpu.VMEM((tokens, 128), f32),
                pltpu.VMEM((2, tokens, 128), bf16),
                pltpu.VMEM((4, tokens, 128), bf16),
                pltpu.VMEM((LARGEST, inner), f32),
                pltpu.VMEM((LARGEST, inner), f32),
                pltpu.VMEM((lane_tiles, LARGEST * 8, 128), f32),
                pltpu.VMEM((LARGEST, inner), bf16),
                pltpu.SemaphoreType.DMA((KINDS, 2, CHUNKS)),
                pltpu.SemaphoreType.DMA((KINDS, 2, CHUNKS)),
                pltpu.SemaphoreType.DMA((18 + CHUNKS,)),
                pltpu.SemaphoreType.DMA((8,)),
                pltpu.SemaphoreType.DMA((2, CHUNKS)),
            ],
            compiler_params=pltpu.CompilerParams(collective_id=0, has_side_effects=True, vmem_limit_bytes=32 * 2**20),
        )(residual, w_view, w_out, conv_view, ssm_state, norm_w, conv_w, conv_b, w_x, w_dt, b_dt, a_log, d_skip)
        r_new, conv_new, ssm_new = pl.pallas_call(
            dump_kernel,
            name="dump",
            out_shape=[
                jax.ShapeDtypeStruct((tokens, width), f32),
                jax.ShapeDtypeStruct((2, 3, tokens, inner), bf16),
                jax.ShapeDtypeStruct(ssm_state.shape, f32),
            ],
            in_specs=[anywhere] * 4,
            out_specs=[hbm] * 3,
            scratch_shapes=[pltpu.SemaphoreType.DMA((2 + 2 * DUMP_PIECES,))],
            compiler_params=pltpu.CompilerParams(vmem_limit_bytes=2**20),
        )(r_val, conv_val, s0, s1)
        return r_new, conv_new.transpose(0, 2, 1, 3), ssm_new

    cache_spec = P(None, 'dp', None, 'tp')
    in_specs = (P('dp', None), P(None, None), P(None, None, None, 'tp'), P(None, None, 'tp'), P(None, 'tp'), P(None, 'tp', None), P(None, None, 'tp'), P(None, 'tp'), P(None, None, 'tp'), P(None, 'tp'), P(None, 'tp', None), cache_spec, cache_spec)
    out_specs = (P('dp', None), cache_spec, cache_spec)
    return jax.shard_map(device_step, mesh=mesh, in_specs=in_specs, out_specs=out_specs, check_vma=False)
```

```python
import functools

import jax
import jax.numpy as jnp
from jax import lax
from jax.experimental.layout import Layout, with_layout_constraint
from jax.experimental import pallas as pl
from jax.experimental.pallas import tpu as pltpu
from jax.sharding import PartitionSpec as P

MESH = pl.DeviceIdType.MESH
LOG2E = 1.4426950408889634
SIZES = (64, 128, 128, 128, 64)
CHUNKS = len(SIZES)
STARTS = tuple(sum(SIZES[:q]) for q in range(CHUNKS))
LARGEST = max(SIZES)
KINDS = 10
ORDER = (0, 1, 5, 2, 5, 0, 3, 1, 4, 2, 4, 3, 0, 1, 0, 2, 1, 3, 5, 2, 4, 0, 5, 3, 1, 4, 5, 2, 0, 3, 1, 4, 5, 0, 2, 3, 1, 0, 4, 1, 2, 0, 1, 3, 2, 4, 3, 2, 4, 0, 3, 1, 0, 4, 2, 1, 3, 2, 0, 4, 3, 1, 4, 2, 3, 4, 1, 0, 2, 3, 4, 1, 0, 2, 0, 1, 3, 4, 2, 3, 4)

W_PIECES = 3
GROUPS = {64: 16, 128: 64}
DUMP_PIECES = 4
ORDER_FIRST = tuple(dict.fromkeys(q for q in ORDER if q < CHUNKS))


def rms_scale(vector, epsilon):
    return lax.rsqrt(jnp.mean(vector * vector, axis=-1, keepdims=True) + epsilon)


def mamba_kernel(
    residual, w_in, w_out, conv_state, ssm_state, norm_w_hbm, conv_w_hbm, conv_b_hbm, w_x_hbm, w_dt_hbm, b_dt_hbm, a_log_hbm, d_skip_hbm,
    r_out, conv_out, ssm0, ssm1,
    res, w_raw, w_xz, wo, conv_old, norm_w, conv_w, conv_b, w_x, w_dt, b_dt, a_log, d_skip, hid, xc_buf, z_buf, part, half_in, quart_in, quart_sum, pair_in, o_acc,
    p_acc, p_send, p_recv, dt_buf, dx_buf, y_part, yg_buf, send_sem, recv_sem, load_sem, small_sem, state_sem,
):
    layers = 2
    tokens, width = res.shape
    inner = wo.shape[1]
    rank = w_dt_hbm.shape[1]
    state = a_log.shape[1]
    lane_tiles = inner // 128
    ssm_bufs = (ssm0, ssm1)

    tp = lax.axis_index("tp")
    core = lax.rem(tp, 2)
    pos_x = lax.rem(lax.div(tp, 2), 2)
    pos_y = lax.div(tp, 4)
    bit_a = pos_x * (1 - core) + pos_y * core
    bit_b = pos_y * (1 - core) + pos_x * core
    peer_c = tp + 1 - 2 * core
    peer_a = tp + (1 - 2 * bit_a) * (2 + 2 * core)
    peer_b = tp + (1 - 2 * bit_b) * (4 - 2 * core)
    peer_d = tp + (1 - 2 * pos_x) * 2 + (1 - 2 * pos_y) * 4
    peers = (peer_c, peer_a, peer_b, peer_d)

    barrier = pltpu.get_barrier_semaphore()
    for peer in peers:
        pl.semaphore_signal(barrier, inc=1, device_id={"tp": peer}, device_id_type=MESH)

    def rows_of(q):
        return pl.ds(STARTS[q], SIZES[q])

    def half_rows(q, which):
        half = SIZES[q] // 2
        return pl.ds(pl.multiple_of(STARTS[q] + which * half, half), half)

    def quart_rows(q, which_half, which):
        quart = SIZES[q] // 4
        return pl.ds(pl.multiple_of(STARTS[q] + which_half * (2 * quart) + which * quart, quart), quart)

    def landing(ref, q, parts):
        return ref.at[pl.ds(STARTS[q] // parts, SIZES[q] // parts)]

    def remote(kind, layer, q, src, dst, peer):
        return pltpu.make_async_remote_copy(
            src_ref=src, dst_ref=dst, send_sem=send_sem.at[kind, layer, q], recv_sem=recv_sem.at[kind, layer, q],
            device_id={"tp": peer}, device_id_type=MESH,
        )

    def p_copy(step, layer, q):
        src = p_send.at[min(step, 1), rows_of(q)]
        return remote(step, layer, q, src, p_recv.at[step, rows_of(q)], peers[step])

    def o_copy(step, layer, q):
        if step == 0:
            return remote(4, layer, q, part.at[half_rows(q, 1 - core)], landing(half_in, q, 2), peer_c)
        if step == 1:
            return remote(5, layer, q, part.at[quart_rows(q, core, 1 - bit_a)], landing(quart_in, q, 4), peer_a)
        return remote(6, layer, q, landing(quart_sum, q, 4), landing(pair_in, q, 4), peer_b)

    def h_copy(step, layer, q):
        ref = hid.at[quart_rows(q, core, 1 - bit_a if step == 2 else bit_a)]
        return remote(7 + step, layer, q, ref, ref, peer_a if step == 0 else peer_c)

    def w_load(layer, piece):
        rows = pl.ds(piece * (w_raw.shape[1] // W_PIECES), w_raw.shape[1] // W_PIECES)
        return pltpu.make_async_copy(w_in.at[layer, rows], w_raw.at[layer, rows], load_sem.at[layer * W_PIECES + piece])

    def res_load(q):
        return pltpu.make_async_copy(residual.at[rows_of(q)], res.at[rows_of(q)], load_sem.at[18 + q])

    def wo_load(layer):
        return pltpu.make_async_copy(w_out.at[layer], wo.at[layer], load_sem.at[10 + layer])

    def conv_load(layer, row):
        dst = conv_old.at[layer] if row == 0 else conv_out.at[layer, row - 1]
        return pltpu.make_async_copy(conv_state.at[layer, row], dst, load_sem.at[12 + 3 * layer + row])

    def state_load(layer, q):
        return pltpu.make_async_copy(ssm_state.at[layer, rows_of(q)], ssm_bufs[layer].at[rows_of(q)], state_sem.at[layer, q])

    small = [
        pltpu.make_async_copy(norm_w_hbm, norm_w, small_sem.at[0]),
        pltpu.make_async_copy(conv_w_hbm, conv_w, small_sem.at[1]),
        pltpu.make_async_copy(conv_b_hbm, conv_b, small_sem.at[2]),
        pltpu.make_async_copy(w_x_hbm, w_x, small_sem.at[3]),
        pltpu.make_async_copy(w_dt_hbm, w_dt.at[:, pl.ds(0, rank)], small_sem.at[4]),
        pltpu.make_async_copy(b_dt_hbm, b_dt, small_sem.at[5]),
        pltpu.make_async_copy(a_log_hbm, a_log, small_sem.at[6]),
        pltpu.make_async_copy(d_skip_hbm, d_skip, small_sem.at[7]),
    ]
    small[0].start()
    res_load(ORDER[0]).start()
    for piece in range(W_PIECES):
        w_load(0, piece).start()
    for layer in range(layers):
        w_dt[layer, rank:] = jnp.zeros((128 - rank, inner), jnp.bfloat16)

    span = 32
    packed = span * lane_tiles * 2
    blocks = width // (2 * span)

    def split_weights(layer, first, count):
        row = lax.broadcasted_iota(jnp.int32, (packed, packed), 0)
        col = lax.broadcasted_iota(jnp.int32, (packed, packed), 1)
        group = lax.div(row, span)
        want = lax.rem(row, span) * (2 * lane_tiles) + lax.rem(group, lane_tiles) * 2 + lax.div(group, lane_tiles)
        pick = jnp.where(col == want, 1.0, 0.0).astype(jnp.bfloat16)

        @pl.loop(0, count // 4)
        def _(step):
            for i in range(4):
                block = first + step * 4 + i
                raw = [w_raw[layer, pl.ds(pl.multiple_of((2 * block + k) * packed, packed), packed), :] for k in range(2)]
                both = jnp.dot(pick, jnp.concatenate(raw, axis=1), preferred_element_type=jnp.float32).astype(jnp.bfloat16)
                for k in range(2):
                    dst = pl.ds(pl.multiple_of((2 * block + k) * span, span), span)
                    for tile in range(2 * lane_tiles):
                        w_xz[layer, dst, tile * 128:(tile + 1) * 128] = both[tile * span:(tile + 1) * span, k * 128:(k + 1) * 128]

    split_step = 4

    def first_norm(q):
        res_load(q).wait()

        @pl.loop(0, SIZES[q] // 32)
        def _(i):
            sub = pl.ds(pl.multiple_of(STARTS[q] + i * 32, 32), 32)
            r = res[sub, :]
            hid[sub, :] = (r * rms_scale(r, 1e-5) * norm_w[0:1, :].astype(jnp.float32)).astype(jnp.bfloat16)

    small[0].wait()
    first_norm(ORDER[0])

    for piece in range(W_PIECES):
        w_load(0, piece).wait()
        if piece == 0:
            for row in range(3):
                conv_load(0, row).start()
            for copy in small[1:]:
                copy.start()
            for q in ORDER_FIRST[1:]:
                res_load(q).start()
        split_weights(0, piece * (blocks // W_PIECES), blocks // W_PIECES)

    for piece in range(W_PIECES):
        w_load(1, piece).start()
    for q in ORDER_FIRST:
        state_load(0, q).start()
    wo_load(0).start()
    for row in range(3):
        conv_load(0, row).wait()
    for copy in small[1:]:
        copy.wait()
    pl.semaphore_wait(barrier, 4)

    wo_ready = [False] * layers

    def stage_in(layer, q):
        rows = rows_of(q)
        if layer == 0:
            if q != ORDER[0]:
                first_norm(q)
        else:
            h_copy(1, layer - 1, q).wait()
            h_copy(2, layer - 1, q).wait()
        xz = jnp.dot(hid[rows, :], w_xz[layer], preferred_element_type=jnp.float32).astype(jnp.bfloat16)
        x_val = xz[:, :inner]
        z = xz[:, inner:].astype(jnp.float32)
        z_buf[rows, :] = z * jax.nn.sigmoid(z)
        conv_out[layer, 2, rows, :] = x_val
        taps = conv_w[layer].astype(jnp.float32)
        pre = conv_old[layer, rows, :].astype(jnp.float32) * taps[0:1]
        pre = pre + conv_out[layer, 0, rows, :].astype(jnp.float32) * taps[1:2]
        pre = pre + conv_out[layer, 1, rows, :].astype(jnp.float32) * taps[2:3]
        pre = pre + x_val.astype(jnp.float32) * taps[3:4]
        pre = pre + conv_b[layer:layer + 1, :].astype(jnp.float32)
        xc = (pre * jax.nn.sigmoid(pre)).astype(jnp.bfloat16)
        xc_buf[rows, :] = xc
        p = jnp.dot(xc, w_x[layer], preferred_element_type=jnp.float32)
        p_acc[rows, :] = p
        p_send[0, rows, :] = p.astype(jnp.bfloat16)
        p_copy(0, layer, q).start()

    def stage_p(layer, q):
        rows = rows_of(q)
        p_copy(0, layer, q).wait()
        p = p_acc[rows, :] + p_recv[0, rows, :].astype(jnp.float32)
        p_acc[rows, :] = p
        p_send[1, rows, :] = p.astype(jnp.bfloat16)
        for step in (3, 1, 2):
            p_copy(step, layer, q).start()

    def stage_ssm(layer, q):
        rows, start, chunk = rows_of(q), STARTS[q], SIZES[q]
        state_buf = ssm_bufs[layer]
        p = p_acc[rows, :]
        for step in (1, 2, 3):
            p_copy(step, layer, q).wait()
            p = p + p_recv[step, rows, :].astype(jnp.float32)
        lane = lax.broadcasted_iota(jnp.int32, p.shape, 1)
        square = p * p
        is_dt = lane < rank
        is_b = jnp.logical_and(lane >= rank, lane < rank + state)

        def scale_of(mask, count):
            total = jnp.sum(jnp.where(mask, square, 0.0), axis=1, keepdims=True)
            return lax.rsqrt(total * (1.0 / count) + 1e-6)

        scale_dt = scale_of(is_dt, rank)
        scale_b = scale_of(is_b, state)
        scale_c = scale_of(lane >= rank + state, state)
        normed = p * jnp.where(is_dt, scale_dt, jnp.where(is_b, scale_b, scale_c))
        dt_low = jnp.where(is_dt, normed, 0.0).astype(jnp.bfloat16)
        pre = jnp.dot(dt_low, w_dt[layer], preferred_element_type=jnp.float32) + b_dt[layer:layer + 1, :]
        dt = jnp.maximum(pre, 0.0) + jnp.log1p(jnp.exp(-jnp.abs(pre)))
        dt_buf[:chunk] = dt
        dx_buf[:chunk] = dt * xc_buf[rows, :].astype(jnp.float32)
        turned = jnp.concatenate([normed] * (128 // chunk), axis=0).T
        b_cols = turned[rank:rank + state, :]
        c_cols = turned[rank + state:, :]
        state_load(layer, q).wait()

        group = GROUPS[chunk]
        rate = jnp.exp(a_log[layer]) * (-LOG2E)

        def scan_group(g, carry):
            b_now, c_now = carry
            first = pl.multiple_of(g * group, group)
            states = state_buf.at[pl.ds(start + first, group)]
            dts = dt_buf.at[pl.ds(first, group)]
            dxs = dx_buf.at[pl.ds(first, group)]
            ys = [y_part.at[tile, pl.ds(pl.multiple_of(first * 8, 8 * group), 8 * group)] for tile in range(lane_tiles)]
            for j in range(group):
                new = jnp.exp2(dts[j:j + 1] * rate) * states[j] + dxs[j:j + 1] * b_now[:, j:j + 1]
                states[j] = new
                weighted = new * c_now[:, j:j + 1]
                partial = weighted[:8] + weighted[8:]
                for tile in range(lane_tiles):
                    ys[tile][j * 8:(j + 1) * 8] = partial[:, tile * 128:(tile + 1) * 128]
            return pltpu.roll(b_now, 128 - group, 1), pltpu.roll(c_now, 128 - group, 1)

        lax.fori_loop(0, chunk // group, scan_group, (b_cols, c_cols))

        @pl.loop(0, chunk // 16)
        def _(g):
            halves = []
            for k in range(2):
                first = g * 128 + k * 64
                by_tile = []
                for tile in range(lane_tiles):
                    total = y_part[tile, pl.ds(first, 8, stride=8), :]
                    for step in range(1, 8):
                        total = total + y_part[tile, pl.ds(first + step, 8, stride=8), :]
                    by_tile.append(total)
                halves.append(jnp.concatenate(by_tile, axis=1))
            sub = pl.ds(pl.multiple_of(g * 16, 16), 16)
            sub_rows = pl.ds(pl.multiple_of(start + g * 16, 16), 16)
            y = jnp.concatenate(halves, axis=0) + d_skip[layer:layer + 1, :] * xc_buf[sub_rows, :].astype(jnp.float32)
            yg_buf[sub, :] = (y * z_buf[sub_rows, :]).astype(jnp.bfloat16)

        if not wo_ready[layer]:
            wo_load(layer).wait()
            wo_ready[layer] = True
        part[rows, :] = jnp.dot(yg_buf[:chunk], wo[layer], preferred_element_type=jnp.float32).astype(jnp.bfloat16)
        o_copy(0, layer, q).start()

    def stage_half(layer, q):
        o_copy(0, layer, q).wait()
        mine = half_rows(q, core)
        part[mine, :] = (part[mine, :].astype(jnp.float32) + half_in[pl.ds(STARTS[q] // 2, SIZES[q] // 2), :].astype(jnp.float32)).astype(jnp.bfloat16)
        o_copy(1, layer, q).start()

    def stage_quart(layer, q):
        o_copy(1, layer, q).wait()
        mine = part[quart_rows(q, core, bit_a), :]
        quarter = pl.ds(STARTS[q] // 4, SIZES[q] // 4)
        quart_sum[quarter, :] = (mine.astype(jnp.float32) + quart_in[quarter, :].astype(jnp.float32)).astype(jnp.bfloat16)
        o_copy(2, layer, q).start()

    def stage_own(layer, q):
        o_copy(2, layer, q).wait()
        quart = SIZES[q] // 4
        for i in range(quart // 16):
            sub = pl.ds(STARTS[q] // 4 + i * 16, 16)
            dst = pl.ds(pl.multiple_of(STARTS[q] + core * (2 * quart) + bit_a * quart + i * 16, 16), 16)
            o_val = quart_sum[sub, :].astype(jnp.float32) + pair_in[sub, :].astype(jnp.float32)
            if layer == 0:
                o_acc[sub, :] = o_val
                r = res[dst, :] + o_val
                hid[dst, :] = (r * rms_scale(r, 1e-5) * norm_w[1:2, :].astype(jnp.float32)).astype(jnp.bfloat16)
            else:
                hid[dst, :] = (o_acc[sub, :] + o_val).astype(jnp.bfloat16)
        h_copy(0, layer, q).start()
        h_copy(1, layer, q).start()

    def stage_forward(layer, q):
        h_copy(0, layer, q).wait()
        h_copy(2, layer, q).start()

    def stage_out(q):
        h_copy(1, layers - 1, q).wait()
        h_copy(2, layers - 1, q).wait()
        rows = rows_of(q)
        r_out[rows, :] = res[rows, :] + hid[rows, :].astype(jnp.float32)

    stages = []
    for layer in range(layers):
        stages.append(functools.partial(stage_in, layer))
        stages.append(functools.partial(stage_p, layer))
        stages.append(functools.partial(stage_ssm, layer))
        stages.append(functools.partial(stage_half, layer))
        stages.append(functools.partial(stage_quart, layer))
        stages.append(functools.partial(stage_own, layer))
        stages.append(functools.partial(stage_forward, layer))
    stages.append(stage_out)

    per_layer = len(stages) // layers
    progress = [0] * CHUNKS
    second_ready = False
    fills = 0
    for q in ORDER:
        if q == CHUNKS:
            if fills == 0:
                for piece in range(W_PIECES):
                    w_load(1, piece).wait()
                for row in range(3):
                    conv_load(1, row).start()
                wo_load(1).start()
                for chunk_index in ORDER_FIRST:
                    state_load(1, chunk_index).start()
            split_weights(1, fills * split_step, split_step)
            fills += 1
        else:
            if progress[q] == per_layer and not second_ready:
                for row in range(3):
                    conv_load(1, row).wait()
                second_ready = True
            stages[progress[q]](q)
            progress[q] += 1


def dump_kernel(r_val, conv_val, ssm0, ssm1, r_hbm, conv_hbm, ssm_hbm, sems):
    copies = [pltpu.make_async_copy(r_val, r_hbm, sems.at[0]), pltpu.make_async_copy(conv_val, conv_hbm, sems.at[1])]
    piece = ssm0.shape[0] // DUMP_PIECES
    for i in range(DUMP_PIECES):
        for layer, ssm in enumerate((ssm0, ssm1)):
            rows = pl.ds(i * piece, piece)
            copies.append(pltpu.make_async_copy(ssm.at[rows], ssm_hbm.at[layer, rows], sems.at[2 + 2 * i + layer]))
    for copy in copies:
        copy.start()
    for copy in copies:
        copy.wait()


def solution(mesh):
    def device_step(residual, norm_w, w_in, conv_w, conv_b, w_x, w_dt, b_dt, a_log, d_skip, w_out, conv_state, ssm_state):
        tokens, width = residual.shape
        inner = w_out.shape[1]
        state = a_log.shape[1]
        lane_tiles = inner // 128
        w_view = w_in.reshape(2, width, 2, lane_tiles, 128).transpose(0, 1, 3, 2, 4)
        w_view = with_layout_constraint(w_view, Layout(major_to_minor=(0, 1, 2, 3, 4))).reshape(2, width * 2 * lane_tiles, 128)
        conv_view = conv_state.transpose(0, 2, 1, 3)
        vmem = pl.BlockSpec(memory_space=pltpu.VMEM)
        anywhere = pl.BlockSpec(memory_space=pl.ANY)
        hbm = pl.BlockSpec(memory_space=pltpu.HBM)
        f32, bf16 = jnp.float32, jnp.bfloat16
        r_val, conv_val, s0, s1 = pl.pallas_call(
            mamba_kernel,
            name="mamba",
            out_shape=[
                pltpu.VMEM((tokens, width), f32),
                pltpu.VMEM((2, 3, tokens, inner), bf16),
                pltpu.VMEM((tokens, state, inner), f32),
                pltpu.VMEM((tokens, state, inner), f32),
            ],
            in_specs=[hbm] * 13,
            out_specs=[vmem] * 4,
            scratch_shapes=[
                pltpu.VMEM((tokens, width), f32),
                pltpu.VMEM((2, width * 2 * lane_tiles, 128), bf16),
                pltpu.VMEM((2, width, 2 * inner), bf16),
                pltpu.VMEM((2, inner, width), bf16),
                pltpu.VMEM((2, tokens, inner), bf16),
                pltpu.VMEM(norm_w.shape, bf16),
                pltpu.VMEM(conv_w.shape, bf16),
                pltpu.VMEM(conv_b.shape, bf16),
                pltpu.VMEM(w_x.shape, bf16),
                pltpu.VMEM((2, 128, inner), bf16),
                pltpu.VMEM(b_dt.shape, f32),
                pltpu.VMEM(a_log.shape, f32),
                pltpu.VMEM(d_skip.shape, f32),
                pltpu.VMEM((tokens, width), bf16),
                pltpu.VMEM((tokens, inner), bf16),
                pltpu.VMEM((tokens, inner), f32),
                pltpu.VMEM((tokens, width), bf16),
                pltpu.VMEM((tokens // 2, width), bf16),
                pltpu.VMEM((tokens // 4, width), bf16),
                pltpu.VMEM((tokens // 4, width), bf16),
                pltpu.VMEM((tokens // 4, width), bf16),
                pltpu.VMEM((tokens // 4, width), f32),
                pltpu.VMEM((tokens, 128), f32),
                pltpu.VMEM((2, tokens, 128), bf16),
                pltpu.VMEM((4, tokens, 128), bf16),
                pltpu.VMEM((LARGEST, inner), f32),
                pltpu.VMEM((LARGEST, inner), f32),
                pltpu.VMEM((lane_tiles, LARGEST * 8, 128), f32),
                pltpu.VMEM((LARGEST, inner), bf16),
                pltpu.SemaphoreType.DMA((KINDS, 2, CHUNKS)),
                pltpu.SemaphoreType.DMA((KINDS, 2, CHUNKS)),
                pltpu.SemaphoreType.DMA((18 + CHUNKS,)),
                pltpu.SemaphoreType.DMA((8,)),
                pltpu.SemaphoreType.DMA((2, CHUNKS)),
            ],
            compiler_params=pltpu.CompilerParams(collective_id=0, has_side_effects=True, vmem_limit_bytes=32 * 2**20),
        )(residual, w_view, w_out, conv_view, ssm_state, norm_w, conv_w, conv_b, w_x, w_dt, b_dt, a_log, d_skip)
        r_new, conv_new, ssm_new = pl.pallas_call(
            dump_kernel,
            name="dump",
            out_shape=[
                jax.ShapeDtypeStruct((tokens, width), f32),
                jax.ShapeDtypeStruct((2, 3, tokens, inner), bf16),
                jax.ShapeDtypeStruct(ssm_state.shape, f32),
            ],
            in_specs=[anywhere] * 4,
            out_specs=[hbm] * 3,
            scratch_shapes=[pltpu.SemaphoreType.DMA((2 + 2 * DUMP_PIECES,))],
            compiler_params=pltpu.CompilerParams(vmem_limit_bytes=2**20),
        )(r_val, conv_val, s0, s1)
        return r_new, conv_new.transpose(0, 2, 1, 3), ssm_new

    cache_spec = P(None, 'dp', None, 'tp')
    in_specs = (P('dp', None), P(None, None), P(None, None, None, 'tp'), P(None, None, 'tp'), P(None, 'tp'), P(None, 'tp', None), P(None, None, 'tp'), P(None, 'tp'), P(None, None, 'tp'), P(None, 'tp'), P(None, 'tp', None), cache_spec, cache_spec)
    out_specs = (P('dp', None), cache_spec, cache_spec)
    return jax.shard_map(device_step, mesh=mesh, in_specs=in_specs, out_specs=out_specs, check_vma=False)
```

```python
import functools

import jax
import jax.numpy as jnp
from jax import lax
from jax.experimental.layout import Layout, with_layout_constraint
from jax.experimental import pallas as pl
from jax.experimental.pallas import tpu as pltpu
from jax.sharding import PartitionSpec as P

MESH = pl.DeviceIdType.MESH
LOG2E = 1.4426950408889634
SIZES = (64, 128, 128, 128, 64)
CHUNKS = len(SIZES)
STARTS = tuple(sum(SIZES[:q]) for q in range(CHUNKS))
LARGEST = max(SIZES)
KINDS = 10
ORDER = (0, 1, 3, 0, 2, 1, 4, 2, 3, 0, 1, 4, 0, 2, 1, 3, 5, 0, 5, 2, 4, 3, 1, 5, 4, 5, 0, 5, 2, 3, 5, 1, 4, 0, 2, 3, 1, 0, 4, 1, 2, 0, 3, 1, 2, 3, 4, 2, 0, 4, 3, 1, 4, 0, 2, 1, 3, 2, 0, 4, 3, 4, 1, 2, 3, 0, 4, 1, 2, 3, 4, 1, 2, 3, 0, 4, 3, 0, 1, 2, 4)

W_PIECES = 3
GROUPS = {64: 16, 128: 64}
DUMP_PIECES = 4
ORDER_FIRST = tuple(dict.fromkeys(q for q in ORDER if q < CHUNKS))


def rms_scale(vector, epsilon):
    return lax.rsqrt(jnp.mean(vector * vector, axis=-1, keepdims=True) + epsilon)


def mamba_kernel(
    residual, w_in, w_out, conv_state, ssm_state, norm_w_hbm, conv_w_hbm, conv_b_hbm, w_x_hbm, w_dt_hbm, b_dt_hbm, a_log_hbm, d_skip_hbm,
    r_out, conv_out, ssm0, ssm1,
    res, w_raw, w_xz, wo, conv_old, norm_w, conv_w, conv_b, w_x, w_dt, b_dt, a_log, d_skip, hid, xc_buf, z_buf, part, half_in, quart_in, quart_sum, pair_in, o_acc,
    p_acc, p_send, p_recv, dt_buf, dx_buf, y_part, yg_buf, send_sem, recv_sem, load_sem, small_sem, state_sem,
):
    layers = 2
    tokens, width = res.shape
    inner = wo.shape[1]
    rank = w_dt_hbm.shape[1]
    state = a_log.shape[1]
    lane_tiles = inner // 128
    ssm_bufs = (ssm0, ssm1)

    tp = lax.axis_index("tp")
    core = lax.rem(tp, 2)
    pos_x = lax.rem(lax.div(tp, 2), 2)
    pos_y = lax.div(tp, 4)
    bit_a = pos_x * (1 - core) + pos_y * core
    bit_b = pos_y * (1 - core) + pos_x * core
    peer_c = tp + 1 - 2 * core
    peer_a = tp + (1 - 2 * bit_a) * (2 + 2 * core)
    peer_b = tp + (1 - 2 * bit_b) * (4 - 2 * core)
    peer_d = tp + (1 - 2 * pos_x) * 2 + (1 - 2 * pos_y) * 4
    peers = (peer_c, peer_a, peer_b, peer_d)

    barrier = pltpu.get_barrier_semaphore()
    for peer in peers:
        pl.semaphore_signal(barrier, inc=1, device_id={"tp": peer}, device_id_type=MESH)

    def rows_of(q):
        return pl.ds(STARTS[q], SIZES[q])

    def half_rows(q, which):
        half = SIZES[q] // 2
        return pl.ds(pl.multiple_of(STARTS[q] + which * half, half), half)

    def quart_rows(q, which_half, which):
        quart = SIZES[q] // 4
        return pl.ds(pl.multiple_of(STARTS[q] + which_half * (2 * quart) + which * quart, quart), quart)

    def landing(ref, q, parts):
        return ref.at[pl.ds(STARTS[q] // parts, SIZES[q] // parts)]

    def remote(kind, layer, q, src, dst, peer):
        return pltpu.make_async_remote_copy(
            src_ref=src, dst_ref=dst, send_sem=send_sem.at[kind, layer, q], recv_sem=recv_sem.at[kind, layer, q],
            device_id={"tp": peer}, device_id_type=MESH,
        )

    def p_copy(step, layer, q):
        src = p_send.at[min(step, 1), rows_of(q)]
        return remote(step, layer, q, src, p_recv.at[step, rows_of(q)], peers[step])

    def o_copy(step, layer, q):
        if step == 0:
            return remote(4, layer, q, part.at[half_rows(q, 1 - core)], landing(half_in, q, 2), peer_c)
        if step == 1:
            return remote(5, layer, q, part.at[quart_rows(q, core, 1 - bit_a)], landing(quart_in, q, 4), peer_a)
        return remote(6, layer, q, landing(quart_sum, q, 4), landing(pair_in, q, 4), peer_b)

    def h_copy(step, layer, q):
        ref = hid.at[quart_rows(q, core, 1 - bit_a if step == 2 else bit_a)]
        return remote(7 + step, layer, q, ref, ref, peer_a if step == 0 else peer_c)

    def w_load(layer, piece):
        rows = pl.ds(piece * (w_raw.shape[1] // W_PIECES), w_raw.shape[1] // W_PIECES)
        return pltpu.make_async_copy(w_in.at[layer, rows], w_raw.at[layer, rows], load_sem.at[layer * W_PIECES + piece])

    def res_load(q):
        return pltpu.make_async_copy(residual.at[rows_of(q)], res.at[rows_of(q)], load_sem.at[18 + q])

    def wo_load(layer):
        return pltpu.make_async_copy(w_out.at[layer], wo.at[layer], load_sem.at[10 + layer])

    def conv_load(layer, row):
        dst = conv_old.at[layer] if row == 0 else conv_out.at[layer, row - 1]
        return pltpu.make_async_copy(conv_state.at[layer, row], dst, load_sem.at[12 + 3 * layer + row])

    def state_load(layer, q):
        return pltpu.make_async_copy(ssm_state.at[layer, rows_of(q)], ssm_bufs[layer].at[rows_of(q)], state_sem.at[layer, q])

    small = [
        pltpu.make_async_copy(norm_w_hbm, norm_w, small_sem.at[0]),
        pltpu.make_async_copy(conv_w_hbm, conv_w, small_sem.at[1]),
        pltpu.make_async_copy(conv_b_hbm, conv_b, small_sem.at[2]),
        pltpu.make_async_copy(w_x_hbm, w_x, small_sem.at[3]),
        pltpu.make_async_copy(w_dt_hbm, w_dt.at[:, pl.ds(0, rank)], small_sem.at[4]),
        pltpu.make_async_copy(b_dt_hbm, b_dt, small_sem.at[5]),
        pltpu.make_async_copy(a_log_hbm, a_log, small_sem.at[6]),
        pltpu.make_async_copy(d_skip_hbm, d_skip, small_sem.at[7]),
    ]
    small[0].start()
    res_load(ORDER[0]).start()
    for piece in range(W_PIECES):
        w_load(0, piece).start()
    for row in range(3):
        conv_load(0, row).start()
    for copy in small[1:]:
        copy.start()
    for layer in range(layers):
        w_dt[layer, rank:] = jnp.zeros((128 - rank, inner), jnp.bfloat16)

    span = 32
    packed = span * lane_tiles * 2
    blocks = width // (2 * span)

    def split_weights(layer, first, count):
        row = lax.broadcasted_iota(jnp.int32, (packed, packed), 0)
        col = lax.broadcasted_iota(jnp.int32, (packed, packed), 1)
        group = lax.div(row, span)
        want = lax.rem(row, span) * (2 * lane_tiles) + lax.rem(group, lane_tiles) * 2 + lax.div(group, lane_tiles)
        pick = jnp.where(col == want, 1.0, 0.0).astype(jnp.bfloat16)

        @pl.loop(0, count // 4)
        def _(step):
            for i in range(4):
                block = first + step * 4 + i
                raw = [w_raw[layer, pl.ds(pl.multiple_of((2 * block + k) * packed, packed), packed), :] for k in range(2)]
                both = jnp.dot(pick, jnp.concatenate(raw, axis=1), preferred_element_type=jnp.float32).astype(jnp.bfloat16)
                for k in range(2):
                    dst = pl.ds(pl.multiple_of((2 * block + k) * span, span), span)
                    for tile in range(2 * lane_tiles):
                        w_xz[layer, dst, tile * 128:(tile + 1) * 128] = both[tile * span:(tile + 1) * span, k * 128:(k + 1) * 128]

    split_step = 4

    def first_norm(q):
        res_load(q).wait()

        @pl.loop(0, SIZES[q] // 32)
        def _(i):
            sub = pl.ds(pl.multiple_of(STARTS[q] + i * 32, 32), 32)
            r = res[sub, :]
            hid[sub, :] = (r * rms_scale(r, 1e-5) * norm_w[0:1, :].astype(jnp.float32)).astype(jnp.bfloat16)

    small[0].wait()
    first_norm(ORDER[0])

    for piece in range(W_PIECES):
        w_load(0, piece).wait()
        if piece == 0:
            for q in ORDER_FIRST[1:]:
                res_load(q).start()
        split_weights(0, piece * (blocks // W_PIECES), blocks // W_PIECES)

    for piece in range(W_PIECES):
        w_load(1, piece).start()
    for q in ORDER_FIRST:
        state_load(0, q).start()
    wo_load(0).start()
    for row in range(3):
        conv_load(0, row).wait()
    for copy in small[1:]:
        copy.wait()
    pl.semaphore_wait(barrier, 4)

    wo_ready = [False] * layers

    def stage_in(layer, q):
        rows = rows_of(q)
        if layer == 0:
            if q != ORDER[0]:
                first_norm(q)
        else:
            h_copy(1, layer - 1, q).wait()
            h_copy(2, layer - 1, q).wait()
        xz = jnp.dot(hid[rows, :], w_xz[layer], preferred_element_type=jnp.float32).astype(jnp.bfloat16)
        x_val = xz[:, :inner]
        z = xz[:, inner:].astype(jnp.float32)
        z_buf[rows, :] = z * jax.nn.sigmoid(z)
        conv_out[layer, 2, rows, :] = x_val
        taps = conv_w[layer].astype(jnp.float32)
        pre = conv_old[layer, rows, :].astype(jnp.float32) * taps[0:1]
        pre = pre + conv_out[layer, 0, rows, :].astype(jnp.float32) * taps[1:2]
        pre = pre + conv_out[layer, 1, rows, :].astype(jnp.float32) * taps[2:3]
        pre = pre + x_val.astype(jnp.float32) * taps[3:4]
        pre = pre + conv_b[layer:layer + 1, :].astype(jnp.float32)
        xc = (pre * jax.nn.sigmoid(pre)).astype(jnp.bfloat16)
        xc_buf[rows, :] = xc
        p = jnp.dot(xc, w_x[layer], preferred_element_type=jnp.float32)
        p_acc[rows, :] = p
        p_send[0, rows, :] = p.astype(jnp.bfloat16)
        p_copy(0, layer, q).start()

    def stage_p(layer, q):
        rows = rows_of(q)
        p_copy(0, layer, q).wait()
        p = p_acc[rows, :] + p_recv[0, rows, :].astype(jnp.float32)
        p_acc[rows, :] = p
        p_send[1, rows, :] = p.astype(jnp.bfloat16)
        for step in (3, 1, 2):
            p_copy(step, layer, q).start()

    def stage_ssm(layer, q):
        rows, start, chunk = rows_of(q), STARTS[q], SIZES[q]
        state_buf = ssm_bufs[layer]
        p = p_acc[rows, :]
        for step in (1, 2, 3):
            p_copy(step, layer, q).wait()
            p = p + p_recv[step, rows, :].astype(jnp.float32)
        lane = lax.broadcasted_iota(jnp.int32, p.shape, 1)
        square = p * p
        is_dt = lane < rank
        is_b = jnp.logical_and(lane >= rank, lane < rank + state)

        def scale_of(mask, count):
            total = jnp.sum(jnp.where(mask, square, 0.0), axis=1, keepdims=True)
            return lax.rsqrt(total * (1.0 / count) + 1e-6)

        scale_dt = scale_of(is_dt, rank)
        scale_b = scale_of(is_b, state)
        scale_c = scale_of(lane >= rank + state, state)
        normed = p * jnp.where(is_dt, scale_dt, jnp.where(is_b, scale_b, scale_c))
        dt_low = jnp.where(is_dt, normed, 0.0).astype(jnp.bfloat16)
        pre = jnp.dot(dt_low, w_dt[layer], preferred_element_type=jnp.float32) + b_dt[layer:layer + 1, :]
        dt = jnp.maximum(pre, 0.0) + jnp.log1p(jnp.exp(-jnp.abs(pre)))
        dt_buf[:chunk] = dt
        dx_buf[:chunk] = dt * xc_buf[rows, :].astype(jnp.float32)
        turned = jnp.concatenate([normed] * (128 // chunk), axis=0).T
        b_cols = turned[rank:rank + state, :]
        c_cols = turned[rank + state:, :]
        state_load(layer, q).wait()

        group = GROUPS[chunk]
        rate = jnp.exp(a_log[layer]) * (-LOG2E)

        def scan_group(g, carry):
            b_now, c_now = carry
            first = pl.multiple_of(g * group, group)
            states = state_buf.at[pl.ds(start + first, group)]
            dts = dt_buf.at[pl.ds(first, group)]
            dxs = dx_buf.at[pl.ds(first, group)]
            ys = [y_part.at[tile, pl.ds(pl.multiple_of(first * 8, 8 * group), 8 * group)] for tile in range(lane_tiles)]
            for j in range(group):
                new = jnp.exp2(dts[j:j + 1] * rate) * states[j] + dxs[j:j + 1] * b_now[:, j:j + 1]
                states[j] = new
                weighted = new * c_now[:, j:j + 1]
                partial = weighted[:8] + weighted[8:]
                for tile in range(lane_tiles):
                    ys[tile][j * 8:(j + 1) * 8] = partial[:, tile * 128:(tile + 1) * 128]
            return pltpu.roll(b_now, 128 - group, 1), pltpu.roll(c_now, 128 - group, 1)

        lax.fori_loop(0, chunk // group, scan_group, (b_cols, c_cols))

        @pl.loop(0, chunk // 16)
        def _(g):
            halves = []
            for k in range(2):
                first = g * 128 + k * 64
                by_tile = []
                for tile in range(lane_tiles):
                    total = y_part[tile, pl.ds(first, 8, stride=8), :]
                    for step in range(1, 8):
                        total = total + y_part[tile, pl.ds(first + step, 8, stride=8), :]
                    by_tile.append(total)
                halves.append(jnp.concatenate(by_tile, axis=1))
            sub = pl.ds(pl.multiple_of(g * 16, 16), 16)
            sub_rows = pl.ds(pl.multiple_of(start + g * 16, 16), 16)
            y = jnp.concatenate(halves, axis=0) + d_skip[layer:layer + 1, :] * xc_buf[sub_rows, :].astype(jnp.float32)
            yg_buf[sub, :] = (y * z_buf[sub_rows, :]).astype(jnp.bfloat16)

        if not wo_ready[layer]:
            wo_load(layer).wait()
            wo_ready[layer] = True
        part[rows, :] = jnp.dot(yg_buf[:chunk], wo[layer], preferred_element_type=jnp.float32).astype(jnp.bfloat16)
        o_copy(0, layer, q).start()

    def stage_half(layer, q):
        o_copy(0, layer, q).wait()
        mine = half_rows(q, core)
        part[mine, :] = (part[mine, :].astype(jnp.float32) + half_in[pl.ds(STARTS[q] // 2, SIZES[q] // 2), :].astype(jnp.float32)).astype(jnp.bfloat16)
        o_copy(1, layer, q).start()

    def stage_quart(layer, q):
        o_copy(1, layer, q).wait()
        mine = part[quart_rows(q, core, bit_a), :]
        quarter = pl.ds(STARTS[q] // 4, SIZES[q] // 4)
        quart_sum[quarter, :] = (mine.astype(jnp.float32) + quart_in[quarter, :].astype(jnp.float32)).astype(jnp.bfloat16)
        o_copy(2, layer, q).start()

    def stage_own(layer, q):
        o_copy(2, layer, q).wait()
        quart = SIZES[q] // 4
        for i in range(quart // 16):
            sub = pl.ds(STARTS[q] // 4 + i * 16, 16)
            dst = pl.ds(pl.multiple_of(STARTS[q] + core * (2 * quart) + bit_a * quart + i * 16, 16), 16)
            o_val = quart_sum[sub, :].astype(jnp.float32) + pair_in[sub, :].astype(jnp.float32)
            if layer == 0:
                o_acc[sub, :] = o_val
                r = res[dst, :] + o_val
                hid[dst, :] = (r * rms_scale(r, 1e-5) * norm_w[1:2, :].astype(jnp.float32)).astype(jnp.bfloat16)
            else:
                hid[dst, :] = (o_acc[sub, :] + o_val).astype(jnp.bfloat16)
        h_copy(0, layer, q).start()
        h_copy(1, layer, q).start()

    def stage_forward(layer, q):
        h_copy(0, layer, q).wait()
        h_copy(2, layer, q).start()

    def stage_out(q):
        h_copy(1, layers - 1, q).wait()
        h_copy(2, layers - 1, q).wait()
        rows = rows_of(q)
        r_out[rows, :] = res[rows, :] + hid[rows, :].astype(jnp.float32)

    stages = []
    for layer in range(layers):
        stages.append(functools.partial(stage_in, layer))
        stages.append(functools.partial(stage_p, layer))
        stages.append(functools.partial(stage_ssm, layer))
        stages.append(functools.partial(stage_half, layer))
        stages.append(functools.partial(stage_quart, layer))
        stages.append(functools.partial(stage_own, layer))
        stages.append(functools.partial(stage_forward, layer))
    stages.append(stage_out)

    per_layer = len(stages) // layers
    progress = [0] * CHUNKS
    second_ready = False
    fills = 0
    for q in ORDER:
        if q == CHUNKS:
            if fills == 0:
                for piece in range(W_PIECES):
                    w_load(1, piece).wait()
                for row in range(3):
                    conv_load(1, row).start()
                wo_load(1).start()
                for chunk_index in ORDER_FIRST:
                    state_load(1, chunk_index).start()
            split_weights(1, fills * split_step, split_step)
            fills += 1
        else:
            if progress[q] == per_layer and not second_ready:
                for row in range(3):
                    conv_load(1, row).wait()
                second_ready = True
            stages[progress[q]](q)
            progress[q] += 1


def dump_kernel(r_val, conv_val, ssm0, ssm1, r_hbm, conv_hbm, ssm_hbm, sems):
    copies = [pltpu.make_async_copy(r_val, r_hbm, sems.at[0]), pltpu.make_async_copy(conv_val, conv_hbm, sems.at[1])]
    piece = ssm0.shape[0] // DUMP_PIECES
    for i in range(DUMP_PIECES):
        for layer, ssm in enumerate((ssm0, ssm1)):
            rows = pl.ds(i * piece, piece)
            copies.append(pltpu.make_async_copy(ssm.at[rows], ssm_hbm.at[layer, rows], sems.at[2 + 2 * i + layer]))
    for copy in copies:
        copy.start()
    for copy in copies:
        copy.wait()


def solution(mesh):
    def device_step(residual, norm_w, w_in, conv_w, conv_b, w_x, w_dt, b_dt, a_log, d_skip, w_out, conv_state, ssm_state):
        tokens, width = residual.shape
        inner = w_out.shape[1]
        state = a_log.shape[1]
        lane_tiles = inner // 128
        w_view = w_in.reshape(2, width, 2, lane_tiles, 128).transpose(0, 1, 3, 2, 4)
        w_view = with_layout_constraint(w_view, Layout(major_to_minor=(0, 1, 2, 3, 4))).reshape(2, width * 2 * lane_tiles, 128)
        conv_view = conv_state.transpose(0, 2, 1, 3)
        vmem = pl.BlockSpec(memory_space=pltpu.VMEM)
        anywhere = pl.BlockSpec(memory_space=pl.ANY)
        hbm = pl.BlockSpec(memory_space=pltpu.HBM)
        f32, bf16 = jnp.float32, jnp.bfloat16
        r_val, conv_val, s0, s1 = pl.pallas_call(
            mamba_kernel,
            name="mamba",
            out_shape=[
                pltpu.VMEM((tokens, width), f32),
                pltpu.VMEM((2, 3, tokens, inner), bf16),
                pltpu.VMEM((tokens, state, inner), f32),
                pltpu.VMEM((tokens, state, inner), f32),
            ],
            in_specs=[hbm] * 13,
            out_specs=[vmem] * 4,
            scratch_shapes=[
                pltpu.VMEM((tokens, width), f32),
                pltpu.VMEM((2, width * 2 * lane_tiles, 128), bf16),
                pltpu.VMEM((2, width, 2 * inner), bf16),
                pltpu.VMEM((2, inner, width), bf16),
                pltpu.VMEM((2, tokens, inner), bf16),
                pltpu.VMEM(norm_w.shape, bf16),
                pltpu.VMEM(conv_w.shape, bf16),
                pltpu.VMEM(conv_b.shape, bf16),
                pltpu.VMEM(w_x.shape, bf16),
                pltpu.VMEM((2, 128, inner), bf16),
                pltpu.VMEM(b_dt.shape, f32),
                pltpu.VMEM(a_log.shape, f32),
                pltpu.VMEM(d_skip.shape, f32),
                pltpu.VMEM((tokens, width), bf16),
                pltpu.VMEM((tokens, inner), bf16),
                pltpu.VMEM((tokens, inner), f32),
                pltpu.VMEM((tokens, width), bf16),
                pltpu.VMEM((tokens // 2, width), bf16),
                pltpu.VMEM((tokens // 4, width), bf16),
                pltpu.VMEM((tokens // 4, width), bf16),
                pltpu.VMEM((tokens // 4, width), bf16),
                pltpu.VMEM((tokens // 4, width), f32),
                pltpu.VMEM((tokens, 128), f32),
                pltpu.VMEM((2, tokens, 128), bf16),
                pltpu.VMEM((4, tokens, 128), bf16),
                pltpu.VMEM((LARGEST, inner), f32),
                pltpu.VMEM((LARGEST, inner), f32),
                pltpu.VMEM((lane_tiles, LARGEST * 8, 128), f32),
                pltpu.VMEM((LARGEST, inner), bf16),
                pltpu.SemaphoreType.DMA((KINDS, 2, CHUNKS)),
                pltpu.SemaphoreType.DMA((KINDS, 2, CHUNKS)),
                pltpu.SemaphoreType.DMA((18 + CHUNKS,)),
                pltpu.SemaphoreType.DMA((8,)),
                pltpu.SemaphoreType.DMA((2, CHUNKS)),
            ],
            compiler_params=pltpu.CompilerParams(collective_id=0, has_side_effects=True, vmem_limit_bytes=32 * 2**20),
        )(residual, w_view, w_out, conv_view, ssm_state, norm_w, conv_w, conv_b, w_x, w_dt, b_dt, a_log, d_skip)
        r_new, conv_new, ssm_new = pl.pallas_call(
            dump_kernel,
            name="dump",
            out_shape=[
                jax.ShapeDtypeStruct((tokens, width), f32),
                jax.ShapeDtypeStruct((2, 3, tokens, inner), bf16),
                jax.ShapeDtypeStruct(ssm_state.shape, f32),
            ],
            in_specs=[anywhere] * 4,
            out_specs=[hbm] * 3,
            scratch_shapes=[pltpu.SemaphoreType.DMA((2 + 2 * DUMP_PIECES,))],
            compiler_params=pltpu.CompilerParams(vmem_limit_bytes=2**20),
        )(r_val, conv_val, s0, s1)
        return r_new, conv_new.transpose(0, 2, 1, 3), ssm_new

    cache_spec = P(None, 'dp', None, 'tp')
    in_specs = (P('dp', None), P(None, None), P(None, None, None, 'tp'), P(None, None, 'tp'), P(None, 'tp'), P(None, 'tp', None), P(None, None, 'tp'), P(None, 'tp'), P(None, None, 'tp'), P(None, 'tp'), P(None, 'tp', None), cache_spec, cache_spec)
    out_specs = (P('dp', None), cache_spec, cache_spec)
    return jax.shard_map(device_step, mesh=mesh, in_specs=in_specs, out_specs=out_specs, check_vma=False)
```

```python
import functools

import jax
import jax.numpy as jnp
from jax import lax
from jax.experimental.layout import Layout, with_layout_constraint
from jax.experimental import pallas as pl
from jax.experimental.pallas import tpu as pltpu
from jax.sharding import PartitionSpec as P

MESH = pl.DeviceIdType.MESH
LOG2E = 1.4426950408889634
SIZES = (64, 128, 128, 128, 64)
CHUNKS = len(SIZES)
STARTS = tuple(sum(SIZES[:q]) for q in range(CHUNKS))
LARGEST = max(SIZES)
KINDS = 10
ORDER = (0, 1, 0, 2, 1, 3, 5, 5, 5, 4, 2, 5, 3, 0, 1, 4, 0, 2, 1, 3, 5, 2, 0, 4, 3, 1, 5, 4, 2, 0, 3, 1, 4, 2, 0, 3, 1, 0, 4, 1, 0, 2, 3, 1, 2, 3, 4, 2, 0, 3, 4, 1, 4, 0, 2, 1, 3, 2, 0, 4, 3, 1, 4, 2, 3, 0, 4, 1, 2, 3, 4, 1, 2, 0, 3, 4, 3, 0, 1, 2, 4)

W_PIECES = 3
GROUPS = {64: 16, 128: 64}
DUMP_PIECES = 4
ORDER_FIRST = tuple(dict.fromkeys(q for q in ORDER if q < CHUNKS))


def rms_scale(vector, epsilon):
    return lax.rsqrt(jnp.mean(vector * vector, axis=-1, keepdims=True) + epsilon)


def mamba_kernel(
    residual, w_in, w_out, conv_state, ssm_state, norm_w_hbm, conv_w_hbm, conv_b_hbm, w_x_hbm, w_dt_hbm, b_dt_hbm, a_log_hbm, d_skip_hbm,
    r_out, conv_out, ssm0, ssm1,
    res, w_raw, w_xz, wo, conv_old, norm_w, conv_w, conv_b, w_x, w_dt, b_dt, a_log, d_skip, hid, xc_buf, z_buf, part, half_in, quart_in, quart_sum, pair_in, o_acc,
    p_acc, p_send, p_recv, dt_buf, dx_buf, y_part, yg_buf, send_sem, recv_sem, load_sem, small_sem, state_sem,
):
    layers = 2
    tokens, width = res.shape
    inner = wo.shape[1]
    rank = w_dt_hbm.shape[1]
    state = a_log.shape[1]
    lane_tiles = inner // 128
    ssm_bufs = (ssm0, ssm1)

    tp = lax.axis_index("tp")
    core = lax.rem(tp, 2)
    pos_x = lax.rem(lax.div(tp, 2), 2)
    pos_y = lax.div(tp, 4)
    bit_a = pos_x * (1 - core) + pos_y * core
    bit_b = pos_y * (1 - core) + pos_x * core
    peer_c = tp + 1 - 2 * core
    peer_a = tp + (1 - 2 * bit_a) * (2 + 2 * core)
    peer_b = tp + (1 - 2 * bit_b) * (4 - 2 * core)
    peer_d = tp + (1 - 2 * pos_x) * 2 + (1 - 2 * pos_y) * 4
    peers = (peer_c, peer_a, peer_b, peer_d)

    barrier = pltpu.get_barrier_semaphore()
    for peer in peers:
        pl.semaphore_signal(barrier, inc=1, device_id={"tp": peer}, device_id_type=MESH)

    def rows_of(q):
        return pl.ds(STARTS[q], SIZES[q])

    def half_rows(q, which):
        half = SIZES[q] // 2
        return pl.ds(pl.multiple_of(STARTS[q] + which * half, half), half)

    def quart_rows(q, which_half, which):
        quart = SIZES[q] // 4
        return pl.ds(pl.multiple_of(STARTS[q] + which_half * (2 * quart) + which * quart, quart), quart)

    def landing(ref, q, parts):
        return ref.at[pl.ds(STARTS[q] // parts, SIZES[q] // parts)]

    def remote(kind, layer, q, src, dst, peer):
        return pltpu.make_async_remote_copy(
            src_ref=src, dst_ref=dst, send_sem=send_sem.at[kind, layer, q], recv_sem=recv_sem.at[kind, layer, q],
            device_id={"tp": peer}, device_id_type=MESH,
        )

    def p_copy(step, layer, q):
        src = p_send.at[min(step, 1), rows_of(q)]
        return remote(step, layer, q, src, p_recv.at[step, rows_of(q)], peers[step])

    def o_copy(step, layer, q):
        if step == 0:
            return remote(4, layer, q, part.at[half_rows(q, 1 - core)], landing(half_in, q, 2), peer_c)
        if step == 1:
            return remote(5, layer, q, part.at[quart_rows(q, core, 1 - bit_a)], landing(quart_in, q, 4), peer_a)
        return remote(6, layer, q, landing(quart_sum, q, 4), landing(pair_in, q, 4), peer_b)

    def h_copy(step, layer, q):
        ref = hid.at[quart_rows(q, core, 1 - bit_a if step == 2 else bit_a)]
        return remote(7 + step, layer, q, ref, ref, peer_a if step == 0 else peer_c)

    def w_load(layer, piece):
        rows = pl.ds(piece * (w_raw.shape[1] // W_PIECES), w_raw.shape[1] // W_PIECES)
        return pltpu.make_async_copy(w_in.at[layer, rows], w_raw.at[layer, rows], load_sem.at[layer * W_PIECES + piece])

    def res_load(q):
        return pltpu.make_async_copy(residual.at[rows_of(q)], res.at[rows_of(q)], load_sem.at[18 + q])

    def wo_load(layer):
        return pltpu.make_async_copy(w_out.at[layer], wo.at[layer], load_sem.at[10 + layer])

    def conv_load(layer, row):
        dst = conv_old.at[layer] if row == 0 else conv_out.at[layer, row - 1]
        return pltpu.make_async_copy(conv_state.at[layer, row], dst, load_sem.at[12 + 3 * layer + row])

    def state_load(layer, q):
        return pltpu.make_async_copy(ssm_state.at[layer, rows_of(q)], ssm_bufs[layer].at[rows_of(q)], state_sem.at[layer, q])

    small = [
        pltpu.make_async_copy(norm_w_hbm, norm_w, small_sem.at[0]),
        pltpu.make_async_copy(conv_w_hbm, conv_w, small_sem.at[1]),
        pltpu.make_async_copy(conv_b_hbm, conv_b, small_sem.at[2]),
        pltpu.make_async_copy(w_x_hbm, w_x, small_sem.at[3]),
        pltpu.make_async_copy(w_dt_hbm, w_dt.at[:, pl.ds(0, rank)], small_sem.at[4]),
        pltpu.make_async_copy(b_dt_hbm, b_dt, small_sem.at[5]),
        pltpu.make_async_copy(a_log_hbm, a_log, small_sem.at[6]),
        pltpu.make_async_copy(d_skip_hbm, d_skip, small_sem.at[7]),
    ]
    small[0].start()
    res_load(ORDER[0]).start()
    for piece in range(W_PIECES):
        w_load(0, piece).start()
    for q in range(CHUNKS):
        if q != ORDER[0]:
            res_load(q).start()
    for row in range(3):
        conv_load(0, row).start()
    for copy in small[1:]:
        copy.start()
    for layer in range(layers):
        w_dt[layer, rank:] = jnp.zeros((128 - rank, inner), jnp.bfloat16)

    span = 32
    packed = span * lane_tiles * 2
    blocks = width // (2 * span)

    def split_weights(layer, first, count):
        row = lax.broadcasted_iota(jnp.int32, (packed, packed), 0)
        col = lax.broadcasted_iota(jnp.int32, (packed, packed), 1)
        group = lax.div(row, span)
        want = lax.rem(row, span) * (2 * lane_tiles) + lax.rem(group, lane_tiles) * 2 + lax.div(group, lane_tiles)
        pick = jnp.where(col == want, 1.0, 0.0).astype(jnp.bfloat16)

        @pl.loop(0, count // 4)
        def _(step):
            for i in range(4):
                block = first + step * 4 + i
                raw = [w_raw[layer, pl.ds(pl.multiple_of((2 * block + k) * packed, packed), packed), :] for k in range(2)]
                both = jnp.dot(pick, jnp.concatenate(raw, axis=1), preferred_element_type=jnp.float32).astype(jnp.bfloat16)
                for k in range(2):
                    dst = pl.ds(pl.multiple_of((2 * block + k) * span, span), span)
                    for tile in range(2 * lane_tiles):
                        w_xz[layer, dst, tile * 128:(tile + 1) * 128] = both[tile * span:(tile + 1) * span, k * 128:(k + 1) * 128]

    split_step = 4

    def first_norm(q):
        res_load(q).wait()

        @pl.loop(0, SIZES[q] // 32)
        def _(i):
            sub = pl.ds(pl.multiple_of(STARTS[q] + i * 32, 32), 32)
            r = res[sub, :]
            hid[sub, :] = (r * rms_scale(r, 1e-5) * norm_w[0:1, :].astype(jnp.float32)).astype(jnp.bfloat16)

    small[0].wait()
    first_norm(ORDER[0])

    for piece in range(W_PIECES):
        w_load(0, piece).wait()
        split_weights(0, piece * (blocks // W_PIECES), blocks // W_PIECES)

    for piece in range(W_PIECES):
        w_load(1, piece).start()
    for q in ORDER_FIRST:
        state_load(0, q).start()
    wo_load(0).start()
    for row in range(3):
        conv_load(0, row).wait()
    for copy in small[1:]:
        copy.wait()
    pl.semaphore_wait(barrier, 4)

    wo_ready = [False] * layers

    def stage_in(layer, q):
        rows = rows_of(q)
        if layer == 0:
            if q != ORDER[0]:
                first_norm(q)
        else:
            h_copy(1, layer - 1, q).wait()
            h_copy(2, layer - 1, q).wait()
        xz = jnp.dot(hid[rows, :], w_xz[layer], preferred_element_type=jnp.float32).astype(jnp.bfloat16)
        x_val = xz[:, :inner]
        z = xz[:, inner:].astype(jnp.float32)
        z_buf[rows, :] = z * jax.nn.sigmoid(z)
        conv_out[layer, 2, rows, :] = x_val
        taps = conv_w[layer].astype(jnp.float32)
        pre = conv_old[layer, rows, :].astype(jnp.float32) * taps[0:1]
        pre = pre + conv_out[layer, 0, rows, :].astype(jnp.float32) * taps[1:2]
        pre = pre + conv_out[layer, 1, rows, :].astype(jnp.float32) * taps[2:3]
        pre = pre + x_val.astype(jnp.float32) * taps[3:4]
        pre = pre + conv_b[layer:layer + 1, :].astype(jnp.float32)
        xc = (pre * jax.nn.sigmoid(pre)).astype(jnp.bfloat16)
        xc_buf[rows, :] = xc
        p = jnp.dot(xc, w_x[layer], preferred_element_type=jnp.float32)
        p_acc[rows, :] = p
        p_send[0, rows, :] = p.astype(jnp.bfloat16)
        p_copy(0, layer, q).start()

    def stage_p(layer, q):
        rows = rows_of(q)
        p_copy(0, layer, q).wait()
        p = p_acc[rows, :] + p_recv[0, rows, :].astype(jnp.float32)
        p_acc[rows, :] = p
        p_send[1, rows, :] = p.astype(jnp.bfloat16)
        for step in (3, 1, 2):
            p_copy(step, layer, q).start()

    def stage_ssm(layer, q):
        rows, start, chunk = rows_of(q), STARTS[q], SIZES[q]
        state_buf = ssm_bufs[layer]
        p = p_acc[rows, :]
        for step in (1, 2, 3):
            p_copy(step, layer, q).wait()
            p = p + p_recv[step, rows, :].astype(jnp.float32)
        lane = lax.broadcasted_iota(jnp.int32, p.shape, 1)
        square = p * p
        is_dt = lane < rank
        is_b = jnp.logical_and(lane >= rank, lane < rank + state)

        def scale_of(mask, count):
            total = jnp.sum(jnp.where(mask, square, 0.0), axis=1, keepdims=True)
            return lax.rsqrt(total * (1.0 / count) + 1e-6)

        scale_dt = scale_of(is_dt, rank)
        scale_b = scale_of(is_b, state)
        scale_c = scale_of(lane >= rank + state, state)
        normed = p * jnp.where(is_dt, scale_dt, jnp.where(is_b, scale_b, scale_c))
        dt_low = jnp.where(is_dt, normed, 0.0).astype(jnp.bfloat16)
        pre = jnp.dot(dt_low, w_dt[layer], preferred_element_type=jnp.float32) + b_dt[layer:layer + 1, :]
        dt = jnp.maximum(pre, 0.0) + jnp.log1p(jnp.exp(-jnp.abs(pre)))
        dt_buf[:chunk] = dt
        dx_buf[:chunk] = dt * xc_buf[rows, :].astype(jnp.float32)
        turned = jnp.concatenate([normed] * (128 // chunk), axis=0).T
        b_cols = turned[rank:rank + state, :]
        c_cols = turned[rank + state:, :]
        state_load(layer, q).wait()

        group = GROUPS[chunk]
        rate = jnp.exp(a_log[layer]) * (-LOG2E)

        def scan_group(g, carry):
            b_now, c_now = carry
            first = pl.multiple_of(g * group, group)
            states = state_buf.at[pl.ds(start + first, group)]
            dts = dt_buf.at[pl.ds(first, group)]
            dxs = dx_buf.at[pl.ds(first, group)]
            ys = [y_part.at[tile, pl.ds(pl.multiple_of(first * 8, 8 * group), 8 * group)] for tile in range(lane_tiles)]
            for j in range(group):
                new = jnp.exp2(dts[j:j + 1] * rate) * states[j] + dxs[j:j + 1] * b_now[:, j:j + 1]
                states[j] = new
                weighted = new * c_now[:, j:j + 1]
                partial = weighted[:8] + weighted[8:]
                for tile in range(lane_tiles):
                    ys[tile][j * 8:(j + 1) * 8] = partial[:, tile * 128:(tile + 1) * 128]
            return pltpu.roll(b_now, 128 - group, 1), pltpu.roll(c_now, 128 - group, 1)

        lax.fori_loop(0, chunk // group, scan_group, (b_cols, c_cols))

        @pl.loop(0, chunk // 16)
        def _(g):
            halves = []
            for k in range(2):
                first = g * 128 + k * 64
                by_tile = []
                for tile in range(lane_tiles):
                    total = y_part[tile, pl.ds(first, 8, stride=8), :]
                    for step in range(1, 8):
                        total = total + y_part[tile, pl.ds(first + step, 8, stride=8), :]
                    by_tile.append(total)
                halves.append(jnp.concatenate(by_tile, axis=1))
            sub = pl.ds(pl.multiple_of(g * 16, 16), 16)
            sub_rows = pl.ds(pl.multiple_of(start + g * 16, 16), 16)
            y = jnp.concatenate(halves, axis=0) + d_skip[layer:layer + 1, :] * xc_buf[sub_rows, :].astype(jnp.float32)
            yg_buf[sub, :] = (y * z_buf[sub_rows, :]).astype(jnp.bfloat16)

        if not wo_ready[layer]:
            wo_load(layer).wait()
            wo_ready[layer] = True
        part[rows, :] = jnp.dot(yg_buf[:chunk], wo[layer], preferred_element_type=jnp.float32).astype(jnp.bfloat16)
        o_copy(0, layer, q).start()

    def stage_half(layer, q):
        o_copy(0, layer, q).wait()
        mine = half_rows(q, core)
        part[mine, :] = (part[mine, :].astype(jnp.float32) + half_in[pl.ds(STARTS[q] // 2, SIZES[q] // 2), :].astype(jnp.float32)).astype(jnp.bfloat16)
        o_copy(1, layer, q).start()

    def stage_quart(layer, q):
        o_copy(1, layer, q).wait()
        mine = part[quart_rows(q, core, bit_a), :]
        quarter = pl.ds(STARTS[q] // 4, SIZES[q] // 4)
        quart_sum[quarter, :] = (mine.astype(jnp.float32) + quart_in[quarter, :].astype(jnp.float32)).astype(jnp.bfloat16)
        o_copy(2, layer, q).start()

    def stage_own(layer, q):
        o_copy(2, layer, q).wait()
        quart = SIZES[q] // 4
        for i in range(quart // 16):
            sub = pl.ds(STARTS[q] // 4 + i * 16, 16)
            dst = pl.ds(pl.multiple_of(STARTS[q] + core * (2 * quart) + bit_a * quart + i * 16, 16), 16)
            o_val = quart_sum[sub, :].astype(jnp.float32) + pair_in[sub, :].astype(jnp.float32)
            if layer == 0:
                o_acc[sub, :] = o_val
                r = res[dst, :] + o_val
                hid[dst, :] = (r * rms_scale(r, 1e-5) * norm_w[1:2, :].astype(jnp.float32)).astype(jnp.bfloat16)
            else:
                hid[dst, :] = (o_acc[sub, :] + o_val).astype(jnp.bfloat16)
        h_copy(0, layer, q).start()
        h_copy(1, layer, q).start()

    def stage_forward(layer, q):
        h_copy(0, layer, q).wait()
        h_copy(2, layer, q).start()

    def stage_out(q):
        h_copy(1, layers - 1, q).wait()
        h_copy(2, layers - 1, q).wait()
        rows = rows_of(q)
        r_out[rows, :] = res[rows, :] + hid[rows, :].astype(jnp.float32)

    stages = []
    for layer in range(layers):
        stages.append(functools.partial(stage_in, layer))
        stages.append(functools.partial(stage_p, layer))
        stages.append(functools.partial(stage_ssm, layer))
        stages.append(functools.partial(stage_half, layer))
        stages.append(functools.partial(stage_quart, layer))
        stages.append(functools.partial(stage_own, layer))
        stages.append(functools.partial(stage_forward, layer))
    stages.append(stage_out)

    per_layer = len(stages) // layers
    progress = [0] * CHUNKS
    second_ready = False
    fills = 0
    for q in ORDER:
        if q == CHUNKS:
            if fills == 0:
                for piece in range(W_PIECES):
                    w_load(1, piece).wait()
                for row in range(3):
                    conv_load(1, row).start()
                wo_load(1).start()
                for chunk_index in ORDER_FIRST:
                    state_load(1, chunk_index).start()
            split_weights(1, fills * split_step, split_step)
            fills += 1
        else:
            if progress[q] == per_layer and not second_ready:
                for row in range(3):
                    conv_load(1, row).wait()
                second_ready = True
            stages[progress[q]](q)
            progress[q] += 1


def dump_kernel(r_val, conv_val, ssm0, ssm1, r_hbm, conv_hbm, ssm_hbm, sems):
    copies = [pltpu.make_async_copy(r_val, r_hbm, sems.at[0]), pltpu.make_async_copy(conv_val, conv_hbm, sems.at[1])]
    piece = ssm0.shape[0] // DUMP_PIECES
    for i in range(DUMP_PIECES):
        for layer, ssm in enumerate((ssm0, ssm1)):
            rows = pl.ds(i * piece, piece)
            copies.append(pltpu.make_async_copy(ssm.at[rows], ssm_hbm.at[layer, rows], sems.at[2 + 2 * i + layer]))
    for copy in copies:
        copy.start()
    for copy in copies:
        copy.wait()


def solution(mesh):
    def device_step(residual, norm_w, w_in, conv_w, conv_b, w_x, w_dt, b_dt, a_log, d_skip, w_out, conv_state, ssm_state):
        tokens, width = residual.shape
        inner = w_out.shape[1]
        state = a_log.shape[1]
        lane_tiles = inner // 128
        w_view = w_in.reshape(2, width, 2, lane_tiles, 128).transpose(0, 1, 3, 2, 4)
        w_view = with_layout_constraint(w_view, Layout(major_to_minor=(0, 1, 2, 3, 4))).reshape(2, width * 2 * lane_tiles, 128)
        conv_view = conv_state.transpose(0, 2, 1, 3)
        vmem = pl.BlockSpec(memory_space=pltpu.VMEM)
        anywhere = pl.BlockSpec(memory_space=pl.ANY)
        hbm = pl.BlockSpec(memory_space=pltpu.HBM)
        f32, bf16 = jnp.float32, jnp.bfloat16
        r_val, conv_val, s0, s1 = pl.pallas_call(
            mamba_kernel,
            name="mamba",
            out_shape=[
                pltpu.VMEM((tokens, width), f32),
                pltpu.VMEM((2, 3, tokens, inner), bf16),
                pltpu.VMEM((tokens, state, inner), f32),
                pltpu.VMEM((tokens, state, inner), f32),
            ],
            in_specs=[hbm] * 13,
            out_specs=[vmem] * 4,
            scratch_shapes=[
                pltpu.VMEM((tokens, width), f32),
                pltpu.VMEM((2, width * 2 * lane_tiles, 128), bf16),
                pltpu.VMEM((2, width, 2 * inner), bf16),
                pltpu.VMEM((2, inner, width), bf16),
                pltpu.VMEM((2, tokens, inner), bf16),
                pltpu.VMEM(norm_w.shape, bf16),
                pltpu.VMEM(conv_w.shape, bf16),
                pltpu.VMEM(conv_b.shape, bf16),
                pltpu.VMEM(w_x.shape, bf16),
                pltpu.VMEM((2, 128, inner), bf16),
                pltpu.VMEM(b_dt.shape, f32),
                pltpu.VMEM(a_log.shape, f32),
                pltpu.VMEM(d_skip.shape, f32),
                pltpu.VMEM((tokens, width), bf16),
                pltpu.VMEM((tokens, inner), bf16),
                pltpu.VMEM((tokens, inner), f32),
                pltpu.VMEM((tokens, width), bf16),
                pltpu.VMEM((tokens // 2, width), bf16),
                pltpu.VMEM((tokens // 4, width), bf16),
                pltpu.VMEM((tokens // 4, width), bf16),
                pltpu.VMEM((tokens // 4, width), bf16),
                pltpu.VMEM((tokens // 4, width), f32),
                pltpu.VMEM((tokens, 128), f32),
                pltpu.VMEM((2, tokens, 128), bf16),
                pltpu.VMEM((4, tokens, 128), bf16),
                pltpu.VMEM((LARGEST, inner), f32),
                pltpu.VMEM((LARGEST, inner), f32),
                pltpu.VMEM((lane_tiles, LARGEST * 8, 128), f32),
                pltpu.VMEM((LARGEST, inner), bf16),
                pltpu.SemaphoreType.DMA((KINDS, 2, CHUNKS)),
                pltpu.SemaphoreType.DMA((KINDS, 2, CHUNKS)),
                pltpu.SemaphoreType.DMA((18 + CHUNKS,)),
                pltpu.SemaphoreType.DMA((8,)),
                pltpu.SemaphoreType.DMA((2, CHUNKS)),
            ],
            compiler_params=pltpu.CompilerParams(collective_id=0, has_side_effects=True, vmem_limit_bytes=32 * 2**20),
        )(residual, w_view, w_out, conv_view, ssm_state, norm_w, conv_w, conv_b, w_x, w_dt, b_dt, a_log, d_skip)
        r_new, conv_new, ssm_new = pl.pallas_call(
            dump_kernel,
            name="dump",
            out_shape=[
                jax.ShapeDtypeStruct((tokens, width), f32),
                jax.ShapeDtypeStruct((2, 3, tokens, inner), bf16),
                jax.ShapeDtypeStruct(ssm_state.shape, f32),
            ],
            in_specs=[anywhere] * 4,
            out_specs=[hbm] * 3,
            scratch_shapes=[pltpu.SemaphoreType.DMA((2 + 2 * DUMP_PIECES,))],
            compiler_params=pltpu.CompilerParams(vmem_limit_bytes=2**20),
        )(r_val, conv_val, s0, s1)
        return r_new, conv_new.transpose(0, 2, 1, 3), ssm_new

    cache_spec = P(None, 'dp', None, 'tp')
    in_specs = (P('dp', None), P(None, None), P(None, None, None, 'tp'), P(None, None, 'tp'), P(None, 'tp'), P(None, 'tp', None), P(None, None, 'tp'), P(None, 'tp'), P(None, None, 'tp'), P(None, 'tp'), P(None, 'tp', None), cache_spec, cache_spec)
    out_specs = (P('dp', None), cache_spec, cache_spec)
    return jax.shard_map(device_step, mesh=mesh, in_specs=in_specs, out_specs=out_specs, check_vma=False)
```
